512 devices in a mesh: gy: 64 (over x, z, core), gx: 8 (over y).
Axes of the slice: x: 4, y: 8, z: 8, core: 2. Of those that a mesh axis runs over, the one named last changes fastest.
Arguments:
- level_set: float32 [4096, 4096], P('gy', 'gx'), may hold values from -6 to 6
- velocity: float32 [2, 4096, 4096], P(None, 'gy', 'gx'), may hold values from -2 to 2
- particles: float32 [32768, 3, 128], P(('gy', 'gx')), may hold values from -0.5 to 0.5
- escaped: int32 [32768, 128], P(('gy', 'gx')), may hold values 0 or 1
- home_cell: int32 [32768], P(('gy', 'gx')), may hold values from 0 to 32767
- land_cell: int32 [32768], P(('gy', 'gx')), may hold values from 0 to 32767
- dest_rank: int32 [32768], P(('gy', 'gx')), may hold values from 0 to 63, as said below
- block_count: int32 [512], P(('gy', 'gx')), may hold values from 48 to 64, as said below
Outputs:
- new_level: float32 [4096, 4096], P('gy', 'gx')
- moved_blocks: float32 [131072, 4, 128], P(('gy', 'gx'))
The draws below stay inside these ranges and needn't reach their ends.
Inputs may be any that keep to these rules, and one draw needn't show every extreme that they name: `block_count`: live blocks are the first ones of a device; in every draw some device holds 64 live blocks. `dest_rank`: among one device's live blocks at most 4 go to one band; in every draw one band receives exactly 4 live blocks from every device.
All inputs are finite; a program needn't handle non-finite values. No bound on the sum of `escaped` on one device may be relied on, other than what follows from the above.
Results may differ from the reference program's by a relative error of at most 0.0003.
Values sent between devices are 32-bit elements; how exact they have to be, the bound alone decides.
No kernel may reach another device: no remote copies, remote signals or barrier semaphores. Data moves between devices by JAX's collectives and lax.ppermute only.
A program may use at most 64 MiB of HBM per device.

```python
import math
import jax
import jax.numpy as jnp
from jax import lax

CY = 64
CX = 512
NB_DEV = 64
PPB = 128
CAP = 4
NY = 4096
NX = 4096
BLOCKS = 32768
RECV = 131072
N_GY = 64
N_GX = 8
DEVICES = 512


def migration_plan(key):
    slot_count = N_GY * CAP
    hot_band = jax.random.randint(jax.random.fold_in(key, 7), (), 0, N_GY)
    is_hot = (jnp.arange(slot_count, dtype=jnp.int32) // CAP == hot_band).astype(jnp.int32)

    def one_device(device_index):
        subkeys = jax.random.split(jax.random.fold_in(key, 1000 + device_index), 4)
        scores = (jax.random.randint(subkeys[0], (slot_count,), 0, 2 ** 20) + is_hot * 2 ** 22) * slot_count
        scores = scores + jnp.arange(slot_count, dtype=jnp.int32)
        chosen = jnp.argsort(-scores)[:NB_DEV] // CAP
        halfway = NB_DEV // 2
        front_part = jax.random.permutation(subkeys[1], chosen[:halfway])
        back_part = jax.random.permutation(subkeys[2], chosen[halfway:])
        live_total = jax.random.randint(subkeys[3], (), NB_DEV - NB_DEV // 4, NB_DEV + 1)
        return (jnp.concatenate([front_part, back_part]), live_total)
    destinations, tallies = jax.vmap(one_device)(jnp.arange(DEVICES, dtype=jnp.int32))
    filled_device = jax.random.randint(jax.random.fold_in(key, 9), (), 0, DEVICES)
    tallies = jnp.where(jnp.arange(DEVICES, dtype=jnp.int32) == filled_device, NB_DEV, tallies)
    return (destinations.reshape(-1).astype(jnp.int32), tallies.astype(jnp.int32))


def cell_draw(key):
    subkeys = jax.random.split(key, 4)
    row_pick = jax.random.randint(subkeys[0], (BLOCKS,), 0, CY)
    column_pick = jax.random.randint(subkeys[1], (BLOCKS,), 0, CX)
    row_pick = jnp.where(jax.random.randint(subkeys[2], (BLOCKS,), 0, 4) == 0, CY - 1, row_pick)
    column_pick = jnp.where(jax.random.randint(subkeys[3], (BLOCKS,), 0, 4) == 0, CX - 1, column_pick)
    return (row_pick * CX + column_pick).astype(jnp.int32)


def draw_dest_rank(key, part):
    return migration_plan(key)[0]


def draw_block_count(key, part):
    return migration_plan(key)[1]


def draw_home_cell(key, part):
    return cell_draw(jax.random.fold_in(key, 21))


def draw_land_cell(key, part):
    return cell_draw(jax.random.fold_in(key, 22))


def draw_level_set(key, part):
    subkeys = jax.random.split(jax.random.fold_in(key, 31), 2)
    row_global = jnp.arange(NY, dtype=jnp.int32)[:, None]
    column_global = jnp.arange(NX, dtype=jnp.int32)[None, :]
    row_local = row_global % CY
    column_local = column_global % CX
    near_edge = (row_local < 9) | (row_local >= CY - 9) | (column_local < 9) | (column_local >= CX - 9)
    parity = ((row_global + column_global) % 2 * 2 - 1).astype(jnp.float32)
    magnitude = jnp.clip(1.0 + 2.0 * jnp.abs(jax.random.normal(subkeys[0], (NY, NX), jnp.float32)), 1.0, 6.0)
    flipped = jax.random.uniform(subkeys[1], (NY, NX), jnp.float32) < 0.25
    signed = jnp.where(flipped, -1.0, 1.0) * parity * magnitude
    return jnp.where(near_edge, signed, 0.05 * signed).astype(jnp.float32)


def draw_velocity(key, part):
    subkeys = jax.random.split(jax.random.fold_in(key, 41), 2)
    magnitude = jax.random.uniform(subkeys[0], (2, NY, NX), jnp.float32, 1.0, 2.0)
    positive = jax.random.uniform(subkeys[1], (2, NY, NX), jnp.float32) < 0.5
    return jnp.where(positive, magnitude, -magnitude).astype(jnp.float32)


def set_ends(values, stream_key, low, largest):
    dims = values.shape
    place = [jax.random.randint(jax.random.fold_in(stream_key, axis), (), 0, dims[axis]) for axis in range(len(dims))]
    values = values.at[tuple(place)].set(low)
    longest = dims.index(max(dims))
    place[longest] = (place[longest] + 1) % dims[longest]
    return values.at[tuple(place)].set(largest)


def steps_of(rng, extent, cuts, low, high):
    level, own = 1.0, jax.random.fold_in(rng, 6)
    for dim, blocks in cuts:
        steps = jnp.exp(jax.random.uniform(jax.random.fold_in(own, dim), (blocks,), jnp.float32, low / len(cuts), high / len(cuts)))
        level = level * jnp.repeat(steps, extent[dim] // blocks).reshape([-1 if axis == dim else 1 for axis in range(len(extent))])
    return level


def setup_inputs(seed: int = 0) -> dict:
    key_of = jax.random.split(jax.random.key(seed), 9)
    level_set = draw_level_set(jax.random.fold_in(key_of[8], 71), 0)
    velocity = draw_velocity(jax.random.fold_in(key_of[8], 71), 0)
    particles = jnp.clip(jax.random.uniform(key_of[2], (BLOCKS, 3, PPB), jnp.float32, -0.5, 0.5) * steps_of(key_of[2], (BLOCKS, 3, PPB), ((0, 512),), -0.4, 0.0), -0.5, 0.5)
    escaped = set_ends((jax.random.randint(key_of[3], (BLOCKS, PPB), 0, 2) < 1).astype(jnp.int32), jax.random.fold_in(key_of[3], 1), 0, 1)
    home_cell = draw_home_cell(jax.random.fold_in(key_of[8], 71), 0)
    land_cell = draw_land_cell(jax.random.fold_in(key_of[8], 71), 0)
    dest_rank = draw_dest_rank(jax.random.fold_in(key_of[8], 71), 0)
    block_count = draw_block_count(jax.random.fold_in(key_of[8], 71), 0)
    return dict(level_set=level_set, velocity=velocity, particles=particles, escaped=escaped, home_cell=home_cell, land_cell=land_cell, dest_rank=dest_rank, block_count=block_count)


time_step = 0.3
epsilon_weno = 1e-6


def blended(a, b, c, d, e):
    smooth_one = 13.0 / 12.0 * (a - 2.0 * b + c) ** 2 + 0.25 * (a - 4.0 * b + 3.0 * c) ** 2
    smooth_two = 13.0 / 12.0 * (b - 2.0 * c + d) ** 2 + 0.25 * (b - d) ** 2
    smooth_three = 13.0 / 12.0 * (c - 2.0 * d + e) ** 2 + 0.25 * (3.0 * c - 4.0 * d + e) ** 2
    weight_one = 0.1 / (smooth_one + epsilon_weno) ** 2
    weight_two = 0.6 / (smooth_two + epsilon_weno) ** 2
    weight_three = 0.3 / (smooth_three + epsilon_weno) ** 2
    weight_sum = weight_one + weight_two + weight_three
    candidate = (weight_one * (a / 3.0 - 7.0 * b / 6.0 + 11.0 * c / 6.0)
                 + weight_two * (-b / 6.0 + 5.0 * c / 6.0 + d / 3.0)
                 + weight_three * (c / 3.0 + 5.0 * d / 6.0 - e / 6.0))
    return candidate / weight_sum


def upwinded(shifted, advecting):
    differences = [shifted(k + 1) - shifted(k) for k in range(-3, 3)]
    left_sided = blended(differences[0], differences[1], differences[2], differences[3], differences[4])
    right_sided = blended(differences[5], differences[4], differences[3], differences[2], differences[1])
    return advecting * jnp.where(advecting > 0, left_sided, right_sided)


def tendency(padded, along_x, along_y):
    height = along_x.shape[0]
    across = along_x.shape[1]

    def columns(k):
        return padded[3:3 + height, 3 + k:3 + k + across]

    def rows_at(k):
        return padded[3 + k:3 + k + height, 3:3 + across]

    return -(upwinded(columns, along_x) + upwinded(rows_at, along_y))


def full_tendency(surface, velocity):
    padded = jnp.pad(surface, 3, mode="wrap")
    band_rows = math.gcd(NY, 256)

    def one_band(start):
        window = lax.dynamic_slice_in_dim(padded, start, band_rows + 6, 0)
        along_x = lax.dynamic_slice_in_dim(velocity[0], start, band_rows, 0)
        along_y = lax.dynamic_slice_in_dim(velocity[1], start, band_rows, 0)
        return tendency(window, along_x, along_y)

    starts = jnp.arange(NY // band_rows, dtype=jnp.int32) * band_rows
    return lax.map(one_band, starts).reshape(NY, NX)


def advect(offset_x, offset_y, corners):
    fraction_y = offset_y + 0.5
    fraction_x = offset_x + 0.5

    def mixture(component):
        c = corners[:, component]
        return ((1.0 - fraction_y) * (1.0 - fraction_x) * c[:, 0:1] + fraction_y * (1.0 - fraction_x) * c[:, 1:2]
                + (1.0 - fraction_y) * fraction_x * c[:, 2:3] + fraction_y * fraction_x * c[:, 3:4])

    return offset_x + time_step * mixture(0), offset_y + time_step * mixture(1)


def reference(level_set, velocity, particles, escaped, home_cell, land_cell, dest_rank, block_count):
    section_one = level_set + time_step * full_tendency(level_set, velocity)
    section_two = 0.75 * level_set + 0.25 * (section_one + time_step * full_tendency(section_one, velocity))
    section_three = level_set / 3.0 + 2.0 / 3.0 * (section_two + time_step * full_tendency(section_two, velocity))

    blocks = jnp.arange(BLOCKS, dtype=jnp.int32)
    device = blocks // NB_DEV
    band_index = device // N_GX
    strip_index = device % N_GX
    local_index = blocks % NB_DEV
    is_live = local_index < block_count[device]
    home_row = band_index * CY + home_cell // CX
    home_column = strip_index * CX + home_cell % CX
    next_row = (home_row + 1) % NY
    next_column = (home_column + 1) % NX
    corners = jnp.stack([velocity[:, home_row, home_column], velocity[:, next_row, home_column],
                         velocity[:, home_row, next_column], velocity[:, next_row, next_column]], axis=-1)
    corners = jnp.transpose(corners, (1, 0, 2))
    new_x, new_y = advect(particles[:, 0, :], particles[:, 1, :], corners)
    radius = particles[:, 2, :]
    weight = escaped.astype(jnp.float32) * radius
    moved_rows = jnp.stack([new_x, new_y, radius, weight], axis=1)

    grouped = dest_rank.reshape(DEVICES, NB_DEV)
    live_grid = is_live.reshape(DEVICES, NB_DEV)
    position = jnp.arange(NB_DEV, dtype=jnp.int32)
    earlier_same = ((grouped[:, None, :] == grouped[:, :, None]) & live_grid[:, None, :]
                    & (position[None, :] < position[:, None])[None])
    slot_rank = jnp.sum(earlier_same.astype(jnp.int32), axis=2).reshape(-1)
    target = (dest_rank * N_GX + strip_index) * (N_GY * CAP) + band_index * CAP + slot_rank
    target = jnp.where(is_live, target, RECV)
    moved_blocks = jnp.zeros((RECV, 4, PPB), jnp.float32).at[target].set(moved_rows, mode="drop")

    land_row = dest_rank * CY + land_cell // CX
    land_next = (land_row + 1) % NY
    land_column = strip_index * CX + land_cell % CX
    land_right = (land_column + 1) % NX
    fraction_y = new_y + 0.5
    fraction_x = new_x + 0.5
    carried = weight * is_live.astype(jnp.float32)[:, None]
    low_low = jnp.sum(carried * (1.0 - fraction_y) * (1.0 - fraction_x), axis=1)
    high_low = jnp.sum(carried * fraction_y * (1.0 - fraction_x), axis=1)
    low_high = jnp.sum(carried * (1.0 - fraction_y) * fraction_x, axis=1)
    high_high = jnp.sum(carried * fraction_y * fraction_x, axis=1)
    deposit = jnp.zeros((NY, NX), jnp.float32)
    deposit = deposit.at[land_row, land_column].add(low_low)
    deposit = deposit.at[land_next, land_column].add(high_low)
    deposit = deposit.at[land_row, land_right].add(low_high)
    deposit = deposit.at[land_next, land_right].add(high_high)
    return section_three + deposit, moved_blocks
```

```python
import functools
import jax
import jax.numpy as jnp
from jax import lax
from jax.experimental import pallas as pl
from jax.experimental.pallas import tpu as pltpu
from jax.sharding import PartitionSpec as P

CAP = 4
DT = 0.3
INTERPRET = False
F32 = jnp.float32
BF16 = jnp.bfloat16


def iota(shape, dim):
    return lax.broadcasted_iota(jnp.int32, shape, dim).astype(F32)


def split3(x):
    hi = x.astype(BF16)
    rest = x - hi.astype(F32)
    mid = rest.astype(BF16)
    lo = (rest - mid.astype(F32)).astype(BF16)
    return hi, mid, lo


def mm(a, b):
    return lax.dot_general(a, b, (((1,), (0,)), ((), ())), preferred_element_type=F32)


def exact_pick(one_hot, x):
    hi, mid, lo = split3(x)
    return (mm(one_hot, hi) + mm(one_hot, mid)) + mm(one_hot, lo)


def eye(n):
    return iota((n, n), 0) == iota((n, n), 1)


def to_column(row, n):
    return jnp.sum(jnp.where(eye(n), jnp.broadcast_to(row, (n, n)), 0.0), axis=1, keepdims=True)


def to_row(col, n):
    return jnp.sum(jnp.where(eye(n), jnp.broadcast_to(col, (n, n)), 0.0), axis=0, keepdims=True)


def one_hot(mask):
    return jnp.where(mask, 1.0, 0.0).astype(BF16)


def floor_div(x, k):
    return jnp.floor((x + 0.5) * (1.0 / k))


def call(body, outs, *args, scratch=()):
    vm = pl.BlockSpec(memory_space=pltpu.VMEM)
    return pl.pallas_call(
        body,
        out_shape=tuple(outs),
        in_specs=[vm] * len(args),
        out_specs=tuple(vm for _ in outs),
        scratch_shapes=list(scratch),
        interpret=INTERPRET,
    )(*args)


def prepare_body(u_ref, v_ref, rad_ref, esc_ref, ints_ref, count_ref, meta_ref, w_ref, sel_ref):
    n = rad_ref.shape[0]
    height, across = u_ref.shape
    ints = ints_ref[...].astype(F32)
    home = to_column(ints[0:1], n)
    land = to_column(ints[1:2], n)
    dest_row = ints[2:3]
    dest = to_column(dest_row, n)
    count = count_ref[...].astype(F32)
    row = floor_div(home, across)
    col = home - row * across
    land_row = floor_div(land, across)
    land_col = land - land_row * across
    other = iota((n, n), 0)
    mine = iota((n, n), 1)
    same = (dest == dest_row) & (other < mine) & (other < count)
    rank_row = jnp.sum(jnp.where(same, 1.0, 0.0), axis=0, keepdims=True)
    live_row = iota((1, n), 1) < count
    slot_row = jnp.where(live_row, dest_row * CAP + rank_row, -1.0)
    slot = to_column(slot_row, n)
    lane = iota((n, height), 1)
    pick = jnp.concatenate([one_hot(lane == row), one_hot(lane == row + 1.0)], axis=0)
    lanes = iota((n, across), 1)
    at0 = lanes == col
    at1 = lanes == col + 1.0
    parts = []
    for ref in (u_ref, v_ref):
        both = exact_pick(pick, ref[...])
        low = both[0:n]
        high = both[n:]
        for where_at in (at0, at1):
            for rows in (low, high):
                parts.append(jnp.sum(jnp.where(where_at, rows, 0.0), axis=1, keepdims=True))
    columns = parts + [row, col, land_row, land_col, slot]
    lane = iota((n, 128), 1)
    meta = jnp.zeros((n, 128), F32)
    for i, value in enumerate(columns):
        meta = jnp.where(lane == float(i), value, meta)
    meta_ref[...] = meta
    w_ref[...] = esc_ref[...].astype(F32) * rad_ref[...]
    total = sel_ref.shape[0]
    step = 4 * CAP + 1
    r = iota((total, 1), 0)
    d = floor_div(r, step)
    q = r - d * step
    code = jnp.where(q < 4.0 * CAP, d * (4.0 * CAP) + q, -1000.0)
    slots = jnp.concatenate([slot_row * 4.0 + float(j) for j in range(4)], axis=1)
    slots = jnp.where(jnp.concatenate([slot_row] * 4, axis=1) < 0.0, -1.0, slots)
    sel_ref[...] = one_hot(code == slots)


def edges_body(f_ref, u_ref, v_ref, below_ref, meta_ref, x_ref, y_ref, w_ref, left_ref, right_ref, meta2_ref):
    n = x_ref.shape[0]
    height, across = f_ref.shape
    meta = meta_ref[...]
    lane = iota((n, 128), 1)
    row = meta[:, 8:9]
    col = meta[:, 9:10]
    last = row == float(height - 1)
    lanes = iota((n, across), 1)
    at0 = (lanes == col) & last
    at1 = (lanes == col + 1.0) & last
    for base, r in ((0, 9), (4, 15)):
        line = jnp.broadcast_to(below_ref[r : r + 1, :], (n, across))
        c10 = jnp.sum(jnp.where(at0, line, 0.0), axis=1, keepdims=True)
        c11 = jnp.sum(jnp.where(at1, line, 0.0), axis=1, keepdims=True)
        meta = meta + jnp.where(lane == float(base + 1), c10, 0.0) + jnp.where(lane == float(base + 3), c11, 0.0)
    meta2_ref[...] = meta
    far = across - 128

    def pack_left(f, u, v):
        lane = iota(f.shape, 1)
        return jnp.where(lane < 16.0, f, jnp.where(lane < 32.0, pltpu.roll(u, 16, 1), pltpu.roll(v, 32, 1)))

    def pack_right(f, u, v, m):
        lane = iota(f.shape, 1)
        out = jnp.where(
            lane >= 112.0, f, jnp.where(lane >= 96.0, pltpu.roll(u, 112, 1), pltpu.roll(v, 96, 1))
        )
        return jnp.where(lane < 16.0, m, out)

    left_ref[0:height] = pack_left(f_ref[:, 0:128], u_ref[:, 0:128], v_ref[:, 0:128])
    right_ref[0:height] = pack_right(f_ref[:, far:], u_ref[:, far:], v_ref[:, far:], meta)
    zero = jnp.zeros((8, 128), F32)
    left_ref[height : height + 8] = pack_left(below_ref[0:8, 0:128], below_ref[9:17, 0:128], below_ref[15:23, 0:128])
    left_ref[height + 8 : height + 16] = pack_left(below_ref[8:16, 0:128], zero, zero)
    right_ref[height : height + 8] = pack_right(below_ref[0:8, far:], below_ref[9:17, far:], below_ref[15:23, far:], zero)
    right_ref[height + 8 : height + 16] = pack_right(below_ref[8:16, far:], zero, zero, zero)
    top = height + 16
    right_ref[top : top + n] = x_ref[...]
    right_ref[top + n : top + 2 * n] = y_ref[...]
    right_ref[top + 2 * n : top + 3 * n] = w_ref[...]


def halo_tiles(from_right, from_left):
    lane = iota(from_right.shape, 1)
    right_side = lane < 64.0
    f = jnp.where(right_side, from_right, from_left)
    u = jnp.where(right_side, pltpu.roll(from_right, 112, 1), pltpu.roll(from_left, 16, 1))
    v = jnp.where(right_side, pltpu.roll(from_right, 96, 1), pltpu.roll(from_left, 32, 1))
    return f, u, v


def moved_particles(meta, x, y, column, across):
    n = x.shape[0]
    row = meta[:, 8:9]
    last = meta[:, 9:10] == float(across - 1)
    lane = iota((n, column.shape[0]), 1)
    pick = jnp.concatenate([one_hot((lane == row) & last), one_hot((lane == row + 1.0) & last)], axis=0)
    both = exact_pick(pick, column)
    low = both[0:n]
    high = both[n:]
    u = [meta[:, 0:1], meta[:, 1:2], meta[:, 2:3] + low[:, 16:17], meta[:, 3:4] + high[:, 16:17]]
    v = [meta[:, 4:5], meta[:, 5:6], meta[:, 6:7] + low[:, 32:33], meta[:, 7:8] + high[:, 32:33]]
    fy = y + 0.5
    fx = x + 0.5
    w00 = (1.0 - fy) * (1.0 - fx)
    w10 = fy * (1.0 - fx)
    w01 = (1.0 - fy) * fx
    w11 = fy * fx
    new_x = x + DT * (w00 * u[0] + w10 * u[1] + w01 * u[2] + w11 * u[3])
    new_y = y + DT * (w00 * v[0] + w10 * v[1] + w01 * v[2] + w11 * v[3])
    return new_x, new_y


def lane_sum(x):
    return jnp.sum(x, axis=1, keepdims=True)


def pack_body(
    f_ref, u_ref, v_ref, x_ref, y_ref, rad_ref, w_ref, meta_ref, mine_ref, left_ref, right_ref, sel_ref, out_ref, tail_ref
):
    n = x_ref.shape[0]
    height, across = f_ref.shape
    bands = out_ref.shape[0] // (4 * CAP + 1)
    meta = meta_ref[...]
    top = height + 16
    w = w_ref[...]
    new_x, new_y = moved_particles(meta, x_ref[...], y_ref[...], right_ref[...], across)
    left_meta = left_ref[0:n]
    left_w = left_ref[top + 2 * n : top + 3 * n]
    left_x, left_y = moved_particles(
        left_meta, left_ref[top : top + n], left_ref[top + n : top + 2 * n], mine_ref[...], across
    )
    body = jnp.concatenate([new_x, new_y, rad_ref[...], w], axis=0)
    out_ref[...] = exact_pick(sel_ref[...], body)
    gy = new_y + 0.5
    gx = new_x + 0.5
    sums = [
        meta[:, 10:11],
        meta[:, 11:12],
        lane_sum(w * (1.0 - gy) * (1.0 - gx)),
        lane_sum(w * gy * (1.0 - gx)),
        lane_sum(w * (1.0 - gy) * gx),
        lane_sum(w * gy * gx),
    ]
    lane = iota((n, 128), 1)
    lane16 = lane - 16.0 * jnp.floor(lane * 0.0625)
    mine = jnp.zeros((n, 128), F32)
    for i, value in enumerate(sums):
        mine = jnp.where(lane16 == float(i), value, mine)
    gy = left_y + 0.5
    gx = left_x + 0.5
    over = left_meta[:, 11:12] == float(across - 1)
    sums = [
        left_meta[:, 10:11],
        jnp.where(over, lane_sum(left_w * (1.0 - gy) * gx), 0.0),
        jnp.where(over, lane_sum(left_w * gy * gx), 0.0),
    ]
    theirs = jnp.zeros((n, 128), F32)
    for i, value in enumerate(sums):
        theirs = jnp.where(lane16 == float(8 + i), value, theirs)
    values = jnp.concatenate([mine, theirs], axis=0)
    slot = jnp.concatenate([to_row(meta[:, 12:13], n), to_row(left_meta[:, 12:13], n)], axis=1)
    d4 = iota((bands, 2 * n), 0) * float(CAP)
    choose = jnp.concatenate([one_hot(d4 + float(k) == slot) for k in range(CAP)], axis=0)
    chosen = exact_pick(choose, values)
    lane = iota((bands, 128), 1)
    group = jnp.floor(lane * 0.0625)
    table = jnp.zeros((bands, 128), F32)
    for k in range(CAP):
        table = jnp.where(group == float(k), chosen[k * bands : (k + 1) * bands], table)
    table = table + pltpu.roll(pltpu.roll(table, 1, 0), 64, 1)
    step = 4 * CAP + 1
    out_ref[pl.ds(4 * CAP, bands, stride=step), :] = table
    f4, u4, v4 = halo_tiles(right_ref[height - 16 : height], left_ref[height - 16 : height])
    tail_ref[0:9, 0:across] = f_ref[height - 9 : height]
    tail_ref[9:15, 0:across] = u_ref[height - 6 : height]
    tail_ref[15:21, 0:across] = v_ref[height - 6 : height]
    tail_ref[0:9, across:] = f4[7:16]
    tail_ref[9:15, across:] = u4[10:16]
    tail_ref[15:21, across:] = v4[10:16]
    tail_ref[21:24, :] = jnp.zeros((3, across + 128), F32)


def side_term(speed, e0, e1, e2, e3, e4, d2, d3):
    ahead = speed > 0.0
    p = jnp.where(ahead, e0, e4)
    q = jnp.where(ahead, e1, e3)
    s = jnp.where(ahead, e3, e1)
    c = jnp.where(ahead, d2, d3)
    r = e2
    rr = r * r
    t1 = p * (4.0 * p - 11.0 * q) + (10.0 * (q * q) + 3e-6)
    t2 = q * (4.0 * q - 5.0 * r) + (4.0 * rr + 3e-6)
    t3 = s * (4.0 * s - 11.0 * r) + (10.0 * rr + 3e-6)
    a1 = t2 * t3
    a2 = t1 * t3
    a3 = t1 * t2
    w1 = a1 * a1
    w2 = 6.0 * (a2 * a2)
    w3 = 3.0 * (a3 * a3)
    top = w1 * (2.0 * p - 5.0 * q) - w2 * (q + 2.0 * r) + w3 * (s - 4.0 * r)
    return speed * c + jnp.abs(speed) * (top / (6.0 * (w1 + w2 + w3)))


def stencil_body(f_ref, u_ref, v_ref, below_ref, right_ref, left_ref, above_ref, out_ref, f0, us, vs, f1, f2):
    height, across = f_ref.shape
    width = across + 128
    tiles = width // 128
    off = 16
    span = height + 32
    f4, u4, v4 = halo_tiles(right_ref[...], left_ref[0 : height + 16])
    for buf, own, halo, start, count in ((f0, f_ref, f4, 0, 9), (us, u_ref, u4, 9, 6), (vs, v_ref, v4, 15, 6)):
        for j in range(tiles):
            sl = slice(128 * j, 128 * j + 128)
            top = span * j + off
            if j < tiles - 1:
                buf[top : top + height, :] = own[:, sl]
                buf[top + height : top + height + count, :] = below_ref[start : start + count, sl]
            else:
                buf[top : top + height + 16, :] = halo
            buf[top - count : top, :] = above_ref[start : start + count, sl]

    lane = lax.broadcasted_iota(jnp.int32, (8, 128), 1)

    def stage(src, dst_tiles, base, write):
        rolled = {}

        def shifted(tag, tiles_in, k):
            key = (tag, k)
            if key not in rolled:
                turned = [pltpu.roll(t, (-k) % 128, 1) for t in tiles_in]
                out = []
                for j in range(tiles):
                    if k > 0:
                        out.append(jnp.where(lane < 128 - k, turned[j], turned[(j + 1) % tiles]))
                    else:
                        out.append(jnp.where(lane >= -k, turned[j], turned[(j - 1) % tiles]))
                rolled[key] = out
            return rolled[key]

        f = [src[pl.ds(span * j + base, 8), :] for j in range(tiles)]
        nxt = shifted("f", f, 1)
        d3 = [nxt[j] - f[j] for j in range(tiles)]
        d2 = shifted("d", d3, -1)
        e2 = [d2[j] - d3[j] for j in range(tiles)]
        e0 = shifted("e", e2, -2)
        e1 = shifted("e", e2, -1)
        e3 = shifted("e", e2, 1)
        e4 = shifted("e", e2, 2)
        for j in range(dst_tiles):
            at = span * j + base
            u = us[pl.ds(at, 8), :]
            v = vs[pl.ds(at, 8), :]
            x_term = side_term(u, e0[j], e1[j], e2[j], e3[j], e4[j], d2[j], d3[j])
            rows = [f[j] if k == 0 else src[pl.ds(at + k, 8), :] for k in range(-3, 4)]
            d = [rows[k + 1] - rows[k] for k in range(6)]
            e = [d[k] - d[k + 1] for k in range(5)]
            y_term = side_term(v, e[0], e[1], e[2], e[3], e[4], d[2], d[3])
            write(j, f[j] - DT * (x_term + y_term))

    def first(i, carry):
        base = pl.multiple_of(i * 8 + 8, 8)

        def write(j, value):
            f1[pl.ds(span * j + base, 8), :] = value

        stage(f0, tiles, base, write)
        return carry

    def second(i, carry):
        base = pl.multiple_of(i * 8 + 8, 8)

        def write(j, value):
            at = pl.ds(span * j + base, 8)
            f2[at, :] = 0.75 * f0[at, :] + 0.25 * value

        stage(f1, tiles, base, write)
        return carry

    def third(i, carry):
        base = pl.multiple_of(i * 8 + 16, 8)
        place = pl.multiple_of(i * 8, 8)

        def write(j, value):
            kept = f0[pl.ds(span * j + base, 8), :]
            out_ref[pl.ds(place, 8), 128 * j : 128 * j + 128] = kept * (1.0 / 3.0) + (2.0 / 3.0) * value

        stage(f2, tiles - 1, base, write)
        return carry

    lax.fori_loop(0, height // 8 + 2, first, 0)
    lax.fori_loop(0, height // 8 + 2, second, 0)
    lax.fori_loop(0, height // 8, third, 0)


def deposit_body(recv_ref, base_ref, out_ref, moved_ref):
    height, across = base_ref.shape
    step = 4 * CAP + 1
    bands = recv_ref.shape[0] // step
    block = 4 * CAP
    for g in range(bands):
        moved_ref[block * g : block * g + block] = recv_ref[step * g : step * g + block]
    table = recv_ref[pl.ds(block, bands, stride=step), :]
    lanes = iota((bands, across), 1)
    lane = iota((bands, 128), 1)
    rows = iota((height, bands), 0)
    total = jnp.zeros((height, 2 * across), F32)
    side = jnp.zeros((height, 128), F32)
    first_row = jnp.zeros((bands, across), F32)
    corner = jnp.zeros((bands, 1), F32)

    def two(x):
        hi = x.astype(BF16)
        return hi, (x - hi.astype(F32)).astype(BF16)

    for k in range(CAP):
        o = 16 * k
        part = [table[:, o + i : o + i + 1] for i in range(11)]
        row, col, ll, hl, lh, hh = part[0:6]
        at0 = lanes == col
        at1 = lanes == col + 1.0
        spread = jnp.concatenate(
            [
                jnp.where(at0, ll, 0.0) + jnp.where(at1, lh, 0.0),
                jnp.where(at0, hl, 0.0) + jnp.where(at1, hh, 0.0),
            ],
            axis=1,
        )
        pick = one_hot(rows == to_row(row, bands))
        hi, lo = two(spread)
        total = total + (mm(pick, hi) + mm(pick, lo))
        pick = one_hot(rows == to_row(part[8], bands))
        values = jnp.where(lane == 0.0, part[9], jnp.where(lane == 1.0, part[10], 0.0))
        hi, lo = two(values)
        side = side + (mm(pick, hi) + mm(pick, lo))
        o = 64 + 16 * k
        part = [table[:, o + i : o + i + 1] for i in range(11)]
        row, col, ll, hl, lh, hh = part[0:6]
        edge = row == float(height - 1)
        first_row = (
            first_row
            + jnp.where((lanes == col) & edge, hl, 0.0)
            + jnp.where((lanes == col + 1.0) & edge, hh, 0.0)
        )
        corner = corner + jnp.where(part[8] == float(height - 1), part[10], 0.0)
    same = total[:, 0:across]
    down = pltpu.roll(total[:, across:], 1, 0)
    side_down = pltpu.roll(side, 1, 0)
    r = iota((height, across), 0)
    c = iota((height, across), 1)
    incoming = jnp.sum(first_row, axis=0, keepdims=True)
    incoming = incoming + jnp.where(iota((1, across), 1) == 0.0, jnp.sum(corner), 0.0)
    down = jnp.where(r == 0.0, incoming, down)
    column = side[:, 0:1] + jnp.where(iota((height, 1), 0) == 0.0, 0.0, side_down[:, 1:2])
    out_ref[...] = base_ref[...] + (same + down + jnp.where(c == 0.0, column, 0.0))


def ring(axis, distance):
    n = lax.axis_size(axis)
    return [(i, (i + distance) % n) for i in range(n)]


def shards(level_set, velocity, particles, escaped, home_cell, land_cell, dest_rank, block_count):
    height, across = level_set.shape
    n = particles.shape[0]
    bands = lax.axis_size("gy")
    step = 4 * CAP + 1
    sds = jax.ShapeDtypeStruct
    u, v = velocity[0], velocity[1]
    head = jnp.concatenate([level_set[0:9], u[0:6], v[0:6], jnp.zeros((3, across), F32)], axis=0)
    below = lax.ppermute(head, "gy", ring("gy", -1))
    x, y, radius = particles[:, 0, :], particles[:, 1, :], particles[:, 2, :]
    ints = jnp.stack([home_cell, land_cell, dest_rank], axis=0)
    meta, weight, select = call(
        prepare_body,
        (sds((n, 128), F32), sds((n, 128), F32), sds((bands * step, 4 * n), BF16)),
        u, v, radius, escaped, ints, block_count.reshape(1, 1),
    )
    to_left, to_right, meta = call(
        edges_body,
        (sds((height + 16, 128), F32), sds((height + 16 + 3 * n, 128), F32), sds((n, 128), F32)),
        level_set, u, v, below, meta, x, y, weight,
    )
    from_right = lax.ppermute(to_left, "gx", ring("gx", -1))
    from_left = lax.ppermute(to_right, "gx", ring("gx", 1))
    packed, tail = call(
        pack_body,
        (sds((bands * step, 128), F32), sds((24, across + 128), F32)),
        level_set, u, v, x, y, radius, weight, meta, to_left, from_left, from_right, select,
    )
    arrived = lax.all_to_all(
        packed.reshape(bands * step, 1, 128), "gy", split_axis=0, concat_axis=0, tiled=True
    ).reshape(bands * step, 128)
    above = lax.ppermute(tail, "gy", ring("gy", 1))
    wide = pltpu.VMEM(((across // 128 + 1) * (height + 32), 128), F32)
    (section,) = call(
        stencil_body,
        (sds((height, across), F32),),
        level_set, u, v, below, from_right, from_left, above,
        scratch=[wide] * 5,
    )
    level, moved = call(
        deposit_body,
        (sds((height, across), F32), sds((bands * CAP * 4, 128), F32)),
        arrived, section,
    )
    return level, moved.reshape(bands * CAP, 4, 128)


def solution(mesh):
    in_specs = (
        P("gy", "gx"),
        P(None, "gy", "gx"),
        P(("gy", "gx"), None, None),
        P(("gy", "gx"), None),
        P(("gy", "gx")),
        P(("gy", "gx")),
        P(("gy", "gx")),
        P(("gy", "gx")),
    )
    out_specs = (P("gy", "gx"), P(("gy", "gx"), None, None))
    return jax.shard_map(shards, mesh=mesh, in_specs=in_specs, out_specs=out_specs, check_vma=False)
```

```python
import functools
import jax
import jax.numpy as jnp
from jax import lax
from jax.experimental import pallas as pl
from jax.experimental.pallas import tpu as pltpu
from jax.sharding import PartitionSpec as P

CAP = 4
DT = 0.3
INTERPRET = False
F32 = jnp.float32
BF16 = jnp.bfloat16


def iota(shape, dim):
    return lax.broadcasted_iota(jnp.int32, shape, dim).astype(F32)


def split3(x):
    hi = x.astype(BF16)
    rest = x - hi.astype(F32)
    mid = rest.astype(BF16)
    lo = (rest - mid.astype(F32)).astype(BF16)
    return hi, mid, lo


def mm(a, b):
    return lax.dot_general(a, b, (((1,), (0,)), ((), ())), preferred_element_type=F32)


def exact_pick(one_hot, x):
    hi, mid, lo = split3(x)
    return (mm(one_hot, hi) + mm(one_hot, mid)) + mm(one_hot, lo)


def eye(n):
    return iota((n, n), 0) == iota((n, n), 1)


def to_column(row, n):
    return jnp.sum(jnp.where(eye(n), jnp.broadcast_to(row, (n, n)), 0.0), axis=1, keepdims=True)


def to_row(col, n):
    return jnp.sum(jnp.where(eye(n), jnp.broadcast_to(col, (n, n)), 0.0), axis=0, keepdims=True)


def one_hot(mask):
    return jnp.where(mask, 1.0, 0.0).astype(BF16)


def floor_div(x, k):
    return jnp.floor((x + 0.5) * (1.0 / k))


def call(body, outs, *args, scratch=(), scalars=()):
    vm = pl.BlockSpec(memory_space=pltpu.VMEM)
    sm = pl.BlockSpec(memory_space=pltpu.SMEM)
    return pl.pallas_call(
        body,
        out_shape=tuple(outs),
        in_specs=[sm] * len(scalars) + [vm] * len(args),
        out_specs=tuple(vm for _ in outs),
        scratch_shapes=list(scratch),
        compiler_params=pltpu.CompilerParams(vmem_limit_bytes=16 * 1024 * 1024),
        interpret=INTERPRET,
    )(*scalars, *args)


def prepare_body(count_ref, flow_ref, part_ref, esc_ref, home_ref, land_ref, dest_ref, meta_ref, w_ref, sel_ref):
    n = esc_ref.shape[0]
    height, across = flow_ref.shape[1:]
    home = to_column(home_ref[...].astype(F32), n)
    land = to_column(land_ref[...].astype(F32), n)
    dest_row = dest_ref[...].astype(F32)
    dest = to_column(dest_row, n)
    count = count_ref[0].astype(F32)
    row = floor_div(home, across)
    col = home - row * across
    land_row = floor_div(land, across)
    land_col = land - land_row * across
    other = iota((n, n), 0)
    mine = iota((n, n), 1)
    same = (dest == dest_row) & (other < mine) & (other < count)
    rank_row = jnp.sum(jnp.where(same, 1.0, 0.0), axis=0, keepdims=True)
    live_row = iota((1, n), 1) < count
    slot_row = jnp.where(live_row, dest_row * CAP + rank_row, -1.0)
    slot = to_column(slot_row, n)
    lane = iota((n, height), 1)
    pick = jnp.concatenate([one_hot(lane == row), one_hot(lane == row + 1.0)], axis=0)
    lanes = iota((n, across), 1)
    at0 = lanes == col
    at1 = lanes == col + 1.0
    parts = []
    for component in range(2):
        both = exact_pick(pick, flow_ref[component])
        low = both[0:n]
        high = both[n:]
        for where_at in (at0, at1):
            for rows in (low, high):
                parts.append(jnp.sum(jnp.where(where_at, rows, 0.0), axis=1, keepdims=True))
    columns = parts + [row, col, land_row, land_col, slot]
    lane = iota((n, 128), 1)
    meta = jnp.zeros((n, 128), F32)
    for i, value in enumerate(columns):
        meta = jnp.where(lane == float(i), value, meta)
    meta_ref[...] = meta
    w_ref[...] = esc_ref[...].astype(F32) * part_ref[2]
    total = sel_ref.shape[0]
    step = 4 * CAP + 1
    r = iota((total, 1), 0)
    d = floor_div(r, step)
    q = r - d * step
    code = jnp.where(q < 4.0 * CAP, d * (4.0 * CAP) + q, -1000.0)
    slots = jnp.concatenate([slot_row * 4.0 + float(j) for j in range(4)], axis=1)
    slots = jnp.where(jnp.concatenate([slot_row] * 4, axis=1) < 0.0, -1.0, slots)
    sel_ref[...] = one_hot(code == slots)


def edges_body(f_ref, flow_ref, below_ref, above_ref, meta_ref, part_ref, w_ref, left_ref, right_ref, meta2_ref):
    n = w_ref.shape[0]
    height, across = f_ref.shape
    meta = meta_ref[...]
    lane = iota((n, 128), 1)
    row = meta[:, 8:9]
    col = meta[:, 9:10]
    last = row == float(height - 1)
    lanes = iota((n, across), 1)
    at0 = (lanes == col) & last
    at1 = (lanes == col + 1.0) & last
    for base, r in ((0, 9), (4, 15)):
        line = jnp.broadcast_to(below_ref[r : r + 1, :], (n, across))
        c10 = jnp.sum(jnp.where(at0, line, 0.0), axis=1, keepdims=True)
        c11 = jnp.sum(jnp.where(at1, line, 0.0), axis=1, keepdims=True)
        meta = meta + jnp.where(lane == float(base + 1), c10, 0.0) + jnp.where(lane == float(base + 3), c11, 0.0)
    meta2_ref[...] = meta
    far = across - 128

    def pack_left(f, u, v):
        lane = iota(f.shape, 1)
        return jnp.where(lane < 16.0, f, jnp.where(lane < 32.0, pltpu.roll(u, 16, 1), pltpu.roll(v, 32, 1)))

    def pack_right(f, u, v, m):
        lane = iota(f.shape, 1)
        out = jnp.where(
            lane >= 112.0, f, jnp.where(lane >= 96.0, pltpu.roll(u, 112, 1), pltpu.roll(v, 96, 1))
        )
        return jnp.where(lane < 16.0, m, out)

    zero = jnp.zeros((8, 128), F32)

    def pieces(sl):
        yield 0, height, f_ref[:, sl], flow_ref[0, :, sl], flow_ref[1, :, sl], meta
        for top, ref in ((height, below_ref), (height + 16, above_ref)):
            yield top, 8, ref[0:8, sl], ref[9:17, sl], ref[15:23, sl], zero
            yield top + 8, 8, ref[8:16, sl], zero, zero, zero

    for top, rows, f, u, v, _ in pieces(slice(0, 128)):
        left_ref[top : top + rows] = pack_left(f, u, v)
    for top, rows, f, u, v, m in pieces(slice(far, across)):
        right_ref[top : top + rows] = pack_right(f, u, v, m)
    top = height + 32
    right_ref[top : top + n] = part_ref[0]
    right_ref[top + n : top + 2 * n] = part_ref[1]
    right_ref[top + 2 * n : top + 3 * n] = w_ref[...]


def halo_tiles(from_right, from_left):
    lane = iota(from_right.shape, 1)
    right_side = lane < 64.0
    f = jnp.where(right_side, from_right, from_left)
    u = jnp.where(right_side, pltpu.roll(from_right, 112, 1), pltpu.roll(from_left, 16, 1))
    v = jnp.where(right_side, pltpu.roll(from_right, 96, 1), pltpu.roll(from_left, 32, 1))
    return f, u, v


def moved_particles(meta, x, y, column, across):
    n = x.shape[0]
    row = meta[:, 8:9]
    last = meta[:, 9:10] == float(across - 1)
    lane = iota((n, column.shape[0]), 1)
    pick = jnp.concatenate([one_hot((lane == row) & last), one_hot((lane == row + 1.0) & last)], axis=0)
    both = exact_pick(pick, column)
    low = both[0:n]
    high = both[n:]
    u = [meta[:, 0:1], meta[:, 1:2], meta[:, 2:3] + low[:, 16:17], meta[:, 3:4] + high[:, 16:17]]
    v = [meta[:, 4:5], meta[:, 5:6], meta[:, 6:7] + low[:, 32:33], meta[:, 7:8] + high[:, 32:33]]
    fy = y + 0.5
    fx = x + 0.5
    w00 = (1.0 - fy) * (1.0 - fx)
    w10 = fy * (1.0 - fx)
    w01 = (1.0 - fy) * fx
    w11 = fy * fx
    new_x = x + DT * (w00 * u[0] + w10 * u[1] + w01 * u[2] + w11 * u[3])
    new_y = y + DT * (w00 * v[0] + w10 * v[1] + w01 * v[2] + w11 * v[3])
    return new_x, new_y


def lane_sum(x):
    return jnp.sum(x, axis=1, keepdims=True)


def pack_body(part_ref, w_ref, meta_ref, mine_ref, left_ref, right_ref, sel_ref, out_ref, height, across):
    n = w_ref.shape[0]
    bands = out_ref.shape[0] // (4 * CAP + 1)
    meta = meta_ref[...]
    top = height + 32
    w = w_ref[...]
    new_x, new_y = moved_particles(meta, part_ref[0], part_ref[1], right_ref[0 : height + 16], across)
    left_meta = left_ref[0:n]
    left_w = left_ref[top + 2 * n : top + 3 * n]
    left_x, left_y = moved_particles(
        left_meta, left_ref[top : top + n], left_ref[top + n : top + 2 * n], mine_ref[0 : height + 16], across
    )
    body = jnp.concatenate([new_x, new_y, part_ref[2], w], axis=0)
    out_ref[...] = exact_pick(sel_ref[...], body)
    gy = new_y + 0.5
    gx = new_x + 0.5
    sums = [
        meta[:, 10:11],
        meta[:, 11:12],
        lane_sum(w * (1.0 - gy) * (1.0 - gx)),
        lane_sum(w * gy * (1.0 - gx)),
        lane_sum(w * (1.0 - gy) * gx),
        lane_sum(w * gy * gx),
    ]
    lane = iota((n, 128), 1)
    lane16 = lane - 16.0 * jnp.floor(lane * 0.0625)
    mine = jnp.zeros((n, 128), F32)
    for i, value in enumerate(sums):
        mine = jnp.where(lane16 == float(i), value, mine)
    gy = left_y + 0.5
    gx = left_x + 0.5
    over = left_meta[:, 11:12] == float(across - 1)
    sums = [
        left_meta[:, 10:11],
        jnp.where(over, lane_sum(left_w * (1.0 - gy) * gx), 0.0),
        jnp.where(over, lane_sum(left_w * gy * gx), 0.0),
    ]
    theirs = jnp.zeros((n, 128), F32)
    for i, value in enumerate(sums):
        theirs = jnp.where(lane16 == float(8 + i), value, theirs)
    values = jnp.concatenate([mine, theirs], axis=0)
    slot = jnp.concatenate([to_row(meta[:, 12:13], n), to_row(left_meta[:, 12:13], n)], axis=1)
    d4 = iota((bands, 2 * n), 0) * float(CAP)
    choose = jnp.concatenate([one_hot(d4 + float(k) == slot) for k in range(CAP)], axis=0)
    chosen = exact_pick(choose, values)
    lane = iota((bands, 128), 1)
    group = jnp.floor(lane * 0.0625)
    table = jnp.zeros((bands, 128), F32)
    for k in range(CAP):
        table = jnp.where(group == float(k), chosen[k * bands : (k + 1) * bands], table)
    table = table + pltpu.roll(pltpu.roll(table, 1, 0), 64, 1)
    step = 4 * CAP + 1
    out_ref[pl.ds(4 * CAP, bands, stride=step), :] = table

def side_term(speed, e0, e1, e2, e3, e4, d2, d3):
    ahead = speed > 0.0
    p = jnp.where(ahead, e0, e4)
    q = jnp.where(ahead, e1, e3)
    s = jnp.where(ahead, e3, e1)
    c = jnp.where(ahead, d2, d3)
    r = e2
    rr = r * r
    t1 = p * (4.0 * p - 11.0 * q) + (10.0 * (q * q) + 3e-6)
    t2 = q * (4.0 * q - 5.0 * r) + (4.0 * rr + 3e-6)
    t3 = s * (4.0 * s - 11.0 * r) + (10.0 * rr + 3e-6)
    a1 = t2 * t3
    a2 = t1 * t3
    a3 = t1 * t2
    w1 = a1 * a1
    w2 = 6.0 * (a2 * a2)
    w3 = 3.0 * (a3 * a3)
    top = w1 * (2.0 * p - 5.0 * q) - w2 * (q + 2.0 * r) + w3 * (s - 4.0 * r)
    return speed * c + jnp.abs(speed) * (top / (6.0 * (w1 + w2 + w3)))


def stencil_body(f_ref, flow_ref, below_ref, above_ref, right_ref, left_ref, out_ref, f0, us, vs, f1, f2):
    height, across = f_ref.shape
    width = across + 128
    tiles = width // 128
    off = 16
    span = height + 32
    f4, u4, v4 = halo_tiles(right_ref[...], left_ref[0 : height + 32])
    fields = ((f0, f_ref, f4, 0, 9), (us, flow_ref.at[0], u4, 9, 6), (vs, flow_ref.at[1], v4, 15, 6))
    for buf, own, halo, start, count in fields:
        for j in range(tiles):
            sl = slice(128 * j, 128 * j + 128)
            top = span * j + off
            if j < tiles - 1:
                buf[top : top + height, :] = own[:, sl]
                buf[top + height : top + height + count, :] = below_ref[start : start + count, sl]
                buf[top - count : top, :] = above_ref[start : start + count, sl]
            else:
                buf[top : top + height + count, :] = halo[0 : height + count]
                buf[top - count : top, :] = halo[height + 16 : height + 16 + count]

    lane = lax.broadcasted_iota(jnp.int32, (8, 128), 1)

    def stage(src, dst_tiles, base, write):
        rolled = {}

        def shifted(tag, tiles_in, k):
            key = (tag, k)
            if key not in rolled:
                turned = [pltpu.roll(t, (-k) % 128, 1) for t in tiles_in]
                out = []
                for j in range(tiles):
                    if k > 0:
                        out.append(jnp.where(lane < 128 - k, turned[j], turned[(j + 1) % tiles]))
                    else:
                        out.append(jnp.where(lane >= -k, turned[j], turned[(j - 1) % tiles]))
                rolled[key] = out
            return rolled[key]

        f = [src[pl.ds(span * j + base, 8), :] for j in range(tiles)]
        nxt = shifted("f", f, 1)
        d3 = [nxt[j] - f[j] for j in range(tiles)]
        d2 = shifted("d", d3, -1)
        e2 = [d2[j] - d3[j] for j in range(tiles)]
        e0 = shifted("e", e2, -2)
        e1 = shifted("e", e2, -1)
        e3 = shifted("e", e2, 1)
        e4 = shifted("e", e2, 2)
        for j in range(dst_tiles):
            at = span * j + base
            u = us[pl.ds(at, 8), :]
            v = vs[pl.ds(at, 8), :]
            x_term = side_term(u, e0[j], e1[j], e2[j], e3[j], e4[j], d2[j], d3[j])
            rows = [f[j] if k == 0 else src[pl.ds(at + k, 8), :] for k in range(-3, 4)]
            d = [rows[k + 1] - rows[k] for k in range(6)]
            e = [d[k] - d[k + 1] for k in range(5)]
            y_term = side_term(v, e[0], e[1], e[2], e[3], e[4], d[2], d[3])
            write(j, f[j] - DT * (x_term + y_term))

    def first(i, carry):
        base = pl.multiple_of(i * 8 + 8, 8)

        def write(j, value):
            f1[pl.ds(span * j + base, 8), :] = value

        stage(f0, tiles, base, write)
        return carry

    def second(i, carry):
        base = pl.multiple_of(i * 8 + 8, 8)

        def write(j, value):
            at = pl.ds(span * j + base, 8)
            f2[at, :] = 0.75 * f0[at, :] + 0.25 * value

        stage(f1, tiles, base, write)
        return carry

    def third(i, carry):
        base = pl.multiple_of(i * 8 + 16, 8)
        place = pl.multiple_of(i * 8, 8)

        def write(j, value):
            kept = f0[pl.ds(span * j + base, 8), :]
            out_ref[pl.ds(place, 8), 128 * j : 128 * j + 128] = kept * (1.0 / 3.0) + (2.0 / 3.0) * value

        stage(f2, tiles - 1, base, write)
        return carry

    lax.fori_loop(0, height // 8 + 2, first, 0)
    lax.fori_loop(0, height // 8 + 2, second, 0)
    lax.fori_loop(0, height // 8, third, 0)


def deposit_body(recv_ref, base_ref, out_ref, moved_ref):
    height, across = base_ref.shape
    step = 4 * CAP + 1
    bands = recv_ref.shape[0] // step
    block = 4 * CAP
    for g in range(bands):
        moved_ref[block * g : block * g + block] = recv_ref[step * g : step * g + block]
    table = recv_ref[pl.ds(block, bands, stride=step), :]
    lanes = iota((bands, across), 1)
    lane = iota((bands, 128), 1)
    rows = iota((height, bands), 0)
    total = jnp.zeros((height, 2 * across), F32)
    side = jnp.zeros((height, 128), F32)
    first_row = jnp.zeros((bands, across), F32)
    corner = jnp.zeros((bands, 1), F32)

    def two(x):
        hi = x.astype(BF16)
        return hi, (x - hi.astype(F32)).astype(BF16)

    for k in range(CAP):
        o = 16 * k
        part = [table[:, o + i : o + i + 1] for i in range(11)]
        row, col, ll, hl, lh, hh = part[0:6]
        at0 = lanes == col
        at1 = lanes == col + 1.0
        spread = jnp.concatenate(
            [
                jnp.where(at0, ll, 0.0) + jnp.where(at1, lh, 0.0),
                jnp.where(at0, hl, 0.0) + jnp.where(at1, hh, 0.0),
            ],
            axis=1,
        )
        pick = one_hot(rows == to_row(row, bands))
        hi, lo = two(spread)
        total = total + (mm(pick, hi) + mm(pick, lo))
        pick = one_hot(rows == to_row(part[8], bands))
        values = jnp.where(lane == 0.0, part[9], jnp.where(lane == 1.0, part[10], 0.0))
        hi, lo = two(values)
        side = side + (mm(pick, hi) + mm(pick, lo))
        o = 64 + 16 * k
        part = [table[:, o + i : o + i + 1] for i in range(11)]
        row, col, ll, hl, lh, hh = part[0:6]
        edge = row == float(height - 1)
        first_row = (
            first_row
            + jnp.where((lanes == col) & edge, hl, 0.0)
            + jnp.where((lanes == col + 1.0) & edge, hh, 0.0)
        )
        corner = corner + jnp.where(part[8] == float(height - 1), part[10], 0.0)
    same = total[:, 0:across]
    down = pltpu.roll(total[:, across:], 1, 0)
    side_down = pltpu.roll(side, 1, 0)
    r = iota((height, across), 0)
    c = iota((height, across), 1)
    incoming = jnp.sum(first_row, axis=0, keepdims=True)
    incoming = incoming + jnp.where(iota((1, across), 1) == 0.0, jnp.sum(corner), 0.0)
    down = jnp.where(r == 0.0, incoming, down)
    column = side[:, 0:1] + jnp.where(iota((height, 1), 0) == 0.0, 0.0, side_down[:, 1:2])
    out_ref[...] = base_ref[...] + (same + down + jnp.where(c == 0.0, column, 0.0))


def ring(axis, distance):
    n = lax.axis_size(axis)
    return [(i, (i + distance) % n) for i in range(n)]


def shards(level_set, velocity, particles, escaped, home_cell, land_cell, dest_rank, block_count):
    height, across = level_set.shape
    n = particles.shape[0]
    bands = lax.axis_size("gy")
    step = 4 * CAP + 1
    sds = jax.ShapeDtypeStruct
    u, v = velocity[0], velocity[1]
    pad = jnp.zeros((3, across), F32)
    head = jnp.concatenate([level_set[:9], u[:6], v[:6], pad], axis=0)
    tail = jnp.concatenate([level_set[-9:], u[-6:], v[-6:], pad], axis=0)
    below = lax.ppermute(head, "gy", ring("gy", -1))
    above = lax.ppermute(tail, "gy", ring("gy", 1))
    parts = jnp.transpose(particles, (1, 0, 2))
    meta, weight, select = call(
        prepare_body,
        (sds((n, 128), F32), sds((n, 128), F32), sds((bands * step, 4 * n), BF16)),
        velocity, parts, escaped, home_cell.reshape(1, n), land_cell.reshape(1, n), dest_rank.reshape(1, n),
        scalars=(block_count,),
    )
    to_left, to_right, meta = call(
        edges_body,
        (sds((height + 32, 128), F32), sds((height + 32 + 3 * n, 128), F32), sds((n, 128), F32)),
        level_set, velocity, below, above, meta, parts, weight,
    )
    from_right = lax.ppermute(to_left, "gx", ring("gx", -1))
    from_left = lax.ppermute(to_right, "gx", ring("gx", 1))
    (packed,) = call(
        functools.partial(pack_body, height=height, across=across),
        (sds((bands * step, 128), F32),),
        parts, weight, meta, to_left, from_left, from_right, select,
    )
    arrived = lax.all_to_all(
        packed.reshape(bands * step, 1, 128), "gy", split_axis=0, concat_axis=0, tiled=True
    ).reshape(bands * step, 128)
    wide = pltpu.VMEM(((across // 128 + 1) * (height + 32), 128), F32)
    (section,) = call(
        stencil_body,
        (sds((height, across), F32),),
        level_set, velocity, below, above, from_right, from_left,
        scratch=[wide] * 5,
    )
    level, moved = call(
        deposit_body,
        (sds((height, across), F32), sds((bands * CAP * 4, 128), F32)),
        arrived, section,
    )
    return level, moved.reshape(bands * CAP, 4, 128)


def solution(mesh):
    in_specs = (
        P("gy", "gx"),
        P(None, "gy", "gx"),
        P(("gy", "gx"), None, None),
        P(("gy", "gx"), None),
        P(("gy", "gx")),
        P(("gy", "gx")),
        P(("gy", "gx")),
        P(("gy", "gx")),
    )
    out_specs = (P("gy", "gx"), P(("gy", "gx"), None, None))
    return jax.shard_map(shards, mesh=mesh, in_specs=in_specs, out_specs=out_specs, check_vma=False)
```

```python
import functools
import jax
import jax.numpy as jnp
from jax import lax
from jax.experimental import pallas as pl
from jax.experimental.pallas import tpu as pltpu
from jax.sharding import PartitionSpec as P

CAP = 4
DT = 0.3
INTERPRET = False
F32 = jnp.float32
BF16 = jnp.bfloat16


def iota(shape, dim):
    return lax.broadcasted_iota(jnp.int32, shape, dim).astype(F32)


def split3(x):
    hi = x.astype(BF16)
    rest = x - hi.astype(F32)
    mid = rest.astype(BF16)
    lo = (rest - mid.astype(F32)).astype(BF16)
    return hi, mid, lo


def mm(a, b):
    return lax.dot_general(a, b, (((1,), (0,)), ((), ())), preferred_element_type=F32)


def exact_pick(one_hot, x):
    hi, mid, lo = split3(x)
    return (mm(one_hot, hi) + mm(one_hot, mid)) + mm(one_hot, lo)


def eye(n):
    return iota((n, n), 0) == iota((n, n), 1)


def to_column(row, n):
    return jnp.sum(jnp.where(eye(n), jnp.broadcast_to(row, (n, n)), 0.0), axis=1, keepdims=True)


def to_row(col, n):
    return jnp.sum(jnp.where(eye(n), jnp.broadcast_to(col, (n, n)), 0.0), axis=0, keepdims=True)


def one_hot(mask):
    return jnp.where(mask, 1.0, 0.0).astype(BF16)


def floor_div(x, k):
    return jnp.floor((x + 0.5) * (1.0 / k))


def call(body, outs, *args, scratch=(), scalars=()):
    vm = pl.BlockSpec(memory_space=pltpu.VMEM)
    sm = pl.BlockSpec(memory_space=pltpu.SMEM)
    return pl.pallas_call(
        body,
        out_shape=tuple(outs),
        in_specs=[sm] * len(scalars) + [vm] * len(args),
        out_specs=tuple(vm for _ in outs),
        scratch_shapes=list(scratch),
        compiler_params=pltpu.CompilerParams(vmem_limit_bytes=16 * 1024 * 1024),
        interpret=INTERPRET,
    )(*scalars, *args)


def heads_body(f_ref, flow_ref, head_ref, tail_ref):
    height = f_ref.shape[0]
    for ref, f0, v0 in ((head_ref, 0, 0), (tail_ref, height - 9, height - 6)):
        ref[0:9] = f_ref[f0 : f0 + 9]
        ref[9:15] = flow_ref[0, v0 : v0 + 6]
        ref[15:21] = flow_ref[1, v0 : v0 + 6]
        ref[21:24] = jnp.zeros((3, f_ref.shape[1]), F32)


def prepare_body(count_ref, flow_ref, part_ref, esc_ref, home_ref, land_ref, dest_ref, meta_ref, w_ref, sel_ref, rw_ref):
    n = esc_ref.shape[0]
    height, across = flow_ref.shape[1:]
    home = to_column(home_ref[...].astype(F32), n)
    land = to_column(land_ref[...].astype(F32), n)
    dest_row = dest_ref[...].astype(F32)
    dest = to_column(dest_row, n)
    count = count_ref[0].astype(F32)
    row = floor_div(home, across)
    col = home - row * across
    land_row = floor_div(land, across)
    land_col = land - land_row * across
    other = iota((n, n), 0)
    mine = iota((n, n), 1)
    same = (dest == dest_row) & (other < mine) & (other < count)
    rank_row = jnp.sum(jnp.where(same, 1.0, 0.0), axis=0, keepdims=True)
    live_row = iota((1, n), 1) < count
    slot_row = jnp.where(live_row, dest_row * CAP + rank_row, -1.0)
    slot = to_column(slot_row, n)
    lane = iota((n, height), 1)
    pick = jnp.concatenate([one_hot(lane == row), one_hot(lane == row + 1.0)], axis=0)
    lanes = iota((n, across), 1)
    at0 = lanes == col
    at1 = lanes == col + 1.0
    parts = []
    for component in range(2):
        both = exact_pick(pick, flow_ref[component])
        low = both[0:n]
        high = both[n:]
        for where_at in (at0, at1):
            for rows in (low, high):
                parts.append(jnp.sum(jnp.where(where_at, rows, 0.0), axis=1, keepdims=True))
    columns = parts + [row, col, land_row, land_col, slot]
    lane = iota((n, 128), 1)
    meta = jnp.zeros((n, 128), F32)
    for i, value in enumerate(columns):
        meta = jnp.where(lane == float(i), value, meta)
    meta_ref[...] = meta
    w = esc_ref[...].astype(F32) * part_ref[2]
    w_ref[...] = w
    slots = sel_ref.shape[0]
    bands = slots // CAP
    r = iota((slots, 1), 0)
    k = floor_div(r, bands)
    choose = one_hot((r - k * bands) * CAP + k == slot_row)
    sel_ref[...] = choose
    rw_ref[...] = exact_pick(choose, jnp.concatenate([part_ref[2], w], axis=1))


def pack_left(f, u, v):
    lane = iota(f.shape, 1)
    return jnp.where(lane < 16.0, f, jnp.where(lane < 32.0, pltpu.roll(u, 16, 1), pltpu.roll(v, 32, 1)))


def pack_right(f, u, v, m):
    lane = iota(f.shape, 1)
    out = jnp.where(lane >= 112.0, f, jnp.where(lane >= 96.0, pltpu.roll(u, 112, 1), pltpu.roll(v, 96, 1)))
    return jnp.where(lane < 16.0, m, out)


def corners_body(above_ref, left_ref, right_ref):
    across = above_ref.shape[1]
    zero = jnp.zeros((8, 128), F32)
    near, far = slice(0, 128), slice(across - 128, across)
    left_ref[0:8] = pack_left(above_ref[0:8, near], above_ref[9:17, near], above_ref[15:23, near])
    left_ref[8:16] = pack_left(above_ref[8:16, near], zero, zero)
    right_ref[0:8] = pack_right(above_ref[0:8, far], above_ref[9:17, far], above_ref[15:23, far], zero)
    right_ref[8:16] = pack_right(above_ref[8:16, far], zero, zero, zero)


def edges_body(f_ref, flow_ref, below_ref, meta_ref, part_ref, w_ref, left_ref, right_ref, meta2_ref):
    n = w_ref.shape[0]
    height, across = f_ref.shape
    meta = meta_ref[...]
    lane = iota((n, 128), 1)
    row = meta[:, 8:9]
    col = meta[:, 9:10]
    last = row == float(height - 1)
    lanes = iota((n, across), 1)
    at0 = (lanes == col) & last
    at1 = (lanes == col + 1.0) & last
    for base, r in ((0, 9), (4, 15)):
        line = jnp.broadcast_to(below_ref[r : r + 1, :], (n, across))
        c10 = jnp.sum(jnp.where(at0, line, 0.0), axis=1, keepdims=True)
        c11 = jnp.sum(jnp.where(at1, line, 0.0), axis=1, keepdims=True)
        meta = meta + jnp.where(lane == float(base + 1), c10, 0.0) + jnp.where(lane == float(base + 3), c11, 0.0)
    meta2_ref[...] = meta
    far = across - 128

    zero = jnp.zeros((8, 128), F32)

    def pieces(sl):
        yield 0, height, f_ref[:, sl], flow_ref[0, :, sl], flow_ref[1, :, sl], meta
        yield height, 8, below_ref[0:8, sl], below_ref[9:17, sl], below_ref[15:23, sl], zero
        yield height + 8, 8, below_ref[8:16, sl], zero, zero, zero

    for top, rows, f, u, v, _ in pieces(slice(0, 128)):
        left_ref[top : top + rows] = pack_left(f, u, v)
    for top, rows, f, u, v, m in pieces(slice(far, across)):
        right_ref[top : top + rows] = pack_right(f, u, v, m)
    top = height + 16
    right_ref[top : top + n] = part_ref[0]
    right_ref[top + n : top + 2 * n] = part_ref[1]
    right_ref[top + 2 * n : top + 3 * n] = w_ref[...]


def halo_tiles(from_right, from_left):
    lane = iota(from_right.shape, 1)
    right_side = lane < 64.0
    f = jnp.where(right_side, from_right, from_left)
    u = jnp.where(right_side, pltpu.roll(from_right, 112, 1), pltpu.roll(from_left, 16, 1))
    v = jnp.where(right_side, pltpu.roll(from_right, 96, 1), pltpu.roll(from_left, 32, 1))
    return f, u, v


def moved_particles(meta, x, y, column, across):
    n = x.shape[0]
    row = meta[:, 8:9]
    last = meta[:, 9:10] == float(across - 1)
    lane = iota((n, column.shape[0]), 1)
    pick = jnp.concatenate([one_hot((lane == row) & last), one_hot((lane == row + 1.0) & last)], axis=0)
    both = exact_pick(pick, column)
    low = both[0:n]
    high = both[n:]
    u = [meta[:, 0:1], meta[:, 1:2], meta[:, 2:3] + low[:, 16:17], meta[:, 3:4] + high[:, 16:17]]
    v = [meta[:, 4:5], meta[:, 5:6], meta[:, 6:7] + low[:, 32:33], meta[:, 7:8] + high[:, 32:33]]
    fy = y + 0.5
    fx = x + 0.5
    w00 = (1.0 - fy) * (1.0 - fx)
    w10 = fy * (1.0 - fx)
    w01 = (1.0 - fy) * fx
    w11 = fy * fx
    new_x = x + DT * (w00 * u[0] + w10 * u[1] + w01 * u[2] + w11 * u[3])
    new_y = y + DT * (w00 * v[0] + w10 * v[1] + w01 * v[2] + w11 * v[3])
    return new_x, new_y


def lane_sum(x):
    return jnp.sum(x, axis=1, keepdims=True)


def pack_body(part_ref, w_ref, meta_ref, mine_ref, left_ref, right_ref, sel_ref, rw_ref, out_ref, height, across):
    n = w_ref.shape[0]
    bands = out_ref.shape[0] // (4 * CAP + 1)
    meta = meta_ref[...]
    top = height + 16
    step = 4 * CAP + 1
    w = w_ref[...]
    new_x, new_y = moved_particles(meta, part_ref[0], part_ref[1], right_ref[0 : height + 16], across)
    left_meta = left_ref[0:n]
    left_w = left_ref[top + 2 * n : top + 3 * n]
    left_x, left_y = moved_particles(
        left_meta, left_ref[top : top + n], left_ref[top + n : top + 2 * n], mine_ref[0 : height + 16], across
    )
    choose = sel_ref[...]
    xy = exact_pick(choose, jnp.concatenate([new_x, new_y], axis=1))
    for k in range(CAP):
        rows = slice(k * bands, (k + 1) * bands)
        for j, source, sl in ((0, xy, slice(0, 128)), (1, xy, slice(128, 256)), (2, rw_ref, slice(0, 128)), (3, rw_ref, slice(128, 256))):
            out_ref[pl.ds(4 * k + j, bands, stride=step), :] = source[rows, sl]
    gy = new_y + 0.5
    gx = new_x + 0.5
    sums = [
        meta[:, 10:11],
        meta[:, 11:12],
        lane_sum(w * (1.0 - gy) * (1.0 - gx)),
        lane_sum(w * gy * (1.0 - gx)),
        lane_sum(w * (1.0 - gy) * gx),
        lane_sum(w * gy * gx),
    ]
    lane = iota((n, 128), 1)
    lane16 = lane - 16.0 * jnp.floor(lane * 0.0625)
    mine = jnp.zeros((n, 128), F32)
    for i, value in enumerate(sums):
        mine = jnp.where(lane16 == float(i), value, mine)
    gy = left_y + 0.5
    gx = left_x + 0.5
    over = left_meta[:, 11:12] == float(across - 1)
    sums = [
        left_meta[:, 10:11],
        jnp.where(over, lane_sum(left_w * (1.0 - gy) * gx), 0.0),
        jnp.where(over, lane_sum(left_w * gy * gx), 0.0),
    ]
    theirs = jnp.zeros((n, 128), F32)
    for i, value in enumerate(sums):
        theirs = jnp.where(lane16 == float(8 + i), value, theirs)
    values = jnp.concatenate([mine, theirs], axis=0)
    d4 = iota((bands, n), 0) * float(CAP)
    slot = to_row(left_meta[:, 12:13], n)
    theirs_choose = jnp.concatenate([one_hot(d4 + float(k) == slot) for k in range(CAP)], axis=0)
    chosen = exact_pick(jnp.concatenate([choose, theirs_choose], axis=1), values)
    lane = iota((bands, 128), 1)
    group = jnp.floor(lane * 0.0625)
    table = jnp.zeros((bands, 128), F32)
    for k in range(CAP):
        table = jnp.where(group == float(k), chosen[k * bands : (k + 1) * bands], table)
    table = table + pltpu.roll(pltpu.roll(table, 1, 0), 64, 1)
    out_ref[pl.ds(4 * CAP, bands, stride=step), :] = table


def side_term(speed, e0, e1, e2, e3, e4, d2, d3):
    ahead = speed > 0.0
    p = jnp.where(ahead, e0, e4)
    q = jnp.where(ahead, e1, e3)
    s = jnp.where(ahead, e3, e1)
    c = jnp.where(ahead, d2, d3)
    r = e2
    rr = r * r
    t1 = p * (4.0 * p - 11.0 * q) + (10.0 * (q * q) + 3e-6)
    t2 = q * (4.0 * q - 5.0 * r) + (4.0 * rr + 3e-6)
    t3 = s * (4.0 * s - 11.0 * r) + (10.0 * rr + 3e-6)
    a1 = t2 * t3
    a2 = t1 * t3
    a3 = t1 * t2
    w1 = a1 * a1
    w2 = 6.0 * (a2 * a2)
    w3 = 3.0 * (a3 * a3)
    top = w1 * (2.0 * p - 5.0 * q) - w2 * (q + 2.0 * r) + w3 * (s - 4.0 * r)
    return speed * c + jnp.abs(speed) * (top / (6.0 * (w1 + w2 + w3)))


def stencil_body(f_ref, flow_ref, below_ref, above_ref, right_ref, left_ref, right2_ref, left2_ref, out_ref, f0, us, vs, f1, f2):
    height, across = f_ref.shape
    width = across + 128
    tiles = width // 128
    off = 16
    span = height + 32
    halos = halo_tiles(right_ref[...], left_ref[0 : height + 16])
    uppers = halo_tiles(right2_ref[...], left2_ref[...])
    owns = (f_ref, flow_ref.at[0], flow_ref.at[1])
    for buf, own, halo, upper, start, count in zip((f0, us, vs), owns, halos, uppers, (0, 9, 15), (9, 6, 6)):
        for j in range(tiles):
            sl = slice(128 * j, 128 * j + 128)
            top = span * j + off
            if j < tiles - 1:
                buf[top : top + height, :] = own[:, sl]
                buf[top + height : top + height + count, :] = below_ref[start : start + count, sl]
                buf[top - count : top, :] = above_ref[start : start + count, sl]
            else:
                buf[top : top + height + count, :] = halo[0 : height + count]
                buf[top - count : top, :] = upper[0:count]

    lane = lax.broadcasted_iota(jnp.int32, (8, 128), 1)

    def stage(src, dst_tiles, base, write):
        rolled = {}

        def shifted(tag, tiles_in, k):
            key = (tag, k)
            if key not in rolled:
                turned = [pltpu.roll(t, (-k) % 128, 1) for t in tiles_in]
                out = []
                for j in range(tiles):
                    if k > 0:
                        out.append(jnp.where(lane < 128 - k, turned[j], turned[(j + 1) % tiles]))
                    else:
                        out.append(jnp.where(lane >= -k, turned[j], turned[(j - 1) % tiles]))
                rolled[key] = out
            return rolled[key]

        f = [src[pl.ds(span * j + base, 8), :] for j in range(tiles)]
        nxt = shifted("f", f, 1)
        d3 = [nxt[j] - f[j] for j in range(tiles)]
        d2 = shifted("d", d3, -1)
        e2 = [d2[j] - d3[j] for j in range(tiles)]
        e0 = shifted("e", e2, -2)
        e1 = shifted("e", e2, -1)
        e3 = shifted("e", e2, 1)
        e4 = shifted("e", e2, 2)
        for j in range(dst_tiles):
            at = span * j + base
            u = us[pl.ds(at, 8), :]
            v = vs[pl.ds(at, 8), :]
            x_term = side_term(u, e0[j], e1[j], e2[j], e3[j], e4[j], d2[j], d3[j])
            rows = [f[j] if k == 0 else src[pl.ds(at + k, 8), :] for k in range(-3, 4)]
            d = [rows[k + 1] - rows[k] for k in range(6)]
            e = [d[k] - d[k + 1] for k in range(5)]
            y_term = side_term(v, e[0], e[1], e[2], e[3], e[4], d[2], d[3])
            write(j, f[j] - DT * (x_term + y_term))

    def first(i, carry):
        base = pl.multiple_of(i * 8 + 8, 8)

        def write(j, value):
            f1[pl.ds(span * j + base, 8), :] = value

        stage(f0, tiles, base, write)
        return carry

    def second(i, carry):
        base = pl.multiple_of(i * 8 + 8, 8)

        def write(j, value):
            at = pl.ds(span * j + base, 8)
            f2[at, :] = 0.75 * f0[at, :] + 0.25 * value

        stage(f1, tiles, base, write)
        return carry

    def third(i, carry):
        base = pl.multiple_of(i * 8 + 16, 8)
        place = pl.multiple_of(i * 8, 8)

        def write(j, value):
            kept = f0[pl.ds(span * j + base, 8), :]
            out_ref[pl.ds(place, 8), 128 * j : 128 * j + 128] = kept * (1.0 / 3.0) + (2.0 / 3.0) * value

        stage(f2, tiles - 1, base, write)
        return carry

    lax.fori_loop(0, height // 8 + 2, first, 0)
    lax.fori_loop(0, height // 8 + 2, second, 0)
    lax.fori_loop(0, height // 8, third, 0)


def deposit_body(recv_ref, base_ref, out_ref, moved_ref):
    height, across = base_ref.shape
    step = 4 * CAP + 1
    bands = recv_ref.shape[0] // step
    block = 4 * CAP
    for g in range(bands):
        moved_ref[block * g : block * g + block] = recv_ref[step * g : step * g + block]
    table = recv_ref[pl.ds(block, bands, stride=step), :]
    lanes = iota((bands, across), 1)
    lane = iota((bands, 128), 1)
    rows = iota((height, bands), 0)
    total = jnp.zeros((height, 2 * across), F32)
    side = jnp.zeros((height, 128), F32)
    first_row = jnp.zeros((bands, across), F32)
    corner = jnp.zeros((bands, 1), F32)

    def two(x):
        hi = x.astype(BF16)
        return hi, (x - hi.astype(F32)).astype(BF16)

    for k in range(CAP):
        o = 16 * k
        part = [table[:, o + i : o + i + 1] for i in range(11)]
        row, col, ll, hl, lh, hh = part[0:6]
        at0 = lanes == col
        at1 = lanes == col + 1.0
        spread = jnp.concatenate(
            [
                jnp.where(at0, ll, 0.0) + jnp.where(at1, lh, 0.0),
                jnp.where(at0, hl, 0.0) + jnp.where(at1, hh, 0.0),
            ],
            axis=1,
        )
        pick = one_hot(rows == to_row(row, bands))
        hi, lo = two(spread)
        total = total + (mm(pick, hi) + mm(pick, lo))
        pick = one_hot(rows == to_row(part[8], bands))
        values = jnp.where(lane == 0.0, part[9], jnp.where(lane == 1.0, part[10], 0.0))
        hi, lo = two(values)
        side = side + (mm(pick, hi) + mm(pick, lo))
        o = 64 + 16 * k
        part = [table[:, o + i : o + i + 1] for i in range(11)]
        row, col, ll, hl, lh, hh = part[0:6]
        edge = row == float(height - 1)
        first_row = (
            first_row
            + jnp.where((lanes == col) & edge, hl, 0.0)
            + jnp.where((lanes == col + 1.0) & edge, hh, 0.0)
        )
        corner = corner + jnp.where(part[8] == float(height - 1), part[10], 0.0)
    same = total[:, 0:across]
    down = pltpu.roll(total[:, across:], 1, 0)
    side_down = pltpu.roll(side, 1, 0)
    r = iota((height, across), 0)
    c = iota((height, across), 1)
    incoming = jnp.sum(first_row, axis=0, keepdims=True)
    incoming = incoming + jnp.where(iota((1, across), 1) == 0.0, jnp.sum(corner), 0.0)
    down = jnp.where(r == 0.0, incoming, down)
    column = side[:, 0:1] + jnp.where(iota((height, 1), 0) == 0.0, 0.0, side_down[:, 1:2])
    out_ref[...] = base_ref[...] + (same + down + jnp.where(c == 0.0, column, 0.0))


def ring(axis, distance):
    n = lax.axis_size(axis)
    return [(i, (i + distance) % n) for i in range(n)]


def shards(level_set, velocity, particles, escaped, home_cell, land_cell, dest_rank, block_count):
    height, across = level_set.shape
    n = particles.shape[0]
    bands = lax.axis_size("gy")
    step = 4 * CAP + 1
    sds = jax.ShapeDtypeStruct
    head, tail = call(heads_body, (sds((24, across), F32), sds((24, across), F32)), level_set, velocity)
    below = lax.ppermute(head, "gy", ring("gy", -1))
    above = lax.ppermute(tail, "gy", ring("gy", 1))
    parts = jnp.transpose(particles, (1, 0, 2))
    meta, weight, select, fixed = call(
        prepare_body,
        (
            sds((n, 128), F32),
            sds((n, 128), F32),
            sds((bands * CAP, n), BF16),
            sds((bands * CAP, 256), F32),
        ),
        velocity, parts, escaped, home_cell.reshape(1, n), land_cell.reshape(1, n), dest_rank.reshape(1, n),
        scalars=(block_count,),
    )
    to_left, to_right, meta = call(
        edges_body,
        (sds((height + 16, 128), F32), sds((height + 16 + 3 * n, 128), F32), sds((n, 128), F32)),
        level_set, velocity, below, meta, parts, weight,
    )
    from_left = lax.ppermute(to_right, "gx", ring("gx", 1))
    from_right = lax.ppermute(to_left, "gx", ring("gx", -1))
    (packed,) = call(
        functools.partial(pack_body, height=height, across=across),
        (sds((bands * step, 128), F32),),
        parts, weight, meta, to_left, from_left, from_right, select, fixed,
    )
    arrived = lax.all_to_all(
        packed.reshape(bands * step, 1, 128), "gy", split_axis=0, concat_axis=0, tiled=True
    ).reshape(bands * step, 128)
    to_left2, to_right2 = call(corners_body, (sds((16, 128), F32), sds((16, 128), F32)), above)
    from_left2 = lax.ppermute(to_right2, "gx", ring("gx", 1))
    from_right2 = lax.ppermute(to_left2, "gx", ring("gx", -1))
    wide = pltpu.VMEM(((across // 128 + 1) * (height + 32), 128), F32)
    (section,) = call(
        stencil_body,
        (sds((height, across), F32),),
        level_set, velocity, below, above, from_right, from_left, from_right2, from_left2,
        scratch=[wide] * 5,
    )
    level, moved = call(
        deposit_body,
        (sds((height, across), F32), sds((bands * CAP * 4, 128), F32)),
        arrived, section,
    )
    return level, moved.reshape(bands * CAP, 4, 128)


def solution(mesh):
    in_specs = (
        P("gy", "gx"),
        P(None, "gy", "gx"),
        P(("gy", "gx"), None, None),
        P(("gy", "gx"), None),
        P(("gy", "gx")),
        P(("gy", "gx")),
        P(("gy", "gx")),
        P(("gy", "gx")),
    )
    out_specs = (P("gy", "gx"), P(("gy", "gx"), None, None))
    return jax.shard_map(shards, mesh=mesh, in_specs=in_specs, out_specs=out_specs, check_vma=False)
```

```python
import functools
import jax
import jax.numpy as jnp
from jax import lax
from jax.experimental import pallas as pl
from jax.experimental.pallas import tpu as pltpu
from jax.sharding import PartitionSpec as P

CAP = 4
DT = 0.3
INTERPRET = False
F32 = jnp.float32
BF16 = jnp.bfloat16


def iota(shape, dim):
    return lax.broadcasted_iota(jnp.int32, shape, dim).astype(F32)


def split3(x):
    hi = x.astype(BF16)
    rest = x - hi.astype(F32)
    mid = rest.astype(BF16)
    lo = (rest - mid.astype(F32)).astype(BF16)
    return hi, mid, lo


def mm(a, b):
    return lax.dot_general(a, b, (((1,), (0,)), ((), ())), preferred_element_type=F32)


def exact_pick(one_hot, x):
    hi, mid, lo = split3(x)
    return (mm(one_hot, hi) + mm(one_hot, mid)) + mm(one_hot, lo)


def eye(n):
    return iota((n, n), 0) == iota((n, n), 1)


def to_column(row, n):
    return jnp.sum(jnp.where(eye(n), jnp.broadcast_to(row, (n, n)), 0.0), axis=1, keepdims=True)


def to_row(col, n):
    return jnp.sum(jnp.where(eye(n), jnp.broadcast_to(col, (n, n)), 0.0), axis=0, keepdims=True)


def one_hot(mask):
    return jnp.where(mask, 1.0, 0.0).astype(BF16)


def floor_div(x, k):
    return jnp.floor((x + 0.5) * (1.0 / k))


def call(body, outs, *args, scratch=(), spaces=None, out_spaces=None, scalars=()):
    vm, sm = pltpu.VMEM, pltpu.SMEM
    spaces = spaces or [vm] * len(args)
    out_spaces = out_spaces or [vm] * len(outs)
    spec = lambda space: pl.BlockSpec(memory_space=space)
    return pl.pallas_call(
        body,
        out_shape=tuple(outs),
        in_specs=[spec(sm)] * len(scalars) + [spec(x) for x in spaces],
        out_specs=tuple(spec(x) for x in out_spaces),
        scratch_shapes=list(scratch),
        compiler_params=pltpu.CompilerParams(vmem_limit_bytes=16 * 1024 * 1024),
        interpret=INTERPRET,
    )(*scalars, *args)


def heads_body(f_ref, flow_ref, head_ref, tail_ref, f_rows, flow_rows, sems):
    height = f_ref.shape[0]
    copies = []
    for i, (f_top, flow_top) in enumerate(((0, 0), (height - 16, height - 8))):
        copies.append(pltpu.make_async_copy(f_ref.at[pl.ds(f_top, 16)], f_rows.at[i], sems.at[2 * i]))
        copies.append(pltpu.make_async_copy(flow_ref.at[:, pl.ds(flow_top, 8)], flow_rows.at[i], sems.at[2 * i + 1]))
    for copy in copies:
        copy.start()
    for copy in copies:
        copy.wait()
    for i, (ref, f0, v0) in enumerate(((head_ref, 0, 0), (tail_ref, 7, 2))):
        ref[0:9] = f_rows[i, f0 : f0 + 9]
        ref[9:15] = flow_rows[i, 0, v0 : v0 + 6]
        ref[15:21] = flow_rows[i, 1, v0 : v0 + 6]
        ref[21:24] = jnp.zeros((3, f_ref.shape[1]), F32)


def prepare_body(count_ref, flow_ref, part_ref, esc_ref, home_ref, land_ref, dest_ref, meta_ref, w_ref, sel_ref, rw_ref):
    n = esc_ref.shape[0]
    height, across = flow_ref.shape[1:]
    home = to_column(home_ref[...].astype(F32), n)
    land = to_column(land_ref[...].astype(F32), n)
    dest_row = dest_ref[...].astype(F32)
    dest = to_column(dest_row, n)
    count = count_ref[0].astype(F32)
    row = floor_div(home, across)
    col = home - row * across
    land_row = floor_div(land, across)
    land_col = land - land_row * across
    other = iota((n, n), 0)
    mine = iota((n, n), 1)
    same = (dest == dest_row) & (other < mine) & (other < count)
    rank_row = jnp.sum(jnp.where(same, 1.0, 0.0), axis=0, keepdims=True)
    live_row = iota((1, n), 1) < count
    slot_row = jnp.where(live_row, dest_row * CAP + rank_row, -1.0)
    slot = to_column(slot_row, n)
    lane = iota((n, height), 1)
    pick = jnp.concatenate([one_hot(lane == row), one_hot(lane == row + 1.0)], axis=0)
    lanes = iota((n, across), 1)
    at0 = lanes == col
    at1 = lanes == col + 1.0
    parts = []
    for component in range(2):
        both = exact_pick(pick, flow_ref[component])
        low = both[0:n]
        high = both[n:]
        for where_at in (at0, at1):
            for rows in (low, high):
                parts.append(jnp.sum(jnp.where(where_at, rows, 0.0), axis=1, keepdims=True))
    columns = parts + [row, col, land_row, land_col, slot]
    lane = iota((n, 128), 1)
    meta = jnp.zeros((n, 128), F32)
    for i, value in enumerate(columns):
        meta = jnp.where(lane == float(i), value, meta)
    meta_ref[...] = meta
    w = esc_ref[...].astype(F32) * part_ref[2]
    w_ref[...] = w
    slots = sel_ref.shape[0]
    bands = slots // CAP
    r = iota((slots, 1), 0)
    k = floor_div(r, bands)
    choose = one_hot((r - k * bands) * CAP + k == slot_row)
    sel_ref[...] = choose
    rw_ref[...] = exact_pick(choose, jnp.concatenate([part_ref[2], w], axis=1))


def pack_left(f, u, v):
    lane = iota(f.shape, 1)
    return jnp.where(lane < 16.0, f, jnp.where(lane < 32.0, pltpu.roll(u, 16, 1), pltpu.roll(v, 32, 1)))


def pack_right(f, u, v, m):
    lane = iota(f.shape, 1)
    out = jnp.where(lane >= 112.0, f, jnp.where(lane >= 96.0, pltpu.roll(u, 112, 1), pltpu.roll(v, 96, 1)))
    return jnp.where(lane < 16.0, m, out)


def corners_body(above_ref, left_ref, right_ref):
    across = above_ref.shape[1]
    zero = jnp.zeros((8, 128), F32)
    near, far = slice(0, 128), slice(across - 128, across)
    left_ref[0:8] = pack_left(above_ref[0:8, near], above_ref[9:17, near], above_ref[15:23, near])
    left_ref[8:16] = pack_left(above_ref[8:16, near], zero, zero)
    right_ref[0:8] = pack_right(above_ref[0:8, far], above_ref[9:17, far], above_ref[15:23, far], zero)
    right_ref[8:16] = pack_right(above_ref[8:16, far], zero, zero, zero)


def edges_body(f_ref, flow_ref, below_ref, meta_ref, part_ref, w_ref, left_ref, right_ref, meta2_ref):
    n = w_ref.shape[0]
    height, across = f_ref.shape
    meta = meta_ref[...]
    lane = iota((n, 128), 1)
    row = meta[:, 8:9]
    col = meta[:, 9:10]
    last = row == float(height - 1)
    lanes = iota((n, across), 1)
    at0 = (lanes == col) & last
    at1 = (lanes == col + 1.0) & last
    for base, r in ((0, 9), (4, 15)):
        line = jnp.broadcast_to(below_ref[r : r + 1, :], (n, across))
        c10 = jnp.sum(jnp.where(at0, line, 0.0), axis=1, keepdims=True)
        c11 = jnp.sum(jnp.where(at1, line, 0.0), axis=1, keepdims=True)
        meta = meta + jnp.where(lane == float(base + 1), c10, 0.0) + jnp.where(lane == float(base + 3), c11, 0.0)
    meta2_ref[...] = meta
    far = across - 128

    zero = jnp.zeros((8, 128), F32)

    def pieces(sl):
        yield 0, height, f_ref[:, sl], flow_ref[0, :, sl], flow_ref[1, :, sl], meta
        yield height, 8, below_ref[0:8, sl], below_ref[9:17, sl], below_ref[15:23, sl], zero
        yield height + 8, 8, below_ref[8:16, sl], zero, zero, zero

    for top, rows, f, u, v, _ in pieces(slice(0, 128)):
        left_ref[top : top + rows] = pack_left(f, u, v)
    for top, rows, f, u, v, m in pieces(slice(far, across)):
        right_ref[top : top + rows] = pack_right(f, u, v, m)
    top = height + 16
    right_ref[top : top + n] = part_ref[0]
    right_ref[top + n : top + 2 * n] = part_ref[1]
    right_ref[top + 2 * n : top + 3 * n] = w_ref[...]


def halo_tiles(from_right, from_left):
    lane = iota(from_right.shape, 1)
    right_side = lane < 64.0
    f = jnp.where(right_side, from_right, from_left)
    u = jnp.where(right_side, pltpu.roll(from_right, 112, 1), pltpu.roll(from_left, 16, 1))
    v = jnp.where(right_side, pltpu.roll(from_right, 96, 1), pltpu.roll(from_left, 32, 1))
    return f, u, v


def moved_particles(meta, x, y, column, across):
    n = x.shape[0]
    row = meta[:, 8:9]
    last = meta[:, 9:10] == float(across - 1)
    lane = iota((n, column.shape[0]), 1)
    pick = jnp.concatenate([one_hot((lane == row) & last), one_hot((lane == row + 1.0) & last)], axis=0)
    both = exact_pick(pick, column)
    low = both[0:n]
    high = both[n:]
    u = [meta[:, 0:1], meta[:, 1:2], meta[:, 2:3] + low[:, 16:17], meta[:, 3:4] + high[:, 16:17]]
    v = [meta[:, 4:5], meta[:, 5:6], meta[:, 6:7] + low[:, 32:33], meta[:, 7:8] + high[:, 32:33]]
    fy = y + 0.5
    fx = x + 0.5
    w00 = (1.0 - fy) * (1.0 - fx)
    w10 = fy * (1.0 - fx)
    w01 = (1.0 - fy) * fx
    w11 = fy * fx
    new_x = x + DT * (w00 * u[0] + w10 * u[1] + w01 * u[2] + w11 * u[3])
    new_y = y + DT * (w00 * v[0] + w10 * v[1] + w01 * v[2] + w11 * v[3])
    return new_x, new_y


def lane_sum(x):
    return jnp.sum(x, axis=1, keepdims=True)


def pack_body(part_ref, w_ref, meta_ref, mine_ref, left_ref, right_ref, sel_ref, rw_ref, out_ref, height, across):
    n = w_ref.shape[0]
    bands = out_ref.shape[0] // (4 * CAP + 1)
    meta = meta_ref[...]
    top = height + 16
    step = 4 * CAP + 1
    w = w_ref[...]
    new_x, new_y = moved_particles(meta, part_ref[0], part_ref[1], right_ref[0 : height + 16], across)
    left_meta = left_ref[0:n]
    left_w = left_ref[top + 2 * n : top + 3 * n]
    left_x, left_y = moved_particles(
        left_meta, left_ref[top : top + n], left_ref[top + n : top + 2 * n], mine_ref[0 : height + 16], across
    )
    choose = sel_ref[...]
    xy = exact_pick(choose, jnp.concatenate([new_x, new_y], axis=1))
    for k in range(CAP):
        rows = slice(k * bands, (k + 1) * bands)
        for j, source, sl in ((0, xy, slice(0, 128)), (1, xy, slice(128, 256)), (2, rw_ref, slice(0, 128)), (3, rw_ref, slice(128, 256))):
            out_ref[pl.ds(4 * k + j, bands, stride=step), :] = source[rows, sl]
    gy = new_y + 0.5
    gx = new_x + 0.5
    sums = [
        meta[:, 10:11],
        meta[:, 11:12],
        lane_sum(w * (1.0 - gy) * (1.0 - gx)),
        lane_sum(w * gy * (1.0 - gx)),
        lane_sum(w * (1.0 - gy) * gx),
        lane_sum(w * gy * gx),
    ]
    lane = iota((n, 128), 1)
    lane16 = lane - 16.0 * jnp.floor(lane * 0.0625)
    mine = jnp.zeros((n, 128), F32)
    for i, value in enumerate(sums):
        mine = jnp.where(lane16 == float(i), value, mine)
    gy = left_y + 0.5
    gx = left_x + 0.5
    over = left_meta[:, 11:12] == float(across - 1)
    sums = [
        left_meta[:, 10:11],
        jnp.where(over, lane_sum(left_w * (1.0 - gy) * gx), 0.0),
        jnp.where(over, lane_sum(left_w * gy * gx), 0.0),
    ]
    theirs = jnp.zeros((n, 128), F32)
    for i, value in enumerate(sums):
        theirs = jnp.where(lane16 == float(8 + i), value, theirs)
    values = jnp.concatenate([mine, theirs], axis=0)
    d4 = iota((bands, n), 0) * float(CAP)
    slot = to_row(left_meta[:, 12:13], n)
    theirs_choose = jnp.concatenate([one_hot(d4 + float(k) == slot) for k in range(CAP)], axis=0)
    chosen = exact_pick(jnp.concatenate([choose, theirs_choose], axis=1), values)
    lane = iota((bands, 128), 1)
    group = jnp.floor(lane * 0.0625)
    table = jnp.zeros((bands, 128), F32)
    for k in range(CAP):
        table = jnp.where(group == float(k), chosen[k * bands : (k + 1) * bands], table)
    table = table + pltpu.roll(pltpu.roll(table, 1, 0), 64, 1)
    out_ref[pl.ds(4 * CAP, bands, stride=step), :] = table


def side_term(speed, e0, e1, e2, e3, e4, d2, d3):
    ahead = speed > 0.0
    p = jnp.where(ahead, e0, e4)
    q = jnp.where(ahead, e1, e3)
    s = jnp.where(ahead, e3, e1)
    c = jnp.where(ahead, d2, d3)
    r = e2
    rr = r * r
    t1 = p * (4.0 * p - 11.0 * q) + (10.0 * (q * q) + 3e-6)
    t2 = q * (4.0 * q - 5.0 * r) + (4.0 * rr + 3e-6)
    t3 = s * (4.0 * s - 11.0 * r) + (10.0 * rr + 3e-6)
    a1 = t2 * t3
    a2 = t1 * t3
    a3 = t1 * t2
    w1 = a1 * a1
    w2 = 6.0 * (a2 * a2)
    w3 = 3.0 * (a3 * a3)
    top = w1 * (2.0 * p - 5.0 * q) - w2 * (q + 2.0 * r) + w3 * (s - 4.0 * r)
    return speed * c + jnp.abs(speed) * (top / (6.0 * (w1 + w2 + w3)))


def stencil_body(f_ref, flow_ref, below_ref, above_ref, right_ref, left_ref, right2_ref, left2_ref, out_ref, f0, us, vs, f1, f2):
    height, across = f_ref.shape
    width = across + 128
    tiles = width // 128
    off = 16
    span = height + 32
    halos = halo_tiles(right_ref[...], left_ref[0 : height + 16])
    uppers = halo_tiles(right2_ref[...], left2_ref[...])
    owns = (f_ref, flow_ref.at[0], flow_ref.at[1])
    for buf, own, halo, upper, start, count in zip((f0, us, vs), owns, halos, uppers, (0, 9, 15), (9, 6, 6)):
        for j in range(tiles):
            sl = slice(128 * j, 128 * j + 128)
            top = span * j + off
            if j < tiles - 1:
                buf[top : top + height, :] = own[:, sl]
                buf[top + height : top + height + count, :] = below_ref[start : start + count, sl]
                buf[top - count : top, :] = above_ref[start : start + count, sl]
            else:
                buf[top : top + height + count, :] = halo[0 : height + count]
                buf[top - count : top, :] = upper[0:count]

    lane = lax.broadcasted_iota(jnp.int32, (8, 128), 1)

    def stage(src, dst_tiles, base, write):
        f = [src[pl.ds(span * j + base, 8), :] for j in range(tiles)]

        def shifted(k):
            turned = [pltpu.roll(t, (-k) % 128, 1) for t in f]
            if k > 0:
                return [jnp.where(lane < 128 - k, turned[j], turned[(j + 1) % tiles]) for j in range(dst_tiles)]
            return [jnp.where(lane >= -k, turned[j], turned[(j - 1) % tiles]) for j in range(dst_tiles)]

        near = {k: f if k == 0 else shifted(k) for k in range(-3, 4)}
        for j in range(dst_tiles):
            at = span * j + base
            u = us[pl.ds(at, 8), :]
            v = vs[pl.ds(at, 8), :]
            d = [near[k + 1][j] - near[k][j] for k in range(-3, 3)]
            e = [d[k] - d[k + 1] for k in range(5)]
            x_term = side_term(u, e[0], e[1], e[2], e[3], e[4], d[2], d[3])
            rows = [f[j] if k == 0 else src[pl.ds(at + k, 8), :] for k in range(-3, 4)]
            d = [rows[k + 1] - rows[k] for k in range(6)]
            e = [d[k] - d[k + 1] for k in range(5)]
            y_term = side_term(v, e[0], e[1], e[2], e[3], e[4], d[2], d[3])
            write(j, f[j] - DT * (x_term + y_term))

    def first(i, carry):
        base = pl.multiple_of(i * 8 + 8, 8)

        def write(j, value):
            f1[pl.ds(span * j + base, 8), :] = value

        stage(f0, tiles, base, write)
        return carry

    def second(i, carry):
        base = pl.multiple_of(i * 8 + 8, 8)

        def write(j, value):
            at = pl.ds(span * j + base, 8)
            f2[at, :] = 0.75 * f0[at, :] + 0.25 * value

        stage(f1, tiles, base, write)
        return carry

    def third(i, carry):
        base = pl.multiple_of(i * 8 + 16, 8)
        place = pl.multiple_of(i * 8, 8)

        def write(j, value):
            kept = f0[pl.ds(span * j + base, 8), :]
            out_ref[pl.ds(place, 8), 128 * j : 128 * j + 128] = kept * (1.0 / 3.0) + (2.0 / 3.0) * value

        stage(f2, tiles - 1, base, write)
        return carry

    lax.fori_loop(0, height // 8 + 2, first, 0, unroll=2)
    lax.fori_loop(0, height // 8 + 2, second, 0, unroll=2)
    lax.fori_loop(0, height // 8, third, 0, unroll=2)


def deposit_body(rows_ref, recv_ref, base_ref, out_ref, moved_ref, sem):
    height, across = base_ref.shape
    step = 4 * CAP + 1
    bands = recv_ref.shape[0] // step
    block = 4 * CAP
    copy = pltpu.make_async_copy(rows_ref.at[:, pl.ds(0, block)], moved_ref, sem)
    copy.start()
    table = recv_ref[pl.ds(block, bands, stride=step), :]
    lanes = iota((bands, across), 1)
    lane = iota((bands, 128), 1)
    rows = iota((height, bands), 0)
    total = jnp.zeros((height, 2 * across), F32)
    side = jnp.zeros((height, 128), F32)
    first_row = jnp.zeros((bands, across), F32)
    corner = jnp.zeros((bands, 1), F32)

    def two(x):
        hi = x.astype(BF16)
        return hi, (x - hi.astype(F32)).astype(BF16)

    for k in range(CAP):
        o = 16 * k
        part = [table[:, o + i : o + i + 1] for i in range(11)]
        row, col, ll, hl, lh, hh = part[0:6]
        at0 = lanes == col
        at1 = lanes == col + 1.0
        spread = jnp.concatenate(
            [
                jnp.where(at0, ll, 0.0) + jnp.where(at1, lh, 0.0),
                jnp.where(at0, hl, 0.0) + jnp.where(at1, hh, 0.0),
            ],
            axis=1,
        )
        pick = one_hot(rows == to_row(row, bands))
        hi, lo = two(spread)
        total = total + (mm(pick, hi) + mm(pick, lo))
        pick = one_hot(rows == to_row(part[8], bands))
        values = jnp.where(lane == 0.0, part[9], jnp.where(lane == 1.0, part[10], 0.0))
        hi, lo = two(values)
        side = side + (mm(pick, hi) + mm(pick, lo))
        o = 64 + 16 * k
        part = [table[:, o + i : o + i + 1] for i in range(11)]
        row, col, ll, hl, lh, hh = part[0:6]
        edge = row == float(height - 1)
        first_row = (
            first_row
            + jnp.where((lanes == col) & edge, hl, 0.0)
            + jnp.where((lanes == col + 1.0) & edge, hh, 0.0)
        )
        corner = corner + jnp.where(part[8] == float(height - 1), part[10], 0.0)
    same = total[:, 0:across]
    down = pltpu.roll(total[:, across:], 1, 0)
    side_down = pltpu.roll(side, 1, 0)
    r = iota((height, across), 0)
    c = iota((height, across), 1)
    incoming = jnp.sum(first_row, axis=0, keepdims=True)
    incoming = incoming + jnp.where(iota((1, across), 1) == 0.0, jnp.sum(corner), 0.0)
    down = jnp.where(r == 0.0, incoming, down)
    column = side[:, 0:1] + jnp.where(iota((height, 1), 0) == 0.0, 0.0, side_down[:, 1:2])
    out_ref[...] = base_ref[...] + (same + down + jnp.where(c == 0.0, column, 0.0))
    copy.wait()


def ring(axis, distance):
    n = lax.axis_size(axis)
    return [(i, (i + distance) % n) for i in range(n)]


def shards(level_set, velocity, particles, escaped, home_cell, land_cell, dest_rank, block_count):
    height, across = level_set.shape
    n = particles.shape[0]
    bands = lax.axis_size("gy")
    step = 4 * CAP + 1
    sds = jax.ShapeDtypeStruct
    head, tail = call(
        heads_body,
        (sds((24, across), F32), sds((24, across), F32)),
        pltpu.with_memory_space_constraint(level_set, pltpu.HBM),
        pltpu.with_memory_space_constraint(velocity, pltpu.HBM),
        spaces=[pltpu.HBM, pltpu.HBM],
        scratch=[pltpu.VMEM((2, 16, across), F32), pltpu.VMEM((2, 2, 8, across), F32), pltpu.SemaphoreType.DMA((4,))],
    )
    below = lax.ppermute(head, "gy", ring("gy", -1))
    above = lax.ppermute(tail, "gy", ring("gy", 1))
    parts = jnp.transpose(particles, (1, 0, 2))
    meta, weight, select, fixed = call(
        prepare_body,
        (
            sds((n, 128), F32),
            sds((n, 128), F32),
            sds((bands * CAP, n), BF16),
            sds((bands * CAP, 256), F32),
        ),
        velocity, parts, escaped, home_cell.reshape(1, n), land_cell.reshape(1, n), dest_rank.reshape(1, n),
        scalars=(block_count,),
    )
    to_left, to_right, meta = call(
        edges_body,
        (sds((height + 16, 128), F32), sds((height + 16 + 3 * n, 128), F32), sds((n, 128), F32)),
        level_set, velocity, below, meta, parts, weight,
    )
    from_left = lax.ppermute(to_right, "gx", ring("gx", 1))
    from_right = lax.ppermute(to_left, "gx", ring("gx", -1))
    (packed,) = call(
        functools.partial(pack_body, height=height, across=across),
        (sds((bands * step, 128), F32),),
        parts, weight, meta, to_left, from_left, from_right, select, fixed,
    )
    arrived = lax.all_to_all(
        packed.reshape(bands * step, 1, 128), "gy", split_axis=0, concat_axis=0, tiled=True
    )
    to_left2, to_right2 = call(corners_body, (sds((16, 128), F32), sds((16, 128), F32)), above)
    from_left2 = lax.ppermute(to_right2, "gx", ring("gx", 1))
    from_right2 = lax.ppermute(to_left2, "gx", ring("gx", -1))
    wide = pltpu.VMEM(((across // 128 + 1) * (height + 32), 128), F32)
    (section,) = call(
        stencil_body,
        (sds((height, across), F32),),
        level_set, velocity, below, above, from_right, from_left, from_right2, from_left2,
        scratch=[wide] * 5,
    )
    level, moved = call(
        deposit_body,
        (sds((height, across), F32), sds((bands, 4 * CAP, 1, 128), F32)),
        arrived.reshape(bands, step, 1, 128), arrived.reshape(bands * step, 128), section,
        out_spaces=[pltpu.VMEM, pltpu.HBM],
        scratch=[pltpu.SemaphoreType.DMA],
    )
    return level, moved.reshape(bands * CAP, 4, 128)


def solution(mesh):
    in_specs = (
        P("gy", "gx"),
        P(None, "gy", "gx"),
        P(("gy", "gx"), None, None),
        P(("gy", "gx"), None),
        P(("gy", "gx")),
        P(("gy", "gx")),
        P(("gy", "gx")),
        P(("gy", "gx")),
    )
    out_specs = (P("gy", "gx"), P(("gy", "gx"), None, None))
    return jax.shard_map(shards, mesh=mesh, in_specs=in_specs, out_specs=out_specs, check_vma=False)
```

```python
import functools
import jax
import jax.numpy as jnp
from jax import lax
from jax.experimental import pallas as pl
from jax.experimental.pallas import tpu as pltpu
from jax.sharding import PartitionSpec as P

CAP = 4
DT = 0.3
INTERPRET = False
F32 = jnp.float32
BF16 = jnp.bfloat16


def iota(shape, dim):
    return lax.broadcasted_iota(jnp.int32, shape, dim).astype(F32)


def split3(x):
    hi = x.astype(BF16)
    rest = x - hi.astype(F32)
    mid = rest.astype(BF16)
    lo = (rest - mid.astype(F32)).astype(BF16)
    return hi, mid, lo


def mm(a, b):
    return lax.dot_general(a, b, (((1,), (0,)), ((), ())), preferred_element_type=F32)


def stack3(x):
    return jnp.concatenate(split3(x), axis=0)


def phase(shape, period):
    lane = iota(shape, 1)
    return lane - period * floor_div(lane, period)


def eye(n):
    return iota((n, n), 0) == iota((n, n), 1)


def to_column(row, n):
    return jnp.sum(jnp.where(eye(n), jnp.broadcast_to(row, (n, n)), 0.0), axis=1, keepdims=True)


def to_row(col, n):
    return jnp.sum(jnp.where(eye(n), jnp.broadcast_to(col, (n, n)), 0.0), axis=0, keepdims=True)


def one_hot(mask):
    return jnp.where(mask, 1.0, 0.0).astype(BF16)


def floor_div(x, k):
    return jnp.floor((x + 0.5) * (1.0 / k))


def call(body, outs, *args, scratch=(), spaces=None, out_spaces=None, scalars=()):
    vm, sm = pltpu.VMEM, pltpu.SMEM
    spaces = spaces or [vm] * len(args)
    out_spaces = out_spaces or [vm] * len(outs)
    spec = lambda space: pl.BlockSpec(memory_space=space)
    return pl.pallas_call(
        body,
        out_shape=tuple(outs),
        in_specs=[spec(sm)] * len(scalars) + [spec(x) for x in spaces],
        out_specs=tuple(spec(x) for x in out_spaces),
        scratch_shapes=list(scratch),
        compiler_params=pltpu.CompilerParams(vmem_limit_bytes=16 * 1024 * 1024),
        interpret=INTERPRET,
    )(*scalars, *args)


def heads_body(f_ref, flow_ref, head_ref, tail_ref, f_rows, flow_rows, sems):
    height = f_ref.shape[0]
    copies = []
    for i, (f_top, flow_top) in enumerate(((0, 0), (height - 16, height - 8))):
        copies.append(pltpu.make_async_copy(f_ref.at[pl.ds(f_top, 16)], f_rows.at[i], sems.at[2 * i]))
        copies.append(pltpu.make_async_copy(flow_ref.at[:, pl.ds(flow_top, 8)], flow_rows.at[i], sems.at[2 * i + 1]))
    for copy in copies:
        copy.start()
    for copy in copies:
        copy.wait()
    for i, (ref, f0, v0) in enumerate(((head_ref, 0, 0), (tail_ref, 7, 2))):
        ref[0:9] = f_rows[i, f0 : f0 + 9]
        ref[9:15] = flow_rows[i, 0, v0 : v0 + 6]
        ref[15:21] = flow_rows[i, 1, v0 : v0 + 6]
        ref[21:24] = jnp.zeros((3, f_ref.shape[1]), F32)


def prepare_body(count_ref, flow_ref, part_ref, esc_ref, home_ref, land_ref, dest_ref, meta_ref, w_ref, sel_ref, rw_ref):
    n = esc_ref.shape[0]
    height, across = flow_ref.shape[1:]
    home = to_column(home_ref[...].astype(F32), n)
    land = to_column(land_ref[...].astype(F32), n)
    dest_row = dest_ref[...].astype(F32)
    dest = to_column(dest_row, n)
    count = count_ref[0].astype(F32)
    row = floor_div(home, across)
    col = home - row * across
    land_row = floor_div(land, across)
    land_col = land - land_row * across
    other = iota((n, n), 0)
    mine = iota((n, n), 1)
    same = (dest == dest_row) & (other < mine) & (other < count)
    rank_row = jnp.sum(jnp.where(same, 1.0, 0.0), axis=0, keepdims=True)
    live_row = iota((1, n), 1) < count
    slot_row = jnp.where(live_row, dest_row * CAP + rank_row, -1.0)
    slot = to_column(slot_row, n)
    lane = phase((n, 3 * height), height)
    pick = jnp.concatenate([one_hot(lane == row), one_hot(lane == row + 1.0)], axis=0)
    lanes = iota((n, across), 1)
    at0 = lanes == col
    at1 = lanes == col + 1.0
    parts = []
    for component in range(2):
        both = mm(pick, stack3(flow_ref[component]))
        low = both[0:n]
        high = both[n:]
        for where_at in (at0, at1):
            for rows in (low, high):
                parts.append(jnp.sum(jnp.where(where_at, rows, 0.0), axis=1, keepdims=True))
    columns = parts + [row, col, land_row, land_col, slot]
    lane = iota((n, 128), 1)
    meta = jnp.zeros((n, 128), F32)
    for i, value in enumerate(columns):
        meta = jnp.where(lane == float(i), value, meta)
    meta_ref[...] = meta
    w = esc_ref[...].astype(F32) * part_ref[2]
    w_ref[...] = w
    slots = sel_ref.shape[0]
    bands = slots // CAP
    r = iota((slots, 1), 0)
    k = floor_div(r, bands)
    choose = one_hot((r - k * bands) * CAP + k == jnp.concatenate([slot_row] * 3, axis=1))
    sel_ref[...] = choose
    rw_ref[...] = mm(choose, stack3(jnp.concatenate([part_ref[2], w], axis=1)))


def pack_left(f, u, v):
    lane = iota(f.shape, 1)
    return jnp.where(lane < 16.0, f, jnp.where(lane < 32.0, pltpu.roll(u, 16, 1), pltpu.roll(v, 32, 1)))


def pack_right(f, u, v, m):
    lane = iota(f.shape, 1)
    out = jnp.where(lane >= 112.0, f, jnp.where(lane >= 96.0, pltpu.roll(u, 112, 1), pltpu.roll(v, 96, 1)))
    return jnp.where(lane < 32.0, m, out)


def corners_body(above_ref, left_ref, right_ref):
    across = above_ref.shape[1]
    zero = jnp.zeros((8, 128), F32)
    near, far = slice(0, 128), slice(across - 128, across)
    left_ref[0:8] = pack_left(above_ref[0:8, near], above_ref[9:17, near], above_ref[15:23, near])
    left_ref[8:16] = pack_left(above_ref[8:16, near], zero, zero)
    right_ref[0:8] = pack_right(above_ref[0:8, far], above_ref[9:17, far], above_ref[15:23, far], zero)
    right_ref[8:16] = pack_right(above_ref[8:16, far], zero, zero, zero)


def edges_body(f_ref, flow_ref, below_ref, meta_ref, part_ref, w_ref, left_ref, right_ref, meta2_ref):
    n = w_ref.shape[0]
    height, across = f_ref.shape
    meta = meta_ref[...]
    lane = iota((n, 128), 1)
    row = meta[:, 8:9]
    col = meta[:, 9:10]
    last = row == float(height - 1)
    lanes = iota((n, across), 1)
    at0 = (lanes == col) & last
    at1 = (lanes == col + 1.0) & last
    for base, r in ((0, 9), (4, 15)):
        line = jnp.broadcast_to(below_ref[r : r + 1, :], (n, across))
        c10 = jnp.sum(jnp.where(at0, line, 0.0), axis=1, keepdims=True)
        c11 = jnp.sum(jnp.where(at1, line, 0.0), axis=1, keepdims=True)
        meta = meta + jnp.where(lane == float(base + 1), c10, 0.0) + jnp.where(lane == float(base + 3), c11, 0.0)
    meta2_ref[...] = meta
    x = part_ref[0]
    y = part_ref[1]
    w = w_ref[...]
    fy = y + 0.5
    fx = x + 0.5
    near0 = (1.0 - fy) * (1.0 - fx)
    near1 = fy * (1.0 - fx)
    gx = fx + DT * (near0 * meta[:, 0:1] + near1 * meta[:, 1:2])
    gy = fy + DT * (near0 * meta[:, 4:5] + near1 * meta[:, 5:6])
    e1 = DT * ((1.0 - fy) * fx)
    e2 = DT * (fy * fx)
    wgx, wgy, w1, w2 = w * gx, w * gy, w * e1, w * e2
    moments = [wgx, w1, w2, wgx * gy, wgy * e1, wgy * e2, wgx * e1, wgx * e2, w1 * e1, w1 * e2, w2 * e2]
    sent = meta
    for i, value in enumerate(moments):
        sent = jnp.where(lane == float(16 + i), lane_sum(value), sent)
    far = across - 128

    zero = jnp.zeros((8, 128), F32)

    def pieces(sl):
        yield 0, height, f_ref[:, sl], flow_ref[0, :, sl], flow_ref[1, :, sl], sent
        yield height, 8, below_ref[0:8, sl], below_ref[9:17, sl], below_ref[15:23, sl], zero
        yield height + 8, 8, below_ref[8:16, sl], zero, zero, zero

    for top, rows, f, u, v, _ in pieces(slice(0, 128)):
        left_ref[top : top + rows] = pack_left(f, u, v)
    for top, rows, f, u, v, m in pieces(slice(far, across)):
        right_ref[top : top + rows] = pack_right(f, u, v, m)


def halo_tiles(from_right, from_left):
    lane = iota(from_right.shape, 1)
    right_side = lane < 64.0
    f = jnp.where(right_side, from_right, from_left)
    u = jnp.where(right_side, pltpu.roll(from_right, 112, 1), pltpu.roll(from_left, 16, 1))
    v = jnp.where(right_side, pltpu.roll(from_right, 96, 1), pltpu.roll(from_left, 32, 1))
    return f, u, v


def advanced(x, y, u, v):
    fy = y + 0.5
    fx = x + 0.5
    w00 = (1.0 - fy) * (1.0 - fx)
    w10 = fy * (1.0 - fx)
    w01 = (1.0 - fy) * fx
    w11 = fy * fx
    new_x = x + DT * (w00 * u[0] + w10 * u[1] + w01 * u[2] + w11 * u[3])
    new_y = y + DT * (w00 * v[0] + w10 * v[1] + w01 * v[2] + w11 * v[3])
    return new_x, new_y


def home_corners(meta, column, across):
    n = meta.shape[0]
    depth = column.shape[0]
    row = meta[:, 8:9]
    last = meta[:, 9:10] == float(across - 1)
    lane = phase((n, 3 * depth), depth)
    pick = jnp.concatenate([one_hot((lane == row) & last), one_hot((lane == row + 1.0) & last)], axis=0)
    both = mm(pick, stack3(column))
    low = both[0:n]
    high = both[n:]
    u = [meta[:, 0:1], meta[:, 1:2], meta[:, 2:3] + low[:, 16:17], meta[:, 3:4] + high[:, 16:17]]
    v = [meta[:, 4:5], meta[:, 5:6], meta[:, 6:7] + low[:, 32:33], meta[:, 7:8] + high[:, 32:33]]
    return u, v


def lane_sum(x):
    return jnp.sum(x, axis=1, keepdims=True)


def pack_body(part_ref, w_ref, meta_ref, mine_ref, left_ref, right_ref, sel_ref, rw_ref, out_ref, across):
    n = w_ref.shape[0]
    bands = out_ref.shape[0] // (4 * CAP + 1)
    meta = meta_ref[...]
    step = 4 * CAP + 1
    w = w_ref[...]
    new_x, new_y = advanced(part_ref[0], part_ref[1], *home_corners(meta, right_ref[...], across))
    left_meta = left_ref[0:n]
    (_, _, u1, u2), (_, _, v1, v2) = home_corners(left_meta, mine_ref[...], across)
    m = [left_meta[:, 16 + i : 17 + i] for i in range(11)]
    left_hh = (m[3] + u1 * m[4] + u2 * m[5] + v1 * m[6] + v2 * m[7]) + (
        u1 * v1 * m[8] + (u1 * v2 + u2 * v1) * m[9] + u2 * v2 * m[10]
    )
    left_lh = (m[0] + u1 * m[1] + u2 * m[2]) - left_hh
    choose = sel_ref[...]
    gy = new_y + 0.5
    gx = new_x + 0.5
    sums = [
        meta[:, 10:11],
        meta[:, 11:12],
        lane_sum(w * (1.0 - gy) * (1.0 - gx)),
        lane_sum(w * gy * (1.0 - gx)),
        lane_sum(w * (1.0 - gy) * gx),
        lane_sum(w * gy * gx),
    ]
    lane = iota((n, 128), 1)
    lane16 = lane - 16.0 * jnp.floor(lane * 0.0625)
    mine = jnp.zeros((n, 128), F32)
    for i, value in enumerate(sums):
        mine = jnp.where(lane16 == float(i), value, mine)
    over = left_meta[:, 11:12] == float(across - 1)
    sums = [
        left_meta[:, 10:11],
        jnp.where(over, left_lh, 0.0),
        jnp.where(over, left_hh, 0.0),
    ]
    theirs = jnp.zeros((n, 128), F32)
    for i, value in enumerate(sums):
        theirs = jnp.where(lane16 == float(8 + i), value, theirs)
    picked = mm(choose, stack3(jnp.concatenate([new_x, new_y, mine], axis=1)))
    for k in range(CAP):
        rows = slice(k * bands, (k + 1) * bands)
        for j, source in ((0, picked), (1, picked), (2, rw_ref), (3, rw_ref)):
            sl = slice(128 * (j % 2), 128 * (j % 2) + 128)
            out_ref[pl.ds(4 * k + j, bands, stride=step), :] = source[rows, sl]
    slot = jnp.concatenate([to_row(left_meta[:, 12:13], n)] * 3, axis=1)
    d4 = iota((bands, 3 * n), 0) * float(CAP)
    theirs_choose = jnp.concatenate([one_hot(d4 + float(k) == slot) for k in range(CAP)], axis=0)
    chosen = picked[:, 256:] + mm(theirs_choose, stack3(theirs))
    lane = iota((bands, 128), 1)
    group = jnp.floor(lane * 0.0625)
    table = jnp.zeros((bands, 128), F32)
    for k in range(CAP):
        table = jnp.where(group == float(k), chosen[k * bands : (k + 1) * bands], table)
    table = table + pltpu.roll(pltpu.roll(table, 1, 0), 64, 1)
    out_ref[pl.ds(4 * CAP, bands, stride=step), :] = table


def side_term(speed, e0, e1, e2, e3, e4, d2, d3):
    ahead = speed > 0.0
    p = jnp.where(ahead, e0, e4)
    q = jnp.where(ahead, e1, e3)
    s = jnp.where(ahead, e3, e1)
    c = jnp.where(ahead, d2, d3)
    r = e2
    rr = r * r
    t1 = p * (4.0 * p - 11.0 * q) + (10.0 * (q * q) + 3e-6)
    t2 = q * (4.0 * q - 5.0 * r) + (4.0 * rr + 3e-6)
    t3 = s * (4.0 * s - 11.0 * r) + (10.0 * rr + 3e-6)
    a1 = t2 * t3
    a2 = t1 * t3
    a3 = t1 * t2
    w1 = a1 * a1
    w2 = 6.0 * (a2 * a2)
    w3 = 3.0 * (a3 * a3)
    top = w1 * (2.0 * p - 5.0 * q) - w2 * (q + 2.0 * r) + w3 * (s - 4.0 * r)
    return speed * c + jnp.abs(speed) * (top / (6.0 * (w1 + w2 + w3)))


def stencil_body(f_ref, flow_ref, below_ref, above_ref, right_ref, left_ref, right2_ref, left2_ref, out_ref, f0, us, vs, f1, f2):
    height, across = f_ref.shape
    width = across + 128
    tiles = width // 128
    off = 16
    span = height + 32
    halos = halo_tiles(right_ref[...], left_ref[...])
    uppers = halo_tiles(right2_ref[...], left2_ref[...])
    owns = (f_ref, flow_ref.at[0], flow_ref.at[1])
    for buf, own, halo, upper, start, count in zip((f0, us, vs), owns, halos, uppers, (0, 9, 15), (9, 6, 6)):
        for j in range(tiles):
            sl = slice(128 * j, 128 * j + 128)
            top = span * j + off
            if j < tiles - 1:
                buf[top : top + height, :] = own[:, sl]
                buf[top + height : top + height + count, :] = below_ref[start : start + count, sl]
                buf[top - count : top, :] = above_ref[start : start + count, sl]
            else:
                buf[top : top + height + count, :] = halo[0 : height + count]
                buf[top - count : top, :] = upper[0:count]

    lane = lax.broadcasted_iota(jnp.int32, (8, 128), 1)

    def stage(src, dst_tiles, base, write):
        f = [src[pl.ds(span * j + base, 8), :] for j in range(tiles)]

        def shifted(k):
            turned = [pltpu.roll(t, (-k) % 128, 1) for t in f]
            if k > 0:
                return [jnp.where(lane < 128 - k, turned[j], turned[(j + 1) % tiles]) for j in range(dst_tiles)]
            return [jnp.where(lane >= -k, turned[j], turned[(j - 1) % tiles]) for j in range(dst_tiles)]

        near = {k: f if k == 0 else shifted(k) for k in range(-3, 4)}
        for j in range(dst_tiles):
            at = span * j + base
            u = us[pl.ds(at, 8), :]
            v = vs[pl.ds(at, 8), :]
            d = [near[k + 1][j] - near[k][j] for k in range(-3, 3)]
            e = [d[k] - d[k + 1] for k in range(5)]
            x_term = side_term(u, e[0], e[1], e[2], e[3], e[4], d[2], d[3])
            rows = [f[j] if k == 0 else src[pl.ds(at + k, 8), :] for k in range(-3, 4)]
            d = [rows[k + 1] - rows[k] for k in range(6)]
            e = [d[k] - d[k + 1] for k in range(5)]
            y_term = side_term(v, e[0], e[1], e[2], e[3], e[4], d[2], d[3])
            write(j, f[j] - DT * (x_term + y_term))

    def first(i, carry):
        base = pl.multiple_of(i * 8 + 8, 8)

        def write(j, value):
            f1[pl.ds(span * j + base, 8), :] = value

        stage(f0, tiles, base, write)
        return carry

    def second(i, carry):
        base = pl.multiple_of(i * 8 + 8, 8)

        def write(j, value):
            at = pl.ds(span * j + base, 8)
            f2[at, :] = 0.75 * f0[at, :] + 0.25 * value

        stage(f1, tiles, base, write)
        return carry

    def third(i, carry):
        base = pl.multiple_of(i * 8 + 16, 8)
        place = pl.multiple_of(i * 8, 8)

        def write(j, value):
            kept = f0[pl.ds(span * j + base, 8), :]
            out_ref[pl.ds(place, 8), 128 * j : 128 * j + 128] = kept * (1.0 / 3.0) + (2.0 / 3.0) * value

        stage(f2, tiles - 1, base, write)
        return carry

    lax.fori_loop(0, height // 8 + 2, first, 0, unroll=2)
    lax.fori_loop(0, height // 8 + 2, second, 0, unroll=2)
    lax.fori_loop(0, height // 8, third, 0, unroll=2)


def deposit_body(rows_ref, recv_ref, base_ref, out_ref, moved_ref, sem):
    height, across = base_ref.shape
    step = 4 * CAP + 1
    bands = recv_ref.shape[0] // step
    block = 4 * CAP
    copy = pltpu.make_async_copy(rows_ref.at[:, pl.ds(0, block)], moved_ref, sem)
    copy.start()
    table = recv_ref[pl.ds(block, bands, stride=step), :]
    lanes = iota((bands, across), 1)
    lane = iota((bands, 128), 1)
    rows = iota((height, 2 * CAP * bands), 0)
    spreads, values, spread_rows, value_rows = [], [], [], []
    first_row = jnp.zeros((bands, across), F32)
    corner = jnp.zeros((bands, 1), F32)

    def two(x):
        hi = x.astype(BF16)
        return hi, (x - hi.astype(F32)).astype(BF16)

    for k in range(CAP):
        o = 16 * k
        part = [table[:, o + i : o + i + 1] for i in range(11)]
        row, col, ll, hl, lh, hh = part[0:6]
        at0 = lanes == col
        at1 = lanes == col + 1.0
        spread = jnp.concatenate(
            [
                jnp.where(at0, ll, 0.0) + jnp.where(at1, lh, 0.0),
                jnp.where(at0, hl, 0.0) + jnp.where(at1, hh, 0.0),
            ],
            axis=1,
        )
        spreads += two(spread)
        spread_rows += [to_row(row, bands)] * 2
        values += two(jnp.where(lane == 0.0, part[9], jnp.where(lane == 1.0, part[10], 0.0)))
        value_rows += [to_row(part[8], bands)] * 2
        o = 64 + 16 * k
        part = [table[:, o + i : o + i + 1] for i in range(11)]
        row, col, ll, hl, lh, hh = part[0:6]
        edge = row == float(height - 1)
        first_row = (
            first_row
            + jnp.where((lanes == col) & edge, hl, 0.0)
            + jnp.where((lanes == col + 1.0) & edge, hh, 0.0)
        )
        corner = corner + jnp.where(part[8] == float(height - 1), part[10], 0.0)
    total = mm(one_hot(rows == jnp.concatenate(spread_rows, axis=1)), jnp.concatenate(spreads, axis=0))
    side = mm(one_hot(rows == jnp.concatenate(value_rows, axis=1)), jnp.concatenate(values, axis=0))
    same = total[:, 0:across]
    down = pltpu.roll(total[:, across:], 1, 0)
    side_down = pltpu.roll(side, 1, 0)
    r = iota((height, across), 0)
    c = iota((height, across), 1)
    incoming = jnp.sum(first_row, axis=0, keepdims=True)
    incoming = incoming + jnp.where(iota((1, across), 1) == 0.0, jnp.sum(corner), 0.0)
    down = jnp.where(r == 0.0, incoming, down)
    column = side[:, 0:1] + jnp.where(iota((height, 1), 0) == 0.0, 0.0, side_down[:, 1:2])
    out_ref[...] = base_ref[...] + (same + down + jnp.where(c == 0.0, column, 0.0))
    copy.wait()


def ring(axis, distance):
    n = lax.axis_size(axis)
    return [(i, (i + distance) % n) for i in range(n)]


def shards(level_set, velocity, particles, escaped, home_cell, land_cell, dest_rank, block_count):
    height, across = level_set.shape
    n = particles.shape[0]
    bands = lax.axis_size("gy")
    step = 4 * CAP + 1
    sds = jax.ShapeDtypeStruct
    head, tail = call(
        heads_body,
        (sds((24, across), F32), sds((24, across), F32)),
        pltpu.with_memory_space_constraint(level_set, pltpu.HBM),
        pltpu.with_memory_space_constraint(velocity, pltpu.HBM),
        spaces=[pltpu.HBM, pltpu.HBM],
        scratch=[pltpu.VMEM((2, 16, across), F32), pltpu.VMEM((2, 2, 8, across), F32), pltpu.SemaphoreType.DMA((4,))],
    )
    below = lax.ppermute(head, "gy", ring("gy", -1))
    above = lax.ppermute(tail, "gy", ring("gy", 1))
    parts = jnp.transpose(particles, (1, 0, 2))
    meta, weight, select, fixed = call(
        prepare_body,
        (
            sds((n, 128), F32),
            sds((n, 128), F32),
            sds((bands * CAP, 3 * n), BF16),
            sds((bands * CAP, 256), F32),
        ),
        velocity, parts, escaped, home_cell.reshape(1, n), land_cell.reshape(1, n), dest_rank.reshape(1, n),
        scalars=(block_count,),
    )
    to_left, to_right, meta = call(
        edges_body,
        (sds((height + 16, 128), F32), sds((height + 16, 128), F32), sds((n, 128), F32)),
        level_set, velocity, below, meta, parts, weight,
    )
    from_left = lax.ppermute(to_right, "gx", ring("gx", 1))
    from_right = lax.ppermute(to_left, "gx", ring("gx", -1))
    (packed,) = call(
        functools.partial(pack_body, across=across),
        (sds((bands * step, 128), F32),),
        parts, weight, meta, to_left, from_left, from_right, select, fixed,
    )
    arrived = lax.all_to_all(
        packed.reshape(bands * step, 1, 128), "gy", split_axis=0, concat_axis=0, tiled=True
    )
    to_left2, to_right2 = call(corners_body, (sds((16, 128), F32), sds((16, 128), F32)), above)
    from_left2 = lax.ppermute(to_right2, "gx", ring("gx", 1))
    from_right2 = lax.ppermute(to_left2, "gx", ring("gx", -1))
    wide = pltpu.VMEM(((across // 128 + 1) * (height + 32), 128), F32)
    (section,) = call(
        stencil_body,
        (sds((height, across), F32),),
        level_set, velocity, below, above, from_right, from_left, from_right2, from_left2,
        scratch=[wide] * 5,
    )
    level, moved = call(
        deposit_body,
        (sds((height, across), F32), sds((bands, 4 * CAP, 1, 128), F32)),
        arrived.reshape(bands, step, 1, 128), arrived.reshape(bands * step, 128), section,
        out_spaces=[pltpu.VMEM, pltpu.HBM],
        scratch=[pltpu.SemaphoreType.DMA],
    )
    return level, moved.reshape(bands * CAP, 4, 128)


def solution(mesh):
    in_specs = (
        P("gy", "gx"),
        P(None, "gy", "gx"),
        P(("gy", "gx"), None, None),
        P(("gy", "gx"), None),
        P(("gy", "gx")),
        P(("gy", "gx")),
        P(("gy", "gx")),
        P(("gy", "gx")),
    )
    out_specs = (P("gy", "gx"), P(("gy", "gx"), None, None))
    return jax.shard_map(shards, mesh=mesh, in_specs=in_specs, out_specs=out_specs, check_vma=False)
```

```python
import functools
import jax
import jax.numpy as jnp
from jax import lax
from jax.experimental import pallas as pl
from jax.experimental.pallas import tpu as pltpu
from jax.sharding import PartitionSpec as P

CAP = 4
DT = 0.3
INTERPRET = False
F32 = jnp.float32
BF16 = jnp.bfloat16


def iota(shape, dim):
    return lax.broadcasted_iota(jnp.int32, shape, dim).astype(F32)


def split3(x):
    hi = x.astype(BF16)
    rest = x - hi.astype(F32)
    mid = rest.astype(BF16)
    lo = (rest - mid.astype(F32)).astype(BF16)
    return hi, mid, lo


def mm(a, b):
    return lax.dot_general(a, b, (((1,), (0,)), ((), ())), preferred_element_type=F32)


def stack3(x):
    return jnp.concatenate(split3(x), axis=0)


def phase(shape, period):
    lane = iota(shape, 1)
    return lane - period * floor_div(lane, period)


def eye(n):
    return iota((n, n), 0) == iota((n, n), 1)


def to_column(row, n):
    return jnp.sum(jnp.where(eye(n), jnp.broadcast_to(row, (n, n)), 0.0), axis=1, keepdims=True)


def to_row(col, n):
    return jnp.sum(jnp.where(eye(n), jnp.broadcast_to(col, (n, n)), 0.0), axis=0, keepdims=True)


def one_hot(mask):
    return jnp.where(mask, 1.0, 0.0).astype(BF16)


def floor_div(x, k):
    return jnp.floor((x + 0.5) * (1.0 / k))


def call(body, outs, *args, scratch=(), spaces=None, out_spaces=None, scalars=()):
    vm, sm = pltpu.VMEM, pltpu.SMEM
    spaces = spaces or [vm] * len(args)
    out_spaces = out_spaces or [vm] * len(outs)
    spec = lambda space: pl.BlockSpec(memory_space=space)
    return pl.pallas_call(
        body,
        out_shape=tuple(outs),
        in_specs=[spec(sm)] * len(scalars) + [spec(x) for x in spaces],
        out_specs=tuple(spec(x) for x in out_spaces),
        scratch_shapes=list(scratch),
        compiler_params=pltpu.CompilerParams(vmem_limit_bytes=16 * 1024 * 1024),
        interpret=INTERPRET,
    )(*scalars, *args)


def heads_body(f_ref, flow_ref, head_ref, f_rows, flow_rows, sems):
    copies = [
        pltpu.make_async_copy(f_ref.at[pl.ds(0, 24)], f_rows, sems.at[0]),
        pltpu.make_async_copy(flow_ref.at[:, pl.ds(0, 16)], flow_rows, sems.at[1]),
    ]
    for copy in copies:
        copy.start()
    for copy in copies:
        copy.wait()
    head_ref[0:18] = f_rows[0:18]
    head_ref[18:33] = flow_rows[0, 0:15]
    head_ref[33:48] = flow_rows[1, 0:15]


def prepare_body(count_ref, flow_ref, part_ref, esc_ref, home_ref, land_ref, dest_ref, meta_ref, w_ref, sel_ref, rw_ref):
    n = esc_ref.shape[0]
    height, across = flow_ref.shape[1:]
    home = to_column(home_ref[...].astype(F32), n)
    land = to_column(land_ref[...].astype(F32), n)
    dest_row = dest_ref[...].astype(F32)
    dest = to_column(dest_row, n)
    count = count_ref[0].astype(F32)
    row = floor_div(home, across)
    col = home - row * across
    land_row = floor_div(land, across)
    land_col = land - land_row * across
    other = iota((n, n), 0)
    mine = iota((n, n), 1)
    same = (dest == dest_row) & (other < mine) & (other < count)
    rank_row = jnp.sum(jnp.where(same, 1.0, 0.0), axis=0, keepdims=True)
    live_row = iota((1, n), 1) < count
    slot_row = jnp.where(live_row, dest_row * CAP + rank_row, -1.0)
    slot = to_column(slot_row, n)
    lane = phase((n, 3 * height), height)
    pick = jnp.concatenate([one_hot(lane == row), one_hot(lane == row + 1.0)], axis=0)
    lanes = iota((n, across), 1)
    at0 = lanes == col
    at1 = lanes == col + 1.0
    parts = []
    for component in range(2):
        both = mm(pick, stack3(flow_ref[component]))
        low = both[0:n]
        high = both[n:]
        for where_at in (at0, at1):
            for rows in (low, high):
                parts.append(jnp.sum(jnp.where(where_at, rows, 0.0), axis=1, keepdims=True))
    columns = parts + [row, col, land_row, land_col, slot]
    lane = iota((n, 128), 1)
    meta = jnp.zeros((n, 128), F32)
    for i, value in enumerate(columns):
        meta = jnp.where(lane == float(i), value, meta)
    meta_ref[...] = meta
    w = esc_ref[...].astype(F32) * part_ref[2]
    w_ref[...] = w
    slots = sel_ref.shape[0]
    bands = slots // CAP
    r = iota((slots, 1), 0)
    k = floor_div(r, bands)
    choose = one_hot((r - k * bands) * CAP + k == jnp.concatenate([slot_row] * 3, axis=1))
    sel_ref[...] = choose
    rw_ref[...] = mm(choose, stack3(jnp.concatenate([part_ref[2], w], axis=1)))


def pack_left(f, u, v):
    lane = iota(f.shape, 1)
    return jnp.where(lane < 16.0, f, jnp.where(lane < 32.0, pltpu.roll(u, 16, 1), pltpu.roll(v, 32, 1)))


def pack_right(f, u, v, m):
    lane = iota(f.shape, 1)
    out = jnp.where(lane >= 112.0, f, jnp.where(lane >= 96.0, pltpu.roll(u, 112, 1), pltpu.roll(v, 96, 1)))
    return jnp.where(lane < 32.0, m, out)


def edges_body(f_ref, flow_ref, below_ref, meta_ref, part_ref, w_ref, left_ref, right_ref, meta2_ref):
    n = w_ref.shape[0]
    height, across = f_ref.shape
    meta = meta_ref[...]
    lane = iota((n, 128), 1)
    row = meta[:, 8:9]
    col = meta[:, 9:10]
    last = row == float(height - 1)
    lanes = iota((n, across), 1)
    at0 = (lanes == col) & last
    at1 = (lanes == col + 1.0) & last
    for base, r in ((0, 18), (4, 33)):
        line = jnp.broadcast_to(below_ref[r : r + 1, :], (n, across))
        c10 = jnp.sum(jnp.where(at0, line, 0.0), axis=1, keepdims=True)
        c11 = jnp.sum(jnp.where(at1, line, 0.0), axis=1, keepdims=True)
        meta = meta + jnp.where(lane == float(base + 1), c10, 0.0) + jnp.where(lane == float(base + 3), c11, 0.0)
    meta2_ref[...] = meta
    x = part_ref[0]
    y = part_ref[1]
    w = w_ref[...]
    fy = y + 0.5
    fx = x + 0.5
    near0 = (1.0 - fy) * (1.0 - fx)
    near1 = fy * (1.0 - fx)
    gx = fx + DT * (near0 * meta[:, 0:1] + near1 * meta[:, 1:2])
    gy = fy + DT * (near0 * meta[:, 4:5] + near1 * meta[:, 5:6])
    e1 = DT * ((1.0 - fy) * fx)
    e2 = DT * (fy * fx)
    wgx, wgy, w1, w2 = w * gx, w * gy, w * e1, w * e2
    moments = [wgx, w1, w2, wgx * gy, wgy * e1, wgy * e2, wgx * e1, wgx * e2, w1 * e1, w1 * e2, w2 * e2]
    sent = meta
    for i, value in enumerate(moments):
        sent = jnp.where(lane == float(16 + i), lane_sum(value), sent)
    far = across - 128

    zero = jnp.zeros((8, 128), F32)

    def pieces(sl):
        yield 0, height, f_ref[:, sl], flow_ref[0, :, sl], flow_ref[1, :, sl], sent
        last = pltpu.roll(below_ref[40:48, sl], 7, 0)
        yield height, 8, below_ref[0:8, sl], below_ref[18:26, sl], below_ref[33:41, sl], zero
        yield height + 8, 8, below_ref[8:16, sl], below_ref[26:34, sl], last, zero
        yield height + 16, 8, below_ref[16:24, sl], zero, zero, zero

    for top, rows, f, u, v, _ in pieces(slice(0, 128)):
        left_ref[top : top + rows] = pack_left(f, u, v)
    for top, rows, f, u, v, m in pieces(slice(far, across)):
        right_ref[top : top + rows] = pack_right(f, u, v, m)


def halo_tiles(from_right, from_left):
    lane = iota(from_right.shape, 1)
    right_side = lane < 64.0
    f = jnp.where(right_side, from_right, from_left)
    u = jnp.where(right_side, pltpu.roll(from_right, 112, 1), pltpu.roll(from_left, 16, 1))
    v = jnp.where(right_side, pltpu.roll(from_right, 96, 1), pltpu.roll(from_left, 32, 1))
    return f, u, v


def advanced(x, y, u, v):
    fy = y + 0.5
    fx = x + 0.5
    w00 = (1.0 - fy) * (1.0 - fx)
    w10 = fy * (1.0 - fx)
    w01 = (1.0 - fy) * fx
    w11 = fy * fx
    new_x = x + DT * (w00 * u[0] + w10 * u[1] + w01 * u[2] + w11 * u[3])
    new_y = y + DT * (w00 * v[0] + w10 * v[1] + w01 * v[2] + w11 * v[3])
    return new_x, new_y


def home_corners(meta, column, across):
    n = meta.shape[0]
    depth = column.shape[0]
    row = meta[:, 8:9]
    last = meta[:, 9:10] == float(across - 1)
    lane = phase((n, 3 * depth), depth)
    pick = jnp.concatenate([one_hot((lane == row) & last), one_hot((lane == row + 1.0) & last)], axis=0)
    both = mm(pick, stack3(column))
    low = both[0:n]
    high = both[n:]
    u = [meta[:, 0:1], meta[:, 1:2], meta[:, 2:3] + low[:, 16:17], meta[:, 3:4] + high[:, 16:17]]
    v = [meta[:, 4:5], meta[:, 5:6], meta[:, 6:7] + low[:, 32:33], meta[:, 7:8] + high[:, 32:33]]
    return u, v


def lane_sum(x):
    return jnp.sum(x, axis=1, keepdims=True)


def pack_body(part_ref, w_ref, meta_ref, mine_ref, left_ref, right_ref, sel_ref, rw_ref, out_ref, height, across):
    n = w_ref.shape[0]
    bands = out_ref.shape[0] // (4 * CAP + 1)
    meta = meta_ref[...]
    step = 4 * CAP + 1
    w = w_ref[...]
    new_x, new_y = advanced(part_ref[0], part_ref[1], *home_corners(meta, right_ref[0 : height + 8], across))
    left_meta = left_ref[0:n]
    (_, _, u1, u2), (_, _, v1, v2) = home_corners(left_meta, mine_ref[0 : height + 8], across)
    m = [left_meta[:, 16 + i : 17 + i] for i in range(11)]
    left_hh = (m[3] + u1 * m[4] + u2 * m[5] + v1 * m[6] + v2 * m[7]) + (
        u1 * v1 * m[8] + (u1 * v2 + u2 * v1) * m[9] + u2 * v2 * m[10]
    )
    left_lh = (m[0] + u1 * m[1] + u2 * m[2]) - left_hh
    choose = sel_ref[...]
    gy = new_y + 0.5
    gx = new_x + 0.5
    sums = [
        meta[:, 10:11],
        meta[:, 11:12],
        lane_sum(w * (1.0 - gy) * (1.0 - gx)),
        lane_sum(w * gy * (1.0 - gx)),
        lane_sum(w * (1.0 - gy) * gx),
        lane_sum(w * gy * gx),
    ]
    lane = iota((n, 128), 1)
    lane16 = lane - 16.0 * jnp.floor(lane * 0.0625)
    mine = jnp.zeros((n, 128), F32)
    for i, value in enumerate(sums):
        mine = jnp.where(lane16 == float(i), value, mine)
    over = left_meta[:, 11:12] == float(across - 1)
    sums = [
        left_meta[:, 10:11],
        jnp.where(over, left_lh, 0.0),
        jnp.where(over, left_hh, 0.0),
    ]
    theirs = jnp.zeros((n, 128), F32)
    for i, value in enumerate(sums):
        theirs = jnp.where(lane16 == float(8 + i), value, theirs)
    picked = mm(choose, stack3(jnp.concatenate([new_x, new_y, mine], axis=1)))
    for k in range(CAP):
        rows = slice(k * bands, (k + 1) * bands)
        for j, source in ((0, picked), (1, picked), (2, rw_ref), (3, rw_ref)):
            sl = slice(128 * (j % 2), 128 * (j % 2) + 128)
            out_ref[pl.ds(4 * k + j, bands, stride=step), :] = source[rows, sl]
    slot = jnp.concatenate([to_row(left_meta[:, 12:13], n)] * 3, axis=1)
    d4 = iota((bands, 3 * n), 0) * float(CAP)
    theirs_choose = jnp.concatenate([one_hot(d4 + float(k) == slot) for k in range(CAP)], axis=0)
    chosen = picked[:, 256:] + mm(theirs_choose, stack3(theirs))
    lane = iota((bands, 128), 1)
    group = jnp.floor(lane * 0.0625)
    table = jnp.zeros((bands, 128), F32)
    for k in range(CAP):
        table = jnp.where(group == float(k), chosen[k * bands : (k + 1) * bands], table)
    table = table + pltpu.roll(pltpu.roll(table, 1, 0), 64, 1)
    out_ref[pl.ds(4 * CAP, bands, stride=step), :] = table


def side_term(speed, e0, e1, e2, e3, e4, d2, d3):
    ahead = speed > 0.0
    p = jnp.where(ahead, e0, e4)
    q = jnp.where(ahead, e1, e3)
    s = jnp.where(ahead, e3, e1)
    c = jnp.where(ahead, d2, d3)
    r = e2
    rr = r * r
    t1 = p * (4.0 * p - 11.0 * q) + (10.0 * (q * q) + 3e-6)
    t2 = q * (4.0 * q - 5.0 * r) + (4.0 * rr + 3e-6)
    t3 = s * (4.0 * s - 11.0 * r) + (10.0 * rr + 3e-6)
    a1 = t2 * t3
    a2 = t1 * t3
    a3 = t1 * t2
    w1 = a1 * a1
    w2 = 6.0 * (a2 * a2)
    w3 = 3.0 * (a3 * a3)
    top = w1 * (2.0 * p - 5.0 * q) - w2 * (q + 2.0 * r) + w3 * (s - 4.0 * r)
    return speed * c + jnp.abs(speed) * (top / (6.0 * (w1 + w2 + w3)))


def stencil_body(f_ref, flow_ref, below_ref, right_ref, left_ref, out_ref, next_ref, f0, us, vs, f1, f2):
    height, across = f_ref.shape
    tiles = across // 128 + 1
    span = height + 24
    halos = halo_tiles(right_ref[...], left_ref[...])
    owns = (f_ref, flow_ref.at[0], flow_ref.at[1])
    for buf, own, halo, start, count in zip((f0, us, vs), owns, halos, (0, 18, 33), (18, 15, 15)):
        for j in range(tiles - 1):
            sl = slice(128 * j, 128 * j + 128)
            buf[span * j : span * j + height, :] = own[:, sl]
            buf[span * j + height : span * j + height + count, :] = below_ref[start : start + count, sl]
        buf[span * (tiles - 1) : span * tiles, :] = halo

    lane = lax.broadcasted_iota(jnp.int32, (8, 128), 1)

    def stage(src, dst_tiles, base, write):
        f = [src[pl.ds(span * j + base, 8), :] for j in range(tiles)]

        def shifted(k):
            turned = [pltpu.roll(t, (-k) % 128, 1) for t in f]
            if k > 0:
                return [jnp.where(lane < 128 - k, turned[j], turned[(j + 1) % tiles]) for j in range(dst_tiles)]
            return [jnp.where(lane >= -k, turned[j], turned[(j - 1) % tiles]) for j in range(dst_tiles)]

        near = {k: f if k == 0 else shifted(k) for k in range(-3, 4)}
        for j in range(dst_tiles):
            at = span * j + base
            u = us[pl.ds(at, 8), :]
            v = vs[pl.ds(at, 8), :]
            d = [near[k + 1][j] - near[k][j] for k in range(-3, 3)]
            e = [d[k] - d[k + 1] for k in range(5)]
            x_term = side_term(u, e[0], e[1], e[2], e[3], e[4], d[2], d[3])
            rows = [f[j] if k == 0 else src[pl.ds(at + k, 8), :] for k in range(-3, 4)]
            d = [rows[k + 1] - rows[k] for k in range(6)]
            e = [d[k] - d[k + 1] for k in range(5)]
            y_term = side_term(v, e[0], e[1], e[2], e[3], e[4], d[2], d[3])
            write(j, f[j] - DT * (x_term + y_term))

    def first(i, carry):
        base = i * 8 + 3

        def write(j, value):
            f1[pl.ds(span * j + base, 8), :] = value

        stage(f0, tiles, base, write)
        return carry

    def second(i, carry):
        base = i * 8 + 6

        def write(j, value):
            at = pl.ds(span * j + base, 8)
            f2[at, :] = 0.75 * f0[at, :] + 0.25 * value

        stage(f1, tiles, base, write)
        return carry

    def third(i, carry):
        base = i * 8 + 9

        def write(j, value):
            at = pl.ds(span * j + base, 8)
            out_ref[at, :] = f0[at, :] * (1.0 / 3.0) + (2.0 / 3.0) * value

        stage(f2, tiles - 1, base, write)
        return carry

    lax.fori_loop(0, height // 8 + 2, first, 0, unroll=2)
    lax.fori_loop(0, height // 8 + 1, second, 0, unroll=3)
    lax.fori_loop(0, height // 8, third, 0, unroll=2)
    for j in range(tiles - 1):
        next_ref[16 * j : 16 * j + 16] = out_ref[span * j + height : span * j + height + 16]


def deposit_body(rows_ref, recv_ref, base_ref, first_ref, out_ref, moved_ref, sem):
    height, across = out_ref.shape
    step = 4 * CAP + 1
    bands = recv_ref.shape[0] // step
    block = 4 * CAP
    copy = pltpu.make_async_copy(rows_ref.at[:, pl.ds(0, block)], moved_ref, sem)
    copy.start()
    table = recv_ref[pl.ds(block, bands, stride=step), :]
    lanes = iota((bands, across), 1)
    lane = iota((bands, 128), 1)
    rows = iota((height, 2 * CAP * bands), 0)
    spreads, values, spread_rows, value_rows = [], [], [], []
    first_row = jnp.zeros((bands, across), F32)
    corner = jnp.zeros((bands, 1), F32)

    def two(x):
        hi = x.astype(BF16)
        return hi, (x - hi.astype(F32)).astype(BF16)

    for k in range(CAP):
        o = 16 * k
        part = [table[:, o + i : o + i + 1] for i in range(11)]
        row, col, ll, hl, lh, hh = part[0:6]
        at0 = lanes == col
        at1 = lanes == col + 1.0
        spread = jnp.concatenate(
            [
                jnp.where(at0, ll, 0.0) + jnp.where(at1, lh, 0.0),
                jnp.where(at0, hl, 0.0) + jnp.where(at1, hh, 0.0),
            ],
            axis=1,
        )
        spreads += two(spread)
        spread_rows += [to_row(row, bands)] * 2
        values += two(jnp.where(lane == 0.0, part[9], jnp.where(lane == 1.0, part[10], 0.0)))
        value_rows += [to_row(part[8], bands)] * 2
        o = 64 + 16 * k
        part = [table[:, o + i : o + i + 1] for i in range(11)]
        row, col, ll, hl, lh, hh = part[0:6]
        edge = row == float(height - 1)
        first_row = (
            first_row
            + jnp.where((lanes == col) & edge, hl, 0.0)
            + jnp.where((lanes == col + 1.0) & edge, hh, 0.0)
        )
        corner = corner + jnp.where(part[8] == float(height - 1), part[10], 0.0)
    total = mm(one_hot(rows == jnp.concatenate(spread_rows, axis=1)), jnp.concatenate(spreads, axis=0))
    side = mm(one_hot(rows == jnp.concatenate(value_rows, axis=1)), jnp.concatenate(values, axis=0))
    same = total[:, 0:across]
    down = pltpu.roll(total[:, across:], 1, 0)
    side_down = pltpu.roll(side, 1, 0)
    r = iota((height, across), 0)
    c = iota((height, across), 1)
    incoming = jnp.sum(first_row, axis=0, keepdims=True)
    incoming = incoming + jnp.where(iota((1, across), 1) == 0.0, jnp.sum(corner), 0.0)
    down = jnp.where(r == 0.0, incoming, down)
    column = side[:, 0:1] + jnp.where(iota((height, 1), 0) == 0.0, 0.0, side_down[:, 1:2])
    added = same + down + jnp.where(c == 0.0, column, 0.0)
    span = height + 24
    early = iota((16, 128), 0) < 9.0
    for j in range(across // 128):
        sl = slice(128 * j, 128 * j + 128)
        at = span * j
        level = jnp.where(early, first_ref[16 * j : 16 * j + 16], base_ref[at : at + 16])
        out_ref[0:16, sl] = level + added[0:16, sl]
        out_ref[16:, sl] = base_ref[at + 16 : at + height] + added[16:, sl]
    copy.wait()


def ring(axis, distance):
    n = lax.axis_size(axis)
    return [(i, (i + distance) % n) for i in range(n)]


def shards(level_set, velocity, particles, escaped, home_cell, land_cell, dest_rank, block_count):
    height, across = level_set.shape
    n = particles.shape[0]
    bands = lax.axis_size("gy")
    step = 4 * CAP + 1
    sds = jax.ShapeDtypeStruct
    (head,) = call(
        heads_body,
        (sds((48, across), F32),),
        pltpu.with_memory_space_constraint(level_set, pltpu.HBM),
        pltpu.with_memory_space_constraint(velocity, pltpu.HBM),
        spaces=[pltpu.HBM, pltpu.HBM],
        scratch=[pltpu.VMEM((24, across), F32), pltpu.VMEM((2, 16, across), F32), pltpu.SemaphoreType.DMA((2,))],
    )
    below = lax.ppermute(head, "gy", ring("gy", -1))
    parts = jnp.transpose(particles, (1, 0, 2))
    meta, weight, select, fixed = call(
        prepare_body,
        (
            sds((n, 128), F32),
            sds((n, 128), F32),
            sds((bands * CAP, 3 * n), BF16),
            sds((bands * CAP, 256), F32),
        ),
        velocity, parts, escaped, home_cell.reshape(1, n), land_cell.reshape(1, n), dest_rank.reshape(1, n),
        scalars=(block_count,),
    )
    to_left, to_right, meta = call(
        edges_body,
        (sds((height + 24, 128), F32), sds((height + 24, 128), F32), sds((n, 128), F32)),
        level_set, velocity, below, meta, parts, weight,
    )
    from_left = lax.ppermute(to_right, "gx", ring("gx", 1))
    from_right = lax.ppermute(to_left, "gx", ring("gx", -1))
    (packed,) = call(
        functools.partial(pack_body, height=height, across=across),
        (sds((bands * step, 128), F32),),
        parts, weight, meta, to_left, from_left, from_right, select, fixed,
    )
    arrived = lax.all_to_all(
        packed.reshape(bands * step, 1, 128), "gy", split_axis=0, concat_axis=0, tiled=True
    )
    span = height + 24
    wide = pltpu.VMEM(((across // 128 + 1) * span, 128), F32)
    section, ahead = call(
        stencil_body,
        (sds((across // 128 * span, 128), F32), sds((across // 128 * 16, 128), F32)),
        level_set, velocity, below, from_right, from_left,
        scratch=[wide] * 5,
    )
    first_rows = lax.ppermute(ahead, "gy", ring("gy", 1))
    level, moved = call(
        deposit_body,
        (sds((height, across), F32), sds((bands, 4 * CAP, 1, 128), F32)),
        arrived.reshape(bands, step, 1, 128), arrived.reshape(bands * step, 128), section, first_rows,
        out_spaces=[pltpu.VMEM, pltpu.HBM],
        scratch=[pltpu.SemaphoreType.DMA],
    )
    return level, moved.reshape(bands * CAP, 4, 128)


def solution(mesh):
    in_specs = (
        P("gy", "gx"),
        P(None, "gy", "gx"),
        P(("gy", "gx"), None, None),
        P(("gy", "gx"), None),
        P(("gy", "gx")),
        P(("gy", "gx")),
        P(("gy", "gx")),
        P(("gy", "gx")),
    )
    out_specs = (P("gy", "gx"), P(("gy", "gx"), None, None))
    return jax.shard_map(shards, mesh=mesh, in_specs=in_specs, out_specs=out_specs, check_vma=False)
```

```python
import functools
import jax
import jax.numpy as jnp
from jax import lax
from jax.experimental import pallas as pl
from jax.experimental.pallas import tpu as pltpu
from jax.sharding import PartitionSpec as P

CAP = 4
DT = 0.3
INTERPRET = False
F32 = jnp.float32
BF16 = jnp.bfloat16


def iota(shape, dim):
    return lax.broadcasted_iota(jnp.int32, shape, dim).astype(F32)


def split3(x):
    hi = x.astype(BF16)
    rest = x - hi.astype(F32)
    mid = rest.astype(BF16)
    lo = (rest - mid.astype(F32)).astype(BF16)
    return hi, mid, lo


def mm(a, b):
    return lax.dot_general(a, b, (((1,), (0,)), ((), ())), preferred_element_type=F32)


def stack3(x):
    return jnp.concatenate(split3(x), axis=0)


def phase(shape, period):
    lane = iota(shape, 1)
    return lane - period * floor_div(lane, period)


def eye(n):
    return iota((n, n), 0) == iota((n, n), 1)


def to_column(row, n):
    return jnp.sum(jnp.where(eye(n), jnp.broadcast_to(row, (n, n)), 0.0), axis=1, keepdims=True)


def one_hot(mask):
    return jnp.where(mask, 1.0, 0.0).astype(BF16)


def floor_div(x, k):
    return jnp.floor((x + 0.5) * (1.0 / k))


def call(body, outs, *args, scratch=(), spaces=None, out_spaces=None, scalars=()):
    vm, sm = pltpu.VMEM, pltpu.SMEM
    spaces = spaces or [vm] * len(args)
    out_spaces = out_spaces or [vm] * len(outs)
    spec = lambda space: pl.BlockSpec(memory_space=space)
    return pl.pallas_call(
        body,
        out_shape=tuple(outs),
        in_specs=[spec(sm)] * len(scalars) + [spec(x) for x in spaces],
        out_specs=tuple(spec(x) for x in out_spaces),
        scratch_shapes=list(scratch),
        compiler_params=pltpu.CompilerParams(vmem_limit_bytes=16 * 1024 * 1024),
        interpret=INTERPRET,
    )(*scalars, *args)


def heads_body(f_ref, flow_ref, head_ref, f_rows, flow_rows, sems):
    copies = [
        pltpu.make_async_copy(f_ref.at[pl.ds(0, 24)], f_rows, sems.at[0]),
        pltpu.make_async_copy(flow_ref.at[:, pl.ds(0, 16)], flow_rows, sems.at[1]),
    ]
    for copy in copies:
        copy.start()
    for copy in copies:
        copy.wait()
    head_ref[0:18] = f_rows[0:18]
    head_ref[18:33] = flow_rows[0, 0:15]
    head_ref[33:48] = flow_rows[1, 0:15]


def advanced(x, y, u, v):
    fy = y + 0.5
    fx = x + 0.5
    w00 = (1.0 - fy) * (1.0 - fx)
    w10 = fy * (1.0 - fx)
    w01 = (1.0 - fy) * fx
    w11 = fy * fx
    new_x = x + DT * (w00 * u[0] + w10 * u[1] + w01 * u[2] + w11 * u[3])
    new_y = y + DT * (w00 * v[0] + w10 * v[1] + w01 * v[2] + w11 * v[3])
    return new_x, new_y


def prepare_body(count_ref, flow_ref, part_ref, esc_ref, home_ref, land_ref, dest_ref, meta_ref, w_ref, x_ref, y_ref, sel_ref, rw_ref):
    n = esc_ref.shape[0]
    height, across = flow_ref.shape[1:]
    home = to_column(home_ref[...].astype(F32), n)
    land = to_column(land_ref[...].astype(F32), n)
    dest_row = dest_ref[...].astype(F32)
    dest = to_column(dest_row, n)
    count = count_ref[0].astype(F32)
    row = floor_div(home, across)
    col = home - row * across
    land_row = floor_div(land, across)
    land_col = land - land_row * across
    other = iota((n, n), 0)
    mine = iota((n, n), 1)
    same = (dest == dest_row) & (other < mine) & (other < count)
    rank_row = jnp.sum(jnp.where(same, 1.0, 0.0), axis=0, keepdims=True)
    live_row = iota((1, n), 1) < count
    slot_row = jnp.where(live_row, dest_row * CAP + rank_row, -1.0)
    slot = to_column(slot_row, n)
    lane = phase((n, 3 * height), height)
    pick = jnp.concatenate([one_hot(lane == row), one_hot(lane == row + 1.0)], axis=0)
    lanes = iota((n, across), 1)
    at0 = lanes == col
    at1 = lanes == col + 1.0
    parts = []
    for component in range(2):
        both = mm(pick, stack3(flow_ref[component]))
        low = both[0:n]
        high = both[n:]
        for where_at in (at0, at1):
            for rows in (low, high):
                parts.append(jnp.sum(jnp.where(where_at, rows, 0.0), axis=1, keepdims=True))
    x_ref[...], y_ref[...] = advanced(part_ref[0], part_ref[1], parts[0:4], parts[4:8])
    lane = iota((n, 128), 1)
    meta = jnp.zeros((n, 128), F32)
    for i, value in enumerate((row, col, land_row, land_col, slot)):
        meta = jnp.where(lane == float(8 + i), value, meta)
    meta_ref[...] = meta
    w = esc_ref[...].astype(F32) * part_ref[2]
    w_ref[...] = w
    slots = sel_ref.shape[0]
    bands = slots // CAP
    r = iota((slots, 1), 0)
    k = floor_div(r, bands)
    choose = one_hot((r - k * bands) * CAP + k == jnp.concatenate([slot_row] * 3, axis=1))
    sel_ref[...] = choose
    rw_ref[...] = mm(choose, stack3(jnp.concatenate([part_ref[2], w], axis=1)))


def pack_left(f, u, v):
    lane = iota(f.shape, 1)
    return jnp.where(lane < 16.0, f, jnp.where(lane < 32.0, pltpu.roll(u, 16, 1), pltpu.roll(v, 32, 1)))


def pack_right(f, u, v, m):
    lane = iota(f.shape, 1)
    out = jnp.where(lane >= 112.0, f, jnp.where(lane >= 96.0, pltpu.roll(u, 112, 1), pltpu.roll(v, 96, 1)))
    return jnp.where(lane < 32.0, m, out)


def edges_body(f_ref, flow_ref, below_ref, meta_ref, part_ref, w_ref, x_ref, y_ref, left_ref, right_ref, x2_ref, y2_ref):
    n = w_ref.shape[0]
    height, across = f_ref.shape
    meta = meta_ref[...]
    lane = iota((n, 128), 1)
    row = meta[:, 8:9]
    col = meta[:, 9:10]
    last = row == float(height - 1)
    lanes = iota((n, across), 1)
    at0 = (lanes == col) & last
    at1 = (lanes == col + 1.0) & last
    fix = []
    for r in (18, 33):
        line = jnp.broadcast_to(below_ref[r : r + 1, :], (n, across))
        for where_at in (at0, at1):
            fix.append(jnp.sum(jnp.where(where_at, line, 0.0), axis=1, keepdims=True))
    w = w_ref[...]
    fy = part_ref[1] + 0.5
    fx = part_ref[0] + 0.5
    low1 = fy * (1.0 - fx)
    high1 = fy * fx
    new_x = x_ref[...] + DT * (low1 * fix[0] + high1 * fix[1])
    new_y = y_ref[...] + DT * (low1 * fix[2] + high1 * fix[3])
    x2_ref[...] = new_x
    y2_ref[...] = new_y
    gx = new_x + 0.5
    gy = new_y + 0.5
    e1 = DT * ((1.0 - fy) * fx)
    e2 = DT * high1
    wgx, wgy, w1, w2 = w * gx, w * gy, w * e1, w * e2
    moments = [wgx, w1, w2, wgx * gy, wgy * e1, wgy * e2, wgx * e1, wgx * e2, w1 * e1, w1 * e2, w2 * e2]
    sent = meta
    for i, value in enumerate(moments):
        sent = jnp.where(lane == float(16 + i), lane_sum(value), sent)
    far = across - 128

    zero = jnp.zeros((8, 128), F32)

    def pieces(sl):
        yield 0, height, f_ref[:, sl], flow_ref[0, :, sl], flow_ref[1, :, sl], sent
        last = pltpu.roll(below_ref[40:48, sl], 7, 0)
        yield height, 8, below_ref[0:8, sl], below_ref[18:26, sl], below_ref[33:41, sl], zero
        yield height + 8, 8, below_ref[8:16, sl], below_ref[26:34, sl], last, zero
        yield height + 16, 8, below_ref[16:24, sl], zero, zero, zero

    for top, rows, f, u, v, _ in pieces(slice(0, 128)):
        left_ref[top : top + rows] = pack_left(f, u, v)
    for top, rows, f, u, v, m in pieces(slice(far, across)):
        right_ref[top : top + rows] = pack_right(f, u, v, m)


def halo_tiles(from_right, from_left):
    lane = iota(from_right.shape, 1)
    right_side = lane < 64.0
    f = jnp.where(right_side, from_right, from_left)
    u = jnp.where(right_side, pltpu.roll(from_right, 112, 1), pltpu.roll(from_left, 16, 1))
    v = jnp.where(right_side, pltpu.roll(from_right, 96, 1), pltpu.roll(from_left, 32, 1))
    return f, u, v


def right_corners(meta, column, across):
    n = meta.shape[0]
    depth = column.shape[0]
    row = meta[:, 8:9]
    last = meta[:, 9:10] == float(across - 1)
    lane = phase((n, 3 * depth), depth)
    pick = jnp.concatenate([one_hot((lane == row) & last), one_hot((lane == row + 1.0) & last)], axis=0)
    return mm(pick, stack3(column))


def lane_sum(x):
    return jnp.sum(x, axis=1, keepdims=True)


def pack_body(part_ref, w_ref, x_ref, y_ref, meta_ref, mine_ref, left_ref, right_ref, sel_ref, rw_ref, out_ref, across):
    n = w_ref.shape[0]
    bands = out_ref.shape[0] // (4 * CAP + 1)
    depth = right_ref.shape[0] - 16
    meta = meta_ref[...]
    step = 4 * CAP + 1
    w = w_ref[...]
    left_meta = left_ref[0:n]
    both = right_corners(meta, right_ref[0:depth], across)
    left_both = right_corners(left_meta, mine_ref[0:depth], across)
    fy = part_ref[1] + 0.5
    fx = part_ref[0] + 0.5
    e1 = DT * ((1.0 - fy) * fx)
    e2 = DT * (fy * fx)
    new_x = x_ref[...] + (e1 * both[0:n, 16:17] + e2 * both[n:, 16:17])
    new_y = y_ref[...] + (e1 * both[0:n, 32:33] + e2 * both[n:, 32:33])
    gy = new_y + 0.5
    gx = new_x + 0.5
    wy = w * gy
    wo = w - wy
    sums = [
        meta[:, 10:11],
        meta[:, 11:12],
        lane_sum(wo * (1.0 - gx)),
        lane_sum(wy * (1.0 - gx)),
        lane_sum(wo * gx),
        lane_sum(wy * gx),
    ]
    lane = iota((n, 128), 1)
    lane16 = lane - 16.0 * jnp.floor(lane * 0.0625)
    mine = jnp.zeros((n, 128), F32)
    for i, value in enumerate(sums):
        mine = jnp.where(lane16 == float(i), value, mine)
    facts = jnp.transpose(left_meta)
    flows = jnp.transpose(left_both)
    u1, u2 = flows[16:17, 0:n], flows[16:17, n:]
    v1, v2 = flows[32:33, 0:n], flows[32:33, n:]
    m = [facts[16 + i : 17 + i] for i in range(11)]
    hh = (m[3] + u1 * m[4] + u2 * m[5] + v1 * m[6] + v2 * m[7]) + (
        u1 * v1 * m[8] + (u1 * v2 + u2 * v1) * m[9] + u2 * v2 * m[10]
    )
    lh = (m[0] + u1 * m[1] + u2 * m[2]) - hh
    over = facts[11:12] == float(across - 1)
    line = iota((128, n), 0)
    line16 = line - 16.0 * jnp.floor(line * 0.0625)
    theirs = jnp.where(line16 == 8.0, facts[10:11], 0.0)
    theirs = jnp.where(line16 == 9.0, jnp.where(over, lh, 0.0), theirs)
    theirs = jnp.where(line16 == 10.0, jnp.where(over, hh, 0.0), theirs)
    theirs = jnp.transpose(theirs)
    choose = sel_ref[...]
    picked = mm(choose, stack3(jnp.concatenate([new_x, new_y, mine], axis=1)))
    for k in range(CAP):
        rows = slice(k * bands, (k + 1) * bands)
        for j, source in ((0, picked), (1, picked), (2, rw_ref), (3, rw_ref)):
            sl = slice(128 * (j % 2), 128 * (j % 2) + 128)
            out_ref[pl.ds(4 * k + j, bands, stride=step), :] = source[rows, sl]
    slot = jnp.concatenate([facts[12:13]] * 3, axis=1)
    d4 = iota((bands, 3 * n), 0) * float(CAP)
    theirs_choose = jnp.concatenate([one_hot(d4 + float(k) == slot) for k in range(CAP)], axis=0)
    chosen = picked[:, 256:] + mm(theirs_choose, stack3(theirs))
    lane = iota((bands, 128), 1)
    group = jnp.floor(lane * 0.0625)
    table = jnp.zeros((bands, 128), F32)
    for k in range(CAP):
        table = jnp.where(group == float(k), chosen[k * bands : (k + 1) * bands], table)
    table = table + pltpu.roll(pltpu.roll(table, 1, 0), 64, 1)
    out_ref[pl.ds(4 * CAP, bands, stride=step), :] = table


def side_term(speed, e0, e1, e2, e3, e4, d2, d3):
    ahead = speed > 0.0
    p = jnp.where(ahead, e0, e4)
    q = jnp.where(ahead, e1, e3)
    s = jnp.where(ahead, e3, e1)
    c = jnp.where(ahead, d2, d3)
    r = e2
    rr = r * r
    t1 = p * (4.0 * p - 11.0 * q) + (10.0 * (q * q) + 3e-6)
    t2 = q * (4.0 * q - 5.0 * r) + (4.0 * rr + 3e-6)
    t3 = s * (4.0 * s - 11.0 * r) + (10.0 * rr + 3e-6)
    a1 = t2 * t3
    a2 = t1 * t3
    a3 = t1 * t2
    w1 = a1 * a1
    w2 = 6.0 * (a2 * a2)
    w3 = 3.0 * (a3 * a3)
    top = w1 * (2.0 * p - 5.0 * q) - w2 * (q + 2.0 * r) + w3 * (s - 4.0 * r)
    return speed * c + jnp.abs(speed) * (top / (6.0 * (w1 + w2 + w3)))


def stencil_body(f_ref, flow_ref, below_ref, right_ref, left_ref, out_ref, next_ref, f0, us, vs, f1, f2):
    height, across = f_ref.shape
    tiles = across // 128 + 1
    span = height + 24
    halos = halo_tiles(right_ref[...], left_ref[...])
    owns = (f_ref, flow_ref.at[0], flow_ref.at[1])
    for buf, own, halo, start, count in zip((f0, us, vs), owns, halos, (0, 18, 33), (18, 15, 15)):
        for j in range(tiles - 1):
            sl = slice(128 * j, 128 * j + 128)
            buf[span * j : span * j + height, :] = own[:, sl]
            buf[span * j + height : span * j + height + count, :] = below_ref[start : start + count, sl]
        buf[span * (tiles - 1) : span * tiles, :] = halo

    lane = lax.broadcasted_iota(jnp.int32, (8, 128), 1)

    def stage(src, dst_tiles, base, write):
        f = [src[pl.ds(span * j + base, 8), :] for j in range(tiles)]

        def shifted(k):
            turned = [pltpu.roll(t, (-k) % 128, 1) for t in f]
            if k > 0:
                return [jnp.where(lane < 128 - k, turned[j], turned[(j + 1) % tiles]) for j in range(dst_tiles)]
            return [jnp.where(lane >= -k, turned[j], turned[(j - 1) % tiles]) for j in range(dst_tiles)]

        near = {k: f if k == 0 else shifted(k) for k in range(-3, 4)}
        for j in range(dst_tiles):
            at = span * j + base
            u = us[pl.ds(at, 8), :]
            v = vs[pl.ds(at, 8), :]
            d = [near[k + 1][j] - near[k][j] for k in range(-3, 3)]
            e = [d[k] - d[k + 1] for k in range(5)]
            x_term = side_term(u, e[0], e[1], e[2], e[3], e[4], d[2], d[3])
            rows = [f[j] if k == 0 else src[pl.ds(at + k, 8), :] for k in range(-3, 4)]
            d = [rows[k + 1] - rows[k] for k in range(6)]
            e = [d[k] - d[k + 1] for k in range(5)]
            y_term = side_term(v, e[0], e[1], e[2], e[3], e[4], d[2], d[3])
            write(j, f[j] - DT * (x_term + y_term))

    def first(i, carry):
        base = i * 8 + 3

        def write(j, value):
            f1[pl.ds(span * j + base, 8), :] = value

        stage(f0, tiles, base, write)
        return carry

    def second(i, carry):
        base = i * 8 + 6

        def write(j, value):
            at = pl.ds(span * j + base, 8)
            f2[at, :] = 0.75 * f0[at, :] + 0.25 * value

        stage(f1, tiles, base, write)
        return carry

    def third(i, carry):
        base = i * 8 + 9

        def write(j, value):
            at = pl.ds(span * j + base, 8)
            out_ref[at, :] = f0[at, :] * (1.0 / 3.0) + (2.0 / 3.0) * value

        stage(f2, tiles - 1, base, write)
        return carry

    lax.fori_loop(0, height // 8 + 2, first, 0, unroll=2)
    lax.fori_loop(0, height // 8 + 1, second, 0, unroll=3)
    lax.fori_loop(0, height // 8, third, 0, unroll=2)
    for j in range(tiles - 1):
        next_ref[16 * j : 16 * j + 16] = out_ref[span * j + height : span * j + height + 16]


def deposit_body(rows_ref, recv_ref, base_ref, first_ref, out_ref, moved_ref, sem):
    height, across = out_ref.shape
    step = 4 * CAP + 1
    bands = recv_ref.shape[0] // step
    block = 4 * CAP
    copy = pltpu.make_async_copy(rows_ref.at[:, pl.ds(0, block)], moved_ref, sem)
    copy.start()
    table = recv_ref[pl.ds(block, bands, stride=step), :]
    turned = jnp.transpose(table)
    count = CAP * bands

    def line(first, i):
        return jnp.concatenate([turned[first + 16 * k + i : first + 16 * k + i + 1] for k in range(CAP)], axis=1)

    r = iota((height, count), 0)
    row, col, ll, hl, lh, hh = [line(0, i) for i in range(6)]
    inside = col < float(across - 1)
    at, under = r == row, r == row + 1.0
    low = jnp.where(at, ll, jnp.where(under, hl, 0.0))
    high = jnp.where(inside & at, lh, jnp.where(inside & under, hh, 0.0))
    row, lh, hh = [line(0, 8 + i) for i in range(3)]
    side = jnp.where(r == row, lh, jnp.where(r == row + 1.0, hh, 0.0))
    row, col, _, hl, _, hh = [line(64, i) for i in range(6)]
    top = (r == 0.0) & (row == float(height - 1))
    low = jnp.concatenate([low, jnp.where(top, hl, 0.0)], axis=1)
    high = jnp.concatenate([high, jnp.where(top & (col < float(across - 1)), hh, 0.0)], axis=1)
    side = side + jnp.where((r == 0.0) & (line(64, 8) == float(height - 1)), line(64, 10), 0.0)

    def two(x):
        hi = x.astype(BF16)
        return [hi, (x - hi.astype(F32)).astype(BF16)]

    lanes = iota((bands, across), 1)
    places = [table[:, o + 16 * k + 1 : o + 16 * k + 2] for o in (0, 64) for k in range(CAP)]
    spread = jnp.concatenate([one_hot(lanes == place) for place in places], axis=0)
    total = mm(jnp.concatenate(two(low) + two(high), axis=0), spread)
    same = total[0:height] + total[height : 2 * height]
    right = total[2 * height : 3 * height] + total[3 * height :]
    c = iota((height, across), 1)
    added = same + jnp.where(c == 0.0, lane_sum(side), pltpu.roll(right, 1, 1))
    span = height + 24
    early = iota((16, 128), 0) < 9.0
    for j in range(across // 128):
        sl = slice(128 * j, 128 * j + 128)
        at = span * j
        level = jnp.where(early, first_ref[16 * j : 16 * j + 16], base_ref[at : at + 16])
        out_ref[0:16, sl] = level + added[0:16, sl]
        out_ref[16:, sl] = base_ref[at + 16 : at + height] + added[16:, sl]
    copy.wait()


def ring(axis, distance):
    n = lax.axis_size(axis)
    return [(i, (i + distance) % n) for i in range(n)]


def shards(level_set, velocity, particles, escaped, home_cell, land_cell, dest_rank, block_count):
    height, across = level_set.shape
    n = particles.shape[0]
    bands = lax.axis_size("gy")
    step = 4 * CAP + 1
    sds = jax.ShapeDtypeStruct
    (head,) = call(
        heads_body,
        (sds((48, across), F32),),
        pltpu.with_memory_space_constraint(level_set, pltpu.HBM),
        pltpu.with_memory_space_constraint(velocity, pltpu.HBM),
        spaces=[pltpu.HBM, pltpu.HBM],
        scratch=[pltpu.VMEM((24, across), F32), pltpu.VMEM((2, 16, across), F32), pltpu.SemaphoreType.DMA((2,))],
    )
    below = lax.ppermute(head, "gy", ring("gy", -1))
    parts = jnp.transpose(particles, (1, 0, 2))
    meta, weight, near_x, near_y, select, fixed = call(
        prepare_body,
        (
            *[sds((n, 128), F32)] * 4,
            sds((bands * CAP, 3 * n), BF16),
            sds((bands * CAP, 256), F32),
        ),
        velocity, parts, escaped, home_cell.reshape(1, n), land_cell.reshape(1, n), dest_rank.reshape(1, n),
        scalars=(block_count,),
    )
    to_left, to_right, near_x, near_y = call(
        edges_body,
        (*[sds((height + 24, 128), F32)] * 2, *[sds((n, 128), F32)] * 2),
        level_set, velocity, below, meta, parts, weight, near_x, near_y,
    )
    from_left = lax.ppermute(to_right, "gx", ring("gx", 1))
    from_right = lax.ppermute(to_left, "gx", ring("gx", -1))
    (packed,) = call(
        functools.partial(pack_body, across=across),
        (sds((bands * step, 128), F32),),
        parts, weight, near_x, near_y, meta, to_left, from_left, from_right, select, fixed,
    )
    arrived = lax.all_to_all(
        packed.reshape(bands * step, 1, 128), "gy", split_axis=0, concat_axis=0, tiled=True
    )
    span = height + 24
    wide = pltpu.VMEM(((across // 128 + 1) * span, 128), F32)
    section, ahead = call(
        stencil_body,
        (sds((across // 128 * span, 128), F32), sds((across // 128 * 16, 128), F32)),
        level_set, velocity, below, from_right, from_left,
        scratch=[wide] * 5,
    )
    first_rows = lax.ppermute(ahead, "gy", ring("gy", 1))
    level, moved = call(
        deposit_body,
        (sds((height, across), F32), sds((bands, 4 * CAP, 1, 128), F32)),
        arrived.reshape(bands, step, 1, 128), arrived.reshape(bands * step, 128), section, first_rows,
        out_spaces=[pltpu.VMEM, pltpu.HBM],
        scratch=[pltpu.SemaphoreType.DMA],
    )
    return level, moved.reshape(bands * CAP, 4, 128)


def solution(mesh):
    in_specs = (
        P("gy", "gx"),
        P(None, "gy", "gx"),
        P(("gy", "gx"), None, None),
        P(("gy", "gx"), None),
        P(("gy", "gx")),
        P(("gy", "gx")),
        P(("gy", "gx")),
        P(("gy", "gx")),
    )
    out_specs = (P("gy", "gx"), P(("gy", "gx"), None, None))
    return jax.shard_map(shards, mesh=mesh, in_specs=in_specs, out_specs=out_specs, check_vma=False)
```

```python
import functools
import jax
import jax.numpy as jnp
from jax import lax
from jax.experimental import pallas as pl
from jax.experimental.pallas import tpu as pltpu
from jax.sharding import PartitionSpec as P

CAP = 4
DT = 0.3
INTERPRET = False
F32 = jnp.float32
BF16 = jnp.bfloat16


def iota(shape, dim):
    return lax.broadcasted_iota(jnp.int32, shape, dim).astype(F32)


def split3(x):
    hi = x.astype(BF16)
    rest = x - hi.astype(F32)
    mid = rest.astype(BF16)
    lo = (rest - mid.astype(F32)).astype(BF16)
    return hi, mid, lo


def mm(a, b):
    return lax.dot_general(a, b, (((1,), (0,)), ((), ())), preferred_element_type=F32)


def stack3(x):
    return jnp.concatenate(split3(x), axis=0)


def phase(shape, period):
    lane = iota(shape, 1)
    return lane - period * floor_div(lane, period)


def eye(n):
    return iota((n, n), 0) == iota((n, n), 1)


def to_column(row, n):
    return jnp.sum(jnp.where(eye(n), jnp.broadcast_to(row, (n, n)), 0.0), axis=1, keepdims=True)


def one_hot(mask):
    return jnp.where(mask, 1.0, 0.0).astype(BF16)


def floor_div(x, k):
    return jnp.floor((x + 0.5) * (1.0 / k))


def call(body, outs, *args, scratch=(), spaces=None, out_spaces=None, scalars=()):
    vm, sm = pltpu.VMEM, pltpu.SMEM
    spaces = spaces or [vm] * len(args)
    out_spaces = out_spaces or [vm] * len(outs)
    spec = lambda space: pl.BlockSpec(memory_space=space)
    return pl.pallas_call(
        body,
        out_shape=tuple(outs),
        in_specs=[spec(sm)] * len(scalars) + [spec(x) for x in spaces],
        out_specs=tuple(spec(x) for x in out_spaces),
        scratch_shapes=list(scratch),
        compiler_params=pltpu.CompilerParams(vmem_limit_bytes=16 * 1024 * 1024),
        interpret=INTERPRET,
    )(*scalars, *args)


def heads_body(f_ref, flow_ref, head_ref, f_rows, flow_rows, sems):
    copies = [
        pltpu.make_async_copy(f_ref.at[pl.ds(0, 24)], f_rows, sems.at[0]),
        pltpu.make_async_copy(flow_ref.at[:, pl.ds(0, 16)], flow_rows, sems.at[1]),
    ]
    for copy in copies:
        copy.start()
    for copy in copies:
        copy.wait()
    head_ref[0:18] = f_rows[0:18]
    head_ref[18:33] = flow_rows[0, 0:15]
    head_ref[33:48] = flow_rows[1, 0:15]


def advanced(x, y, u, v):
    fy = y + 0.5
    fx = x + 0.5
    w00 = (1.0 - fy) * (1.0 - fx)
    w10 = fy * (1.0 - fx)
    w01 = (1.0 - fy) * fx
    w11 = fy * fx
    new_x = x + DT * (w00 * u[0] + w10 * u[1] + w01 * u[2] + w11 * u[3])
    new_y = y + DT * (w00 * v[0] + w10 * v[1] + w01 * v[2] + w11 * v[3])
    return new_x, new_y


def put_rows(ref, picked, bands, step):
    for k in range(CAP):
        rows = slice(k * bands, (k + 1) * bands)
        for j in range(2):
            ref[pl.ds(CAP * j + k, bands, stride=step), :] = picked[rows, 128 * j : 128 * j + 128]


def prepare_body(count_ref, flow_ref, part_ref, esc_ref, home_ref, land_ref, dest_ref, meta_ref, w_ref, x_ref, y_ref, sel_ref, rw_ref):
    n = esc_ref.shape[0]
    height, across = flow_ref.shape[1:]
    home = to_column(home_ref[...].astype(F32), n)
    land = to_column(land_ref[...].astype(F32), n)
    dest_row = dest_ref[...].astype(F32)
    dest = to_column(dest_row, n)
    count = count_ref[0].astype(F32)
    row = floor_div(home, across)
    col = home - row * across
    land_row = floor_div(land, across)
    land_col = land - land_row * across
    other = iota((n, n), 0)
    mine = iota((n, n), 1)
    same = (dest == dest_row) & (other < mine) & (other < count)
    rank_row = jnp.sum(jnp.where(same, 1.0, 0.0), axis=0, keepdims=True)
    live_row = iota((1, n), 1) < count
    slot_row = jnp.where(live_row, dest_row * CAP + rank_row, -1.0)
    slot = to_column(slot_row, n)
    lane = phase((n, 3 * height), height)
    pick = jnp.concatenate([one_hot(lane == row), one_hot(lane == row + 1.0)], axis=0)
    lanes = iota((n, across), 1)
    at0 = lanes == col
    at1 = lanes == col + 1.0
    parts = []
    for component in range(2):
        both = mm(pick, stack3(flow_ref[component]))
        low = both[0:n]
        high = both[n:]
        for where_at in (at0, at1):
            for rows in (low, high):
                parts.append(jnp.sum(jnp.where(where_at, rows, 0.0), axis=1, keepdims=True))
    x_ref[...], y_ref[...] = advanced(part_ref[0], part_ref[1], parts[0:4], parts[4:8])
    lane = iota((n, 128), 1)
    meta = jnp.zeros((n, 128), F32)
    for i, value in enumerate((row, col, land_row, land_col, slot)):
        meta = jnp.where(lane == float(8 + i), value, meta)
    meta_ref[...] = meta
    w = esc_ref[...].astype(F32) * part_ref[2]
    w_ref[...] = w
    slots = sel_ref.shape[0]
    bands = slots // CAP
    r = iota((slots, 1), 0)
    k = floor_div(r, bands)
    choose = one_hot((r - k * bands) * CAP + k == jnp.concatenate([slot_row] * 3, axis=1))
    sel_ref[...] = choose
    put_rows(rw_ref, mm(choose, stack3(jnp.concatenate([part_ref[2], w], axis=1))), bands, 2 * CAP)


def pack_left(f, u, v):
    lane = iota(f.shape, 1)
    return jnp.where(lane < 16.0, f, jnp.where(lane < 32.0, pltpu.roll(u, 16, 1), pltpu.roll(v, 32, 1)))


def pack_right(f, u, v, m):
    lane = iota(f.shape, 1)
    out = jnp.where(lane >= 112.0, f, jnp.where(lane >= 96.0, pltpu.roll(u, 112, 1), pltpu.roll(v, 96, 1)))
    return jnp.where(lane < 32.0, m, out)


def edges_body(f_ref, flow_ref, below_ref, meta_ref, part_ref, w_ref, x_ref, y_ref, left_ref, right_ref, x2_ref, y2_ref):
    n = w_ref.shape[0]
    height, across = f_ref.shape
    meta = meta_ref[...]
    lane = iota((n, 128), 1)
    row = meta[:, 8:9]
    col = meta[:, 9:10]
    last = row == float(height - 1)
    lanes = iota((n, across), 1)
    at0 = (lanes == col) & last
    at1 = (lanes == col + 1.0) & last
    fix = []
    for r in (18, 33):
        line = jnp.broadcast_to(below_ref[r : r + 1, :], (n, across))
        for where_at in (at0, at1):
            fix.append(jnp.sum(jnp.where(where_at, line, 0.0), axis=1, keepdims=True))
    w = w_ref[...]
    fy = part_ref[1] + 0.5
    fx = part_ref[0] + 0.5
    low1 = fy * (1.0 - fx)
    high1 = fy * fx
    new_x = x_ref[...] + DT * (low1 * fix[0] + high1 * fix[1])
    new_y = y_ref[...] + DT * (low1 * fix[2] + high1 * fix[3])
    x2_ref[...] = new_x
    y2_ref[...] = new_y
    gx = new_x + 0.5
    gy = new_y + 0.5
    e1 = DT * ((1.0 - fy) * fx)
    e2 = DT * high1
    wgx, wgy, w1, w2 = w * gx, w * gy, w * e1, w * e2
    moments = [wgx, w1, w2, wgx * gy, wgy * e1, wgy * e2, wgx * e1, wgx * e2, w1 * e1, w1 * e2, w2 * e2]
    sent = meta
    for i, value in enumerate(moments):
        sent = jnp.where(lane == float(16 + i), lane_sum(value), sent)
    far = across - 128

    zero = jnp.zeros((8, 128), F32)

    def pieces(sl):
        yield 0, height, f_ref[:, sl], flow_ref[0, :, sl], flow_ref[1, :, sl], sent
        last = pltpu.roll(below_ref[40:48, sl], 7, 0)
        yield height, 8, below_ref[0:8, sl], below_ref[18:26, sl], below_ref[33:41, sl], zero
        yield height + 8, 8, below_ref[8:16, sl], below_ref[26:34, sl], last, zero
        yield height + 16, 8, below_ref[16:24, sl], zero, zero, zero

    for top, rows, f, u, v, _ in pieces(slice(0, 128)):
        left_ref[top : top + rows] = pack_left(f, u, v)
    for top, rows, f, u, v, m in pieces(slice(far, across)):
        right_ref[top : top + rows] = pack_right(f, u, v, m)


def halo_tiles(from_right, from_left):
    lane = iota(from_right.shape, 1)
    right_side = lane < 64.0
    f = jnp.where(right_side, from_right, from_left)
    u = jnp.where(right_side, pltpu.roll(from_right, 112, 1), pltpu.roll(from_left, 16, 1))
    v = jnp.where(right_side, pltpu.roll(from_right, 96, 1), pltpu.roll(from_left, 32, 1))
    return f, u, v


def right_corners(meta, column, across):
    n = meta.shape[0]
    depth = column.shape[0]
    row = meta[:, 8:9]
    last = meta[:, 9:10] == float(across - 1)
    lane = phase((n, 3 * depth), depth)
    pick = jnp.concatenate([one_hot((lane == row) & last), one_hot((lane == row + 1.0) & last)], axis=0)
    return mm(pick, stack3(column))


def lane_sum(x):
    return jnp.sum(x, axis=1, keepdims=True)


def pack_body(part_ref, w_ref, x_ref, y_ref, meta_ref, mine_ref, left_ref, right_ref, sel_ref, out_ref, across):
    n = w_ref.shape[0]
    bands = out_ref.shape[0] // (2 * CAP + 1)
    depth = right_ref.shape[0] - 16
    meta = meta_ref[...]
    step = 2 * CAP + 1
    w = w_ref[...]
    left_meta = left_ref[0:n]
    both = right_corners(meta, right_ref[0:depth], across)
    left_both = right_corners(left_meta, mine_ref[0:depth], across)
    fy = part_ref[1] + 0.5
    fx = part_ref[0] + 0.5
    e1 = DT * ((1.0 - fy) * fx)
    e2 = DT * (fy * fx)
    new_x = x_ref[...] + (e1 * both[0:n, 16:17] + e2 * both[n:, 16:17])
    new_y = y_ref[...] + (e1 * both[0:n, 32:33] + e2 * both[n:, 32:33])
    gy = new_y + 0.5
    gx = new_x + 0.5
    wy = w * gy
    wo = w - wy
    sums = [
        meta[:, 10:11],
        meta[:, 11:12],
        lane_sum(wo * (1.0 - gx)),
        lane_sum(wy * (1.0 - gx)),
        lane_sum(wo * gx),
        lane_sum(wy * gx),
    ]
    lane = iota((n, 128), 1)
    lane16 = lane - 16.0 * jnp.floor(lane * 0.0625)
    mine = jnp.zeros((n, 128), F32)
    for i, value in enumerate(sums):
        mine = jnp.where(lane16 == float(i), value, mine)
    facts = jnp.transpose(left_meta)
    flows = jnp.transpose(left_both)
    u1, u2 = flows[16:17, 0:n], flows[16:17, n:]
    v1, v2 = flows[32:33, 0:n], flows[32:33, n:]
    m = [facts[16 + i : 17 + i] for i in range(11)]
    hh = (m[3] + u1 * m[4] + u2 * m[5] + v1 * m[6] + v2 * m[7]) + (
        u1 * v1 * m[8] + (u1 * v2 + u2 * v1) * m[9] + u2 * v2 * m[10]
    )
    lh = (m[0] + u1 * m[1] + u2 * m[2]) - hh
    over = facts[11:12] == float(across - 1)
    line = iota((128, n), 0)
    line16 = line - 16.0 * jnp.floor(line * 0.0625)
    theirs = jnp.where(line16 == 8.0, facts[10:11], 0.0)
    theirs = jnp.where(line16 == 9.0, jnp.where(over, lh, 0.0), theirs)
    theirs = jnp.where(line16 == 10.0, jnp.where(over, hh, 0.0), theirs)
    theirs = jnp.transpose(theirs)
    choose = sel_ref[...]
    picked = mm(choose, stack3(jnp.concatenate([new_x, new_y, mine], axis=1)))
    put_rows(out_ref, picked, bands, step)
    slot = jnp.concatenate([facts[12:13]] * 3, axis=1)
    d4 = iota((bands, 3 * n), 0) * float(CAP)
    theirs_choose = jnp.concatenate([one_hot(d4 + float(k) == slot) for k in range(CAP)], axis=0)
    chosen = picked[:, 256:] + mm(theirs_choose, stack3(theirs))
    lane = iota((bands, 128), 1)
    group = jnp.floor(lane * 0.0625)
    table = jnp.zeros((bands, 128), F32)
    for k in range(CAP):
        table = jnp.where(group == float(k), chosen[k * bands : (k + 1) * bands], table)
    table = table + pltpu.roll(pltpu.roll(table, 1, 0), 64, 1)
    out_ref[pl.ds(2 * CAP, bands, stride=step), :] = table


def side_term(speed, e0, e1, e2, e3, e4, d2, d3):
    ahead = speed > 0.0
    p = jnp.where(ahead, e0, e4)
    q = jnp.where(ahead, e1, e3)
    s = jnp.where(ahead, e3, e1)
    c = jnp.where(ahead, d2, d3)
    r = e2
    rr = r * r
    t1 = p * (4.0 * p - 11.0 * q) + (10.0 * (q * q) + 3e-6)
    t2 = q * (4.0 * q - 5.0 * r) + (4.0 * rr + 3e-6)
    t3 = s * (4.0 * s - 11.0 * r) + (10.0 * rr + 3e-6)
    a1 = t2 * t3
    a2 = t1 * t3
    a3 = t1 * t2
    w1 = a1 * a1
    w2 = 6.0 * (a2 * a2)
    w3 = 3.0 * (a3 * a3)
    top = w1 * (2.0 * p - 5.0 * q) - w2 * (q + 2.0 * r) + w3 * (s - 4.0 * r)
    return speed * c + jnp.abs(speed) * (top / (6.0 * (w1 + w2 + w3)))


def stencil_body(f_ref, flow_ref, below_ref, right_ref, left_ref, out_ref, next_ref, f0, us, vs, f1, f2):
    height, across = f_ref.shape
    tiles = across // 128 + 1
    span = height + 24
    halos = halo_tiles(right_ref[...], left_ref[...])
    owns = (f_ref, flow_ref.at[0], flow_ref.at[1])
    for buf, own, halo, start, count in zip((f0, us, vs), owns, halos, (0, 18, 33), (18, 15, 15)):
        for j in range(tiles - 1):
            sl = slice(128 * j, 128 * j + 128)
            buf[span * j : span * j + height, :] = own[:, sl]
            buf[span * j + height : span * j + height + count, :] = below_ref[start : start + count, sl]
        buf[span * (tiles - 1) : span * tiles, :] = halo

    lane = lax.broadcasted_iota(jnp.int32, (8, 128), 1)

    def stage(src, dst_tiles, base, write):
        f = [src[pl.ds(span * j + base, 8), :] for j in range(tiles)]

        def shifted(k):
            turned = [pltpu.roll(t, (-k) % 128, 1) for t in f]
            if k > 0:
                return [jnp.where(lane < 128 - k, turned[j], turned[(j + 1) % tiles]) for j in range(dst_tiles)]
            return [jnp.where(lane >= -k, turned[j], turned[(j - 1) % tiles]) for j in range(dst_tiles)]

        near = {k: f if k == 0 else shifted(k) for k in range(-3, 4)}
        for j in range(dst_tiles):
            at = span * j + base
            u = us[pl.ds(at, 8), :]
            v = vs[pl.ds(at, 8), :]
            d = [near[k + 1][j] - near[k][j] for k in range(-3, 3)]
            e = [d[k] - d[k + 1] for k in range(5)]
            x_term = side_term(u, e[0], e[1], e[2], e[3], e[4], d[2], d[3])
            rows = [f[j] if k == 0 else src[pl.ds(at + k, 8), :] for k in range(-3, 4)]
            d = [rows[k + 1] - rows[k] for k in range(6)]
            e = [d[k] - d[k + 1] for k in range(5)]
            y_term = side_term(v, e[0], e[1], e[2], e[3], e[4], d[2], d[3])
            write(j, f[j] - DT * (x_term + y_term))

    def first(i, carry):
        base = i * 8 + 3

        def write(j, value):
            f1[pl.ds(span * j + base, 8), :] = value

        stage(f0, tiles, base, write)
        return carry

    def second(i, carry):
        base = i * 8 + 6

        def write(j, value):
            at = pl.ds(span * j + base, 8)
            f2[at, :] = 0.75 * f0[at, :] + 0.25 * value

        stage(f1, tiles, base, write)
        return carry

    def third(i, carry):
        base = i * 8 + 9

        def write(j, value):
            at = pl.ds(span * j + base, 8)
            out_ref[at, :] = f0[at, :] * (1.0 / 3.0) + (2.0 / 3.0) * value

        stage(f2, tiles - 1, base, write)
        return carry

    lax.fori_loop(0, height // 8 + 2, first, 0, unroll=2)
    lax.fori_loop(0, height // 8 + 1, second, 0, unroll=3)
    lax.fori_loop(0, height // 8, third, 0, unroll=2)
    for j in range(tiles - 1):
        next_ref[16 * j : 16 * j + 16] = out_ref[span * j + height : span * j + height + 16]


def deposit_body(fixed_ref, rows_ref, recv_ref, base_ref, first_ref, out_ref, moved_ref, sems):
    height, across = out_ref.shape
    step = 2 * CAP + 1
    bands = recv_ref.shape[0] // step
    copies = []
    for j, source in enumerate((rows_ref, rows_ref, fixed_ref, fixed_ref)):
        part = source.at[:, pl.ds(CAP * (j % 2), CAP)]
        copies.append(pltpu.make_async_copy(part, moved_ref.at[:, :, j], sems.at[j]))
    for copy in copies:
        copy.start()
    table = recv_ref[pl.ds(2 * CAP, bands, stride=step), :]
    turned = jnp.transpose(table)
    count = CAP * bands

    def line(first, i):
        return jnp.concatenate([turned[first + 16 * k + i : first + 16 * k + i + 1] for k in range(CAP)], axis=1)

    r = iota((height, count), 0)
    row, col, ll, hl, lh, hh = [line(0, i) for i in range(6)]
    inside = col < float(across - 1)
    at, under = r == row, r == row + 1.0
    low = jnp.where(at, ll, jnp.where(under, hl, 0.0))
    high = jnp.where(inside & at, lh, jnp.where(inside & under, hh, 0.0))
    row, lh, hh = [line(0, 8 + i) for i in range(3)]
    side = jnp.where(r == row, lh, jnp.where(r == row + 1.0, hh, 0.0))
    row, col, _, hl, _, hh = [line(64, i) for i in range(6)]
    top = (r == 0.0) & (row == float(height - 1))
    low = jnp.concatenate([low, jnp.where(top, hl, 0.0)], axis=1)
    high = jnp.concatenate([high, jnp.where(top & (col < float(across - 1)), hh, 0.0)], axis=1)
    side = side + jnp.where((r == 0.0) & (line(64, 8) == float(height - 1)), line(64, 10), 0.0)

    def two(x):
        hi = x.astype(BF16)
        return [hi, (x - hi.astype(F32)).astype(BF16)]

    lanes = iota((bands, across), 1)
    places = [table[:, o + 16 * k + 1 : o + 16 * k + 2] for o in (0, 64) for k in range(CAP)]
    spread = jnp.concatenate([one_hot(lanes == place) for place in places], axis=0)
    total = mm(jnp.concatenate(two(low) + two(high), axis=0), spread)
    same = total[0:height] + total[height : 2 * height]
    right = total[2 * height : 3 * height] + total[3 * height :]
    c = iota((height, across), 1)
    added = same + jnp.where(c == 0.0, lane_sum(side), pltpu.roll(right, 1, 1))
    span = height + 24
    early = iota((16, 128), 0) < 9.0
    for j in range(across // 128):
        sl = slice(128 * j, 128 * j + 128)
        at = span * j
        level = jnp.where(early, first_ref[16 * j : 16 * j + 16], base_ref[at : at + 16])
        out_ref[0:16, sl] = level + added[0:16, sl]
        out_ref[16:, sl] = base_ref[at + 16 : at + height] + added[16:, sl]
    for copy in copies:
        copy.wait()


def ring(axis, distance):
    n = lax.axis_size(axis)
    return [(i, (i + distance) % n) for i in range(n)]


def shards(level_set, velocity, particles, escaped, home_cell, land_cell, dest_rank, block_count):
    height, across = level_set.shape
    n = particles.shape[0]
    bands = lax.axis_size("gy")
    step = 2 * CAP + 1
    sds = jax.ShapeDtypeStruct
    (head,) = call(
        heads_body,
        (sds((48, across), F32),),
        pltpu.with_memory_space_constraint(level_set, pltpu.HBM),
        pltpu.with_memory_space_constraint(velocity, pltpu.HBM),
        spaces=[pltpu.HBM, pltpu.HBM],
        scratch=[pltpu.VMEM((24, across), F32), pltpu.VMEM((2, 16, across), F32), pltpu.SemaphoreType.DMA((2,))],
    )
    below = lax.ppermute(head, "gy", ring("gy", -1))
    parts = jnp.transpose(particles, (1, 0, 2))
    meta, weight, near_x, near_y, select, fixed = call(
        prepare_body,
        (
            *[sds((n, 128), F32)] * 4,
            sds((bands * CAP, 3 * n), BF16),
            sds((bands * 2 * CAP, 128), F32),
        ),
        velocity, parts, escaped, home_cell.reshape(1, n), land_cell.reshape(1, n), dest_rank.reshape(1, n),
        scalars=(block_count,),
    )
    settled = lax.all_to_all(
        fixed.reshape(bands, 2 * CAP, 128), "gy", split_axis=0, concat_axis=0, tiled=True
    )
    to_left, to_right, near_x, near_y = call(
        edges_body,
        (*[sds((height + 24, 128), F32)] * 2, *[sds((n, 128), F32)] * 2),
        level_set, velocity, below, meta, parts, weight, near_x, near_y,
    )
    from_left = lax.ppermute(to_right, "gx", ring("gx", 1))
    from_right = lax.ppermute(to_left, "gx", ring("gx", -1))
    (packed,) = call(
        functools.partial(pack_body, across=across),
        (sds((bands * step, 128), F32),),
        parts, weight, near_x, near_y, meta, to_left, from_left, from_right, select,
    )
    arrived = lax.all_to_all(
        packed.reshape(bands * step, 1, 128), "gy", split_axis=0, concat_axis=0, tiled=True
    )
    span = height + 24
    wide = pltpu.VMEM(((across // 128 + 1) * span, 128), F32)
    section, ahead = call(
        stencil_body,
        (sds((across // 128 * span, 128), F32), sds((across // 128 * 16, 128), F32)),
        level_set, velocity, below, from_right, from_left,
        scratch=[wide] * 5,
    )
    first_rows = lax.ppermute(ahead, "gy", ring("gy", 1))
    level, moved = call(
        deposit_body,
        (sds((height, across), F32), sds((bands, CAP, 4, 1, 128), F32)),
        settled.reshape(bands, 2 * CAP, 1, 128), arrived.reshape(bands, step, 1, 128), arrived.reshape(bands * step, 128), section, first_rows,
        out_spaces=[pltpu.VMEM, pltpu.HBM],
        scratch=[pltpu.SemaphoreType.DMA((4,))],
    )
    return level, moved.reshape(bands * CAP, 4, 128)


def solution(mesh):
    in_specs = (
        P("gy", "gx"),
        P(None, "gy", "gx"),
        P(("gy", "gx"), None, None),
        P(("gy", "gx"), None),
        P(("gy", "gx")),
        P(("gy", "gx")),
        P(("gy", "gx")),
        P(("gy", "gx")),
    )
    out_specs = (P("gy", "gx"), P(("gy", "gx"), None, None))
    return jax.shard_map(shards, mesh=mesh, in_specs=in_specs, out_specs=out_specs, check_vma=False)
```

```python
import functools
import jax
import jax.numpy as jnp
from jax import lax
from jax.experimental import pallas as pl
from jax.experimental.pallas import tpu as pltpu
from jax.sharding import PartitionSpec as P

CAP = 4
DT = 0.3
INTERPRET = False
F32 = jnp.float32
BF16 = jnp.bfloat16


def iota(shape, dim):
    return lax.broadcasted_iota(jnp.int32, shape, dim).astype(F32)


def split3(x):
    hi = x.astype(BF16)
    rest = x - hi.astype(F32)
    mid = rest.astype(BF16)
    lo = (rest - mid.astype(F32)).astype(BF16)
    return hi, mid, lo


def mm(a, b):
    return lax.dot_general(a, b, (((1,), (0,)), ((), ())), preferred_element_type=F32)


def stack3(x):
    return jnp.concatenate(split3(x), axis=0)


def phase(shape, period):
    lane = iota(shape, 1)
    return lane - period * floor_div(lane, period)


def eye(n):
    return iota((n, n), 0) == iota((n, n), 1)


def to_column(row, n):
    return jnp.sum(jnp.where(eye(n), jnp.broadcast_to(row, (n, n)), 0.0), axis=1, keepdims=True)


def one_hot(mask):
    return jnp.where(mask, 1.0, 0.0).astype(BF16)


def floor_div(x, k):
    return jnp.floor((x + 0.5) * (1.0 / k))


def call(body, outs, *args, scratch=(), spaces=None, out_spaces=None, scalars=(), aliases={}):
    vm, sm = pltpu.VMEM, pltpu.SMEM
    spaces = spaces or [vm] * len(args)
    out_spaces = out_spaces or [vm] * len(outs)
    spec = lambda space: pl.BlockSpec(memory_space=space)
    return pl.pallas_call(
        body,
        out_shape=tuple(outs),
        in_specs=[spec(sm)] * len(scalars) + [spec(x) for x in spaces],
        out_specs=tuple(spec(x) for x in out_spaces),
        scratch_shapes=list(scratch),
        input_output_aliases=aliases,
        compiler_params=pltpu.CompilerParams(vmem_limit_bytes=16 * 1024 * 1024),
        interpret=INTERPRET,
    )(*scalars, *args)


def heads_body(f_ref, flow_ref, head_ref, f_rows, flow_rows, sems):
    copies = [
        pltpu.make_async_copy(f_ref.at[pl.ds(0, 24)], f_rows, sems.at[0]),
        pltpu.make_async_copy(flow_ref.at[:, pl.ds(0, 16)], flow_rows, sems.at[1]),
    ]
    for copy in copies:
        copy.start()
    for copy in copies:
        copy.wait()
    head_ref[0:18] = f_rows[0:18]
    head_ref[18:33] = flow_rows[0, 0:15]
    head_ref[33:48] = flow_rows[1, 0:15]


def advanced(x, y, u, v):
    fy = y + 0.5
    fx = x + 0.5
    w00 = (1.0 - fy) * (1.0 - fx)
    w10 = fy * (1.0 - fx)
    w01 = (1.0 - fy) * fx
    w11 = fy * fx
    new_x = x + DT * (w00 * u[0] + w10 * u[1] + w01 * u[2] + w11 * u[3])
    new_y = y + DT * (w00 * v[0] + w10 * v[1] + w01 * v[2] + w11 * v[3])
    return new_x, new_y


def prepare_body(count_ref, flow_ref, part_ref, esc_ref, home_ref, land_ref, dest_ref, meta_ref, w_ref, x_ref, y_ref, sel_ref, rw_ref):
    n = esc_ref.shape[0]
    height, across = flow_ref.shape[1:]
    home = to_column(home_ref[...].astype(F32), n)
    land = to_column(land_ref[...].astype(F32), n)
    dest_row = dest_ref[...].astype(F32)
    dest = to_column(dest_row, n)
    count = count_ref[0].astype(F32)
    row = floor_div(home, across)
    col = home - row * across
    land_row = floor_div(land, across)
    land_col = land - land_row * across
    other = iota((n, n), 0)
    mine = iota((n, n), 1)
    same = (dest == dest_row) & (other < mine) & (other < count)
    rank_row = jnp.sum(jnp.where(same, 1.0, 0.0), axis=0, keepdims=True)
    live_row = iota((1, n), 1) < count
    slot_row = jnp.where(live_row, dest_row * CAP + rank_row, -1.0)
    slot = to_column(slot_row, n)
    lane = phase((n, 3 * height), height)
    pick = jnp.concatenate([one_hot(lane == row), one_hot(lane == row + 1.0)], axis=0)
    lanes = iota((n, across), 1)
    at0 = lanes == col
    at1 = lanes == col + 1.0
    parts = []
    for component in range(2):
        both = mm(pick, stack3(flow_ref[component]))
        low = both[0:n]
        high = both[n:]
        for where_at in (at0, at1):
            for rows in (low, high):
                parts.append(jnp.sum(jnp.where(where_at, rows, 0.0), axis=1, keepdims=True))
    x_ref[...], y_ref[...] = advanced(part_ref[0], part_ref[1], parts[0:4], parts[4:8])
    lane = iota((n, 128), 1)
    meta = jnp.zeros((n, 128), F32)
    for i, value in enumerate((row, col, land_row, land_col, slot)):
        meta = jnp.where(lane == float(8 + i), value, meta)
    meta_ref[...] = meta
    w = esc_ref[...].astype(F32) * part_ref[2]
    w_ref[...] = w
    slots = sel_ref.shape[0]
    bands = slots // CAP
    r = iota((slots, 1), 0)
    k = floor_div(r, bands)
    choose = one_hot((r - k * bands) * CAP + k == jnp.concatenate([slot_row] * 3, axis=1))
    sel_ref[...] = choose
    rw_ref[...] = mm(choose, stack3(jnp.concatenate([part_ref[2], w], axis=1)))


def pack_left(f, u, v):
    lane = iota(f.shape, 1)
    return jnp.where(lane < 16.0, f, jnp.where(lane < 32.0, pltpu.roll(u, 16, 1), pltpu.roll(v, 32, 1)))


def pack_right(f, u, v, m):
    lane = iota(f.shape, 1)
    out = jnp.where(lane >= 112.0, f, jnp.where(lane >= 96.0, pltpu.roll(u, 112, 1), pltpu.roll(v, 96, 1)))
    return jnp.where(lane < 32.0, m, out)


def edges_body(f_ref, flow_ref, below_ref, meta_ref, part_ref, w_ref, x_ref, y_ref, left_ref, right_ref, x2_ref, y2_ref):
    n = w_ref.shape[0]
    height, across = f_ref.shape
    meta = meta_ref[...]
    lane = iota((n, 128), 1)
    row = meta[:, 8:9]
    col = meta[:, 9:10]
    last = row == float(height - 1)
    lanes = iota((n, across), 1)
    at0 = (lanes == col) & last
    at1 = (lanes == col + 1.0) & last
    fix = []
    for r in (18, 33):
        line = jnp.broadcast_to(below_ref[r : r + 1, :], (n, across))
        for where_at in (at0, at1):
            fix.append(jnp.sum(jnp.where(where_at, line, 0.0), axis=1, keepdims=True))
    w = w_ref[...]
    fy = part_ref[1] + 0.5
    fx = part_ref[0] + 0.5
    low1 = fy * (1.0 - fx)
    high1 = fy * fx
    new_x = x_ref[...] + DT * (low1 * fix[0] + high1 * fix[1])
    new_y = y_ref[...] + DT * (low1 * fix[2] + high1 * fix[3])
    x2_ref[...] = new_x
    y2_ref[...] = new_y
    gx = new_x + 0.5
    gy = new_y + 0.5
    e1 = DT * ((1.0 - fy) * fx)
    e2 = DT * high1
    wgx, wgy, w1, w2 = w * gx, w * gy, w * e1, w * e2
    moments = [wgx, w1, w2, wgx * gy, wgy * e1, wgy * e2, wgx * e1, wgx * e2, w1 * e1, w1 * e2, w2 * e2]
    sent = meta
    for i, value in enumerate(moments):
        sent = jnp.where(lane == float(16 + i), lane_sum(value), sent)
    far = across - 128

    zero = jnp.zeros((8, 128), F32)

    def pieces(sl):
        yield 0, height, f_ref[:, sl], flow_ref[0, :, sl], flow_ref[1, :, sl], sent
        last = pltpu.roll(below_ref[40:48, sl], 7, 0)
        yield height, 8, below_ref[0:8, sl], below_ref[18:26, sl], below_ref[33:41, sl], zero
        yield height + 8, 8, below_ref[8:16, sl], below_ref[26:34, sl], last, zero
        yield height + 16, 8, below_ref[16:24, sl], zero, zero, zero

    for top, rows, f, u, v, _ in pieces(slice(0, 128)):
        left_ref[top : top + rows] = pack_left(f, u, v)
    for top, rows, f, u, v, m in pieces(slice(far, across)):
        right_ref[top : top + rows] = pack_right(f, u, v, m)


def halo_tiles(from_right, from_left):
    lane = iota(from_right.shape, 1)
    right_side = lane < 64.0
    f = jnp.where(right_side, from_right, from_left)
    u = jnp.where(right_side, pltpu.roll(from_right, 112, 1), pltpu.roll(from_left, 16, 1))
    v = jnp.where(right_side, pltpu.roll(from_right, 96, 1), pltpu.roll(from_left, 32, 1))
    return f, u, v


def right_corners(meta, column, across):
    n = meta.shape[0]
    depth = column.shape[0]
    row = meta[:, 8:9]
    last = meta[:, 9:10] == float(across - 1)
    lane = phase((n, 3 * depth), depth)
    pick = jnp.concatenate([one_hot((lane == row) & last), one_hot((lane == row + 1.0) & last)], axis=0)
    return mm(pick, stack3(column))


def lane_sum(x):
    return jnp.sum(x, axis=1, keepdims=True)


def pack_body(part_ref, w_ref, x_ref, y_ref, meta_ref, right_ref, sel_ref, rw_ref, out_ref, own_ref, across):
    n = w_ref.shape[0]
    bands = out_ref.shape[0] // (4 * CAP + 1)
    meta = meta_ref[...]
    step = 4 * CAP + 1
    w = w_ref[...]
    both = right_corners(meta, right_ref[0 : right_ref.shape[0] - 16], across)
    fy = part_ref[1] + 0.5
    fx = part_ref[0] + 0.5
    e1 = DT * ((1.0 - fy) * fx)
    e2 = DT * (fy * fx)
    new_x = x_ref[...] + (e1 * both[0:n, 16:17] + e2 * both[n:, 16:17])
    new_y = y_ref[...] + (e1 * both[0:n, 32:33] + e2 * both[n:, 32:33])
    gy = new_y + 0.5
    gx = new_x + 0.5
    wy = w * gy
    wo = w - wy
    sums = [
        meta[:, 10:11],
        meta[:, 11:12],
        lane_sum(wo * (1.0 - gx)),
        lane_sum(wy * (1.0 - gx)),
        lane_sum(wo * gx),
        lane_sum(wy * gx),
    ]
    lane = iota((n, 128), 1)
    lane16 = lane - 16.0 * jnp.floor(lane * 0.0625)
    mine = jnp.zeros((n, 128), F32)
    for i, value in enumerate(sums):
        mine = jnp.where(lane16 == float(i), value, mine)
    picked = mm(sel_ref[...], stack3(jnp.concatenate([new_x, new_y, mine], axis=1)))
    for k in range(CAP):
        rows = slice(k * bands, (k + 1) * bands)
        for j, source in ((0, picked), (1, picked), (2, rw_ref), (3, rw_ref)):
            sl = slice(128 * (j % 2), 128 * (j % 2) + 128)
            out_ref[pl.ds(4 * k + j, bands, stride=step), :] = source[rows, sl]
    own_ref[...] = picked[:, 256:]


def table_body(left_ref, mine_ref, own_ref, held_ref, out_ref, line_ref, sem, n, across):
    del held_ref
    bands = out_ref.shape[0]
    left_meta = left_ref[0:n]
    left_both = right_corners(left_meta, mine_ref[0 : mine_ref.shape[0] - 16], across)
    facts = jnp.transpose(left_meta)
    flows = jnp.transpose(left_both)
    u1, u2 = flows[16:17, 0:n], flows[16:17, n:]
    v1, v2 = flows[32:33, 0:n], flows[32:33, n:]
    m = [facts[16 + i : 17 + i] for i in range(11)]
    hh = (m[3] + u1 * m[4] + u2 * m[5] + v1 * m[6] + v2 * m[7]) + (
        u1 * v1 * m[8] + (u1 * v2 + u2 * v1) * m[9] + u2 * v2 * m[10]
    )
    lh = (m[0] + u1 * m[1] + u2 * m[2]) - hh
    over = facts[11:12] == float(across - 1)
    line = iota((128, n), 0)
    line16 = line - 16.0 * jnp.floor(line * 0.0625)
    theirs = jnp.where(line16 == 8.0, facts[10:11], 0.0)
    theirs = jnp.where(line16 == 9.0, jnp.where(over, lh, 0.0), theirs)
    theirs = jnp.where(line16 == 10.0, jnp.where(over, hh, 0.0), theirs)
    theirs = jnp.transpose(theirs)
    slot = jnp.concatenate([facts[12:13]] * 3, axis=1)
    d4 = iota((bands, 3 * n), 0) * float(CAP)
    theirs_choose = jnp.concatenate([one_hot(d4 + float(k) == slot) for k in range(CAP)], axis=0)
    chosen = own_ref[...] + mm(theirs_choose, stack3(theirs))
    lane = iota((bands, 128), 1)
    group = jnp.floor(lane * 0.0625)
    group = jnp.where(group >= float(CAP), group - float(CAP), group)
    table = jnp.zeros((bands, 128), F32)
    for k in range(CAP):
        table = jnp.where(group == float(k), chosen[k * bands : (k + 1) * bands], table)
    table = jnp.where(lane < 64.0, table, pltpu.roll(table, 1, 0))
    line_ref[...] = table.reshape(bands, 1, 1, 128)
    copy = pltpu.make_async_copy(line_ref, out_ref.at[:, pl.ds(4 * CAP, 1)], sem)
    copy.start()
    copy.wait()


def side_term(speed, e0, e1, e2, e3, e4, d2, d3):
    ahead = speed > 0.0
    p = jnp.where(ahead, e0, e4)
    q = jnp.where(ahead, e1, e3)
    s = jnp.where(ahead, e3, e1)
    c = jnp.where(ahead, d2, d3)
    r = e2
    rr = r * r
    t1 = p * (4.0 * p - 11.0 * q) + (10.0 * (q * q) + 3e-6)
    t2 = q * (4.0 * q - 5.0 * r) + (4.0 * rr + 3e-6)
    t3 = s * (4.0 * s - 11.0 * r) + (10.0 * rr + 3e-6)
    a1 = t2 * t3
    a2 = t1 * t3
    a3 = t1 * t2
    w1 = a1 * a1
    w2 = 6.0 * (a2 * a2)
    w3 = 3.0 * (a3 * a3)
    top = w1 * (2.0 * p - 5.0 * q) - w2 * (q + 2.0 * r) + w3 * (s - 4.0 * r)
    return speed * c + jnp.abs(speed) * (top / (6.0 * (w1 + w2 + w3)))


def stencil_body(f_ref, flow_ref, below_ref, right_ref, left_ref, out_ref, next_ref, f0, us, vs, f1, f2):
    height, across = f_ref.shape
    tiles = across // 128 + 1
    span = height + 24
    halos = halo_tiles(right_ref[...], left_ref[...])
    owns = (f_ref, flow_ref.at[0], flow_ref.at[1])
    for buf, own, halo, start, count in zip((f0, us, vs), owns, halos, (0, 18, 33), (18, 15, 15)):
        for j in range(tiles - 1):
            sl = slice(128 * j, 128 * j + 128)
            buf[span * j : span * j + height, :] = own[:, sl]
            buf[span * j + height : span * j + height + count, :] = below_ref[start : start + count, sl]
        buf[span * (tiles - 1) : span * tiles, :] = halo

    lane = lax.broadcasted_iota(jnp.int32, (8, 128), 1)

    def stage(src, dst_tiles, base, write):
        f = [src[pl.ds(span * j + base, 8), :] for j in range(tiles)]

        def shifted(k):
            turned = [pltpu.roll(t, (-k) % 128, 1) for t in f]
            if k > 0:
                return [jnp.where(lane < 128 - k, turned[j], turned[(j + 1) % tiles]) for j in range(dst_tiles)]
            return [jnp.where(lane >= -k, turned[j], turned[(j - 1) % tiles]) for j in range(dst_tiles)]

        near = {k: f if k == 0 else shifted(k) for k in range(-3, 4)}
        for j in range(dst_tiles):
            at = span * j + base
            u = us[pl.ds(at, 8), :]
            v = vs[pl.ds(at, 8), :]
            d = [near[k + 1][j] - near[k][j] for k in range(-3, 3)]
            e = [d[k] - d[k + 1] for k in range(5)]
            x_term = side_term(u, e[0], e[1], e[2], e[3], e[4], d[2], d[3])
            rows = [f[j] if k == 0 else src[pl.ds(at + k, 8), :] for k in range(-3, 4)]
            d = [rows[k + 1] - rows[k] for k in range(6)]
            e = [d[k] - d[k + 1] for k in range(5)]
            y_term = side_term(v, e[0], e[1], e[2], e[3], e[4], d[2], d[3])
            write(j, f[j] - DT * (x_term + y_term))

    def first(i, carry):
        base = i * 8 + 3

        def write(j, value):
            f1[pl.ds(span * j + base, 8), :] = value

        stage(f0, tiles, base, write)
        return carry

    def second(i, carry):
        base = i * 8 + 6

        def write(j, value):
            at = pl.ds(span * j + base, 8)
            f2[at, :] = 0.75 * f0[at, :] + 0.25 * value

        stage(f1, tiles, base, write)
        return carry

    def third(i, carry):
        base = i * 8 + 9

        def write(j, value):
            at = pl.ds(span * j + base, 8)
            out_ref[at, :] = f0[at, :] * (1.0 / 3.0) + (2.0 / 3.0) * value

        stage(f2, tiles - 1, base, write)
        return carry

    lax.fori_loop(0, height // 8 + 2, first, 0, unroll=2)
    lax.fori_loop(0, height // 8 + 1, second, 0, unroll=3)
    lax.fori_loop(0, height // 8, third, 0, unroll=2)
    for j in range(tiles - 1):
        next_ref[16 * j : 16 * j + 16] = out_ref[span * j + height : span * j + height + 16]


def deposit_body(rows_ref, recv_ref, base_ref, first_ref, out_ref, moved_ref, sem):
    height, across = out_ref.shape
    step = 4 * CAP + 1
    bands = recv_ref.shape[0] // step
    block = 4 * CAP
    copy = pltpu.make_async_copy(rows_ref.at[:, pl.ds(0, block)], moved_ref, sem)
    copy.start()
    table = recv_ref[pl.ds(block, bands, stride=step), :]
    turned = jnp.transpose(table)
    count = CAP * bands

    def line(first, i):
        return jnp.concatenate([turned[first + 16 * k + i : first + 16 * k + i + 1] for k in range(CAP)], axis=1)

    r = iota((height, count), 0)
    row, col, ll, hl, lh, hh = [line(0, i) for i in range(6)]
    inside = col < float(across - 1)
    at, under = r == row, r == row + 1.0
    low = jnp.where(at, ll, jnp.where(under, hl, 0.0))
    high = jnp.where(inside & at, lh, jnp.where(inside & under, hh, 0.0))
    row, lh, hh = [line(0, 8 + i) for i in range(3)]
    side = jnp.where(r == row, lh, jnp.where(r == row + 1.0, hh, 0.0))
    row, col, _, hl, _, hh = [line(64, i) for i in range(6)]
    top = (r == 0.0) & (row == float(height - 1))
    low = jnp.concatenate([low, jnp.where(top, hl, 0.0)], axis=1)
    high = jnp.concatenate([high, jnp.where(top & (col < float(across - 1)), hh, 0.0)], axis=1)
    side = side + jnp.where((r == 0.0) & (line(64, 8) == float(height - 1)), line(64, 10), 0.0)

    def two(x):
        hi = x.astype(BF16)
        return [hi, (x - hi.astype(F32)).astype(BF16)]

    lanes = iota((bands, across), 1)
    places = [table[:, o + 16 * k + 1 : o + 16 * k + 2] for o in (0, 64) for k in range(CAP)]
    spread = jnp.concatenate([one_hot(lanes == place) for place in places], axis=0)
    total = mm(jnp.concatenate(two(low) + two(high), axis=0), spread)
    same = total[0:height] + total[height : 2 * height]
    right = total[2 * height : 3 * height] + total[3 * height :]
    c = iota((height, across), 1)
    added = same + jnp.where(c == 0.0, lane_sum(side), pltpu.roll(right, 1, 1))
    span = height + 24
    early = iota((16, 128), 0) < 9.0
    for j in range(across // 128):
        sl = slice(128 * j, 128 * j + 128)
        at = span * j
        level = jnp.where(early, first_ref[16 * j : 16 * j + 16], base_ref[at : at + 16])
        out_ref[0:16, sl] = level + added[0:16, sl]
        out_ref[16:, sl] = base_ref[at + 16 : at + height] + added[16:, sl]
    copy.wait()


def ring(axis, distance):
    n = lax.axis_size(axis)
    return [(i, (i + distance) % n) for i in range(n)]


def shards(level_set, velocity, particles, escaped, home_cell, land_cell, dest_rank, block_count):
    height, across = level_set.shape
    n = particles.shape[0]
    bands = lax.axis_size("gy")
    step = 4 * CAP + 1
    sds = jax.ShapeDtypeStruct
    (head,) = call(
        heads_body,
        (sds((48, across), F32),),
        pltpu.with_memory_space_constraint(level_set, pltpu.HBM),
        pltpu.with_memory_space_constraint(velocity, pltpu.HBM),
        spaces=[pltpu.HBM, pltpu.HBM],
        scratch=[pltpu.VMEM((24, across), F32), pltpu.VMEM((2, 16, across), F32), pltpu.SemaphoreType.DMA((2,))],
    )
    below = lax.ppermute(head, "gy", ring("gy", -1))
    parts = jnp.transpose(particles, (1, 0, 2))
    meta, weight, near_x, near_y, select, fixed = call(
        prepare_body,
        (
            *[sds((n, 128), F32)] * 4,
            sds((bands * CAP, 3 * n), BF16),
            sds((bands * CAP, 256), F32),
        ),
        velocity, parts, escaped, home_cell.reshape(1, n), land_cell.reshape(1, n), dest_rank.reshape(1, n),
        scalars=(block_count,),
    )
    to_left, to_right, near_x, near_y = call(
        edges_body,
        (*[sds((height + 24, 128), F32)] * 2, *[sds((n, 128), F32)] * 2),
        level_set, velocity, below, meta, parts, weight, near_x, near_y,
    )
    from_right = lax.ppermute(to_left, "gx", ring("gx", -1))
    from_left = lax.ppermute(to_right, "gx", ring("gx", 1))
    packed, own = call(
        functools.partial(pack_body, across=across),
        (sds((bands * step, 128), F32), sds((bands * CAP, 128), F32)),
        parts, weight, near_x, near_y, meta, from_right, select, fixed,
    )
    (packed,) = call(
        functools.partial(table_body, n=n, across=across),
        (pltpu.HBM((bands, step, 1, 128), F32),),
        from_left, to_left, own,
        pltpu.with_memory_space_constraint(packed.reshape(bands, step, 1, 128), pltpu.HBM),
        spaces=[pltpu.VMEM] * 3 + [pltpu.HBM],
        out_spaces=[pltpu.HBM],
        scratch=[pltpu.VMEM((bands, 1, 1, 128), F32), pltpu.SemaphoreType.DMA],
        aliases={3: 0},
    )
    arrived = lax.all_to_all(
        packed.reshape(bands * step, 1, 128), "gy", split_axis=0, concat_axis=0, tiled=True
    )
    span = height + 24
    wide = pltpu.VMEM(((across // 128 + 1) * span, 128), F32)
    section, ahead = call(
        stencil_body,
        (sds((across // 128 * span, 128), F32), sds((across // 128 * 16, 128), F32)),
        level_set, velocity, below, from_right, from_left,
        scratch=[wide] * 5,
    )
    first_rows = lax.ppermute(ahead, "gy", ring("gy", 1))
    level, moved = call(
        deposit_body,
        (sds((height, across), F32), sds((bands, 4 * CAP, 1, 128), F32)),
        arrived.reshape(bands, step, 1, 128), arrived.reshape(bands * step, 128), section, first_rows,
        out_spaces=[pltpu.VMEM, pltpu.HBM],
        scratch=[pltpu.SemaphoreType.DMA],
    )
    return level, moved.reshape(bands * CAP, 4, 128)


def solution(mesh):
    in_specs = (
        P("gy", "gx"),
        P(None, "gy", "gx"),
        P(("gy", "gx"), None, None),
        P(("gy", "gx"), None),
        P(("gy", "gx")),
        P(("gy", "gx")),
        P(("gy", "gx")),
        P(("gy", "gx")),
    )
    out_specs = (P("gy", "gx"), P(("gy", "gx"), None, None))
    return jax.shard_map(shards, mesh=mesh, in_specs=in_specs, out_specs=out_specs, check_vma=False)
```

```python
import functools
import jax
import jax.numpy as jnp
from jax import lax
from jax.experimental import pallas as pl
from jax.experimental.pallas import tpu as pltpu
from jax.sharding import PartitionSpec as P

CAP = 4
DT = 0.3
INTERPRET = False
F32 = jnp.float32
BF16 = jnp.bfloat16


def iota(shape, dim):
    return lax.broadcasted_iota(jnp.int32, shape, dim).astype(F32)


def split3(x):
    hi = x.astype(BF16)
    rest = x - hi.astype(F32)
    mid = rest.astype(BF16)
    lo = (rest - mid.astype(F32)).astype(BF16)
    return hi, mid, lo


def mm(a, b):
    return lax.dot_general(a, b, (((1,), (0,)), ((), ())), preferred_element_type=F32)


def stack3(x):
    return jnp.concatenate(split3(x), axis=0)


def phase(shape, period):
    lane = iota(shape, 1)
    return lane - period * floor_div(lane, period)


def eye(n):
    return iota((n, n), 0) == iota((n, n), 1)


def to_column(row, n):
    return jnp.sum(jnp.where(eye(n), jnp.broadcast_to(row, (n, n)), 0.0), axis=1, keepdims=True)


def one_hot(mask):
    return jnp.where(mask, 1.0, 0.0).astype(BF16)


def floor_div(x, k):
    return jnp.floor((x + 0.5) * (1.0 / k))


def call(body, outs, *args, scratch=(), spaces=None, out_spaces=None, scalars=()):
    vm, sm = pltpu.VMEM, pltpu.SMEM
    spaces = spaces or [vm] * len(args)
    out_spaces = out_spaces or [vm] * len(outs)
    spec = lambda space: pl.BlockSpec(memory_space=space)
    return pl.pallas_call(
        body,
        out_shape=tuple(outs),
        in_specs=[spec(sm)] * len(scalars) + [spec(x) for x in spaces],
        out_specs=tuple(spec(x) for x in out_spaces),
        scratch_shapes=list(scratch),
        compiler_params=pltpu.CompilerParams(vmem_limit_bytes=16 * 1024 * 1024),
        interpret=INTERPRET,
    )(*scalars, *args)


def heads_body(f_ref, flow_ref, head_ref, f_rows, flow_rows, sems):
    copies = [
        pltpu.make_async_copy(f_ref.at[pl.ds(0, 24)], f_rows, sems.at[0]),
        pltpu.make_async_copy(flow_ref.at[:, pl.ds(0, 16)], flow_rows, sems.at[1]),
    ]
    for copy in copies:
        copy.start()
    for copy in copies:
        copy.wait()
    head_ref[0:18] = f_rows[0:18]
    head_ref[18:33] = flow_rows[0, 0:15]
    head_ref[33:48] = flow_rows[1, 0:15]


def advanced(x, y, u, v):
    fy = y + 0.5
    fx = x + 0.5
    w00 = (1.0 - fy) * (1.0 - fx)
    w10 = fy * (1.0 - fx)
    w01 = (1.0 - fy) * fx
    w11 = fy * fx
    new_x = x + DT * (w00 * u[0] + w10 * u[1] + w01 * u[2] + w11 * u[3])
    new_y = y + DT * (w00 * v[0] + w10 * v[1] + w01 * v[2] + w11 * v[3])
    return new_x, new_y


def prepare_body(count_ref, flow_ref, part_ref, esc_ref, home_ref, land_ref, dest_ref, meta_ref, w_ref, x_ref, y_ref, sel_ref, rw_ref):
    n = esc_ref.shape[0]
    height, across = flow_ref.shape[1:]
    home = to_column(home_ref[...].astype(F32), n)
    land = to_column(land_ref[...].astype(F32), n)
    dest_row = dest_ref[...].astype(F32)
    dest = to_column(dest_row, n)
    count = count_ref[0].astype(F32)
    row = floor_div(home, across)
    col = home - row * across
    land_row = floor_div(land, across)
    land_col = land - land_row * across
    other = iota((n, n), 0)
    mine = iota((n, n), 1)
    same = (dest == dest_row) & (other < mine) & (other < count)
    rank_row = jnp.sum(jnp.where(same, 1.0, 0.0), axis=0, keepdims=True)
    live_row = iota((1, n), 1) < count
    slot_row = jnp.where(live_row, dest_row * CAP + rank_row, -1.0)
    slot = to_column(slot_row, n)
    lane = phase((n, 3 * height), height)
    pick = jnp.concatenate([one_hot(lane == row), one_hot(lane == row + 1.0)], axis=0)
    lanes = iota((n, across), 1)
    at0 = lanes == col
    at1 = lanes == col + 1.0
    parts = []
    for component in range(2):
        both = mm(pick, stack3(flow_ref[component]))
        low = both[0:n]
        high = both[n:]
        for where_at in (at0, at1):
            for rows in (low, high):
                parts.append(jnp.sum(jnp.where(where_at, rows, 0.0), axis=1, keepdims=True))
    x_ref[...], y_ref[...] = advanced(part_ref[0], part_ref[1], parts[0:4], parts[4:8])
    lane = iota((n, 128), 1)
    meta = jnp.zeros((n, 128), F32)
    for i, value in enumerate((row, col, land_row, land_col, slot)):
        meta = jnp.where(lane == float(8 + i), value, meta)
    meta_ref[...] = meta
    w = esc_ref[...].astype(F32) * part_ref[2]
    w_ref[...] = w
    slots = sel_ref.shape[0]
    bands = slots // CAP
    r = iota((slots, 1), 0)
    k = floor_div(r, bands)
    choose = one_hot((r - k * bands) * CAP + k == jnp.concatenate([slot_row] * 3, axis=1))
    sel_ref[...] = choose
    rw_ref[...] = mm(choose, stack3(jnp.concatenate([part_ref[2], w], axis=1)))


def pack_left(f, u, v):
    lane = iota(f.shape, 1)
    return jnp.where(lane < 16.0, f, jnp.where(lane < 32.0, pltpu.roll(u, 16, 1), pltpu.roll(v, 32, 1)))


def pack_right(f, u, v, m):
    lane = iota(f.shape, 1)
    out = jnp.where(lane >= 112.0, f, jnp.where(lane >= 96.0, pltpu.roll(u, 112, 1), pltpu.roll(v, 96, 1)))
    return jnp.where(lane < 32.0, m, out)


def edges_body(f_ref, flow_ref, below_ref, meta_ref, part_ref, w_ref, x_ref, y_ref, left_ref, right_ref, x2_ref, y2_ref):
    n = w_ref.shape[0]
    height, across = f_ref.shape
    meta = meta_ref[...]
    lane = iota((n, 128), 1)
    row = meta[:, 8:9]
    col = meta[:, 9:10]
    last = row == float(height - 1)
    lanes = iota((n, across), 1)
    at0 = (lanes == col) & last
    at1 = (lanes == col + 1.0) & last
    fix = []
    for r in (18, 33):
        line = jnp.broadcast_to(below_ref[r : r + 1, :], (n, across))
        for where_at in (at0, at1):
            fix.append(jnp.sum(jnp.where(where_at, line, 0.0), axis=1, keepdims=True))
    w = w_ref[...]
    fy = part_ref[1] + 0.5
    fx = part_ref[0] + 0.5
    low1 = fy * (1.0 - fx)
    high1 = fy * fx
    new_x = x_ref[...] + DT * (low1 * fix[0] + high1 * fix[1])
    new_y = y_ref[...] + DT * (low1 * fix[2] + high1 * fix[3])
    x2_ref[...] = new_x
    y2_ref[...] = new_y
    gx = new_x + 0.5
    gy = new_y + 0.5
    e1 = DT * ((1.0 - fy) * fx)
    e2 = DT * high1
    wgx, wgy, w1, w2 = w * gx, w * gy, w * e1, w * e2
    moments = [wgx, w1, w2, wgx * gy, wgy * e1, wgy * e2, wgx * e1, wgx * e2, w1 * e1, w1 * e2, w2 * e2]
    sent = meta
    for i, value in enumerate(moments):
        sent = jnp.where(lane == float(16 + i), lane_sum(value), sent)
    far = across - 128

    zero = jnp.zeros((8, 128), F32)

    def pieces(sl):
        yield 0, height, f_ref[:, sl], flow_ref[0, :, sl], flow_ref[1, :, sl], sent
        last = pltpu.roll(below_ref[40:48, sl], 7, 0)
        yield height, 8, below_ref[0:8, sl], below_ref[18:26, sl], below_ref[33:41, sl], zero
        yield height + 8, 8, below_ref[8:16, sl], below_ref[26:34, sl], last, zero
        yield height + 16, 8, below_ref[16:24, sl], zero, zero, zero

    for top, rows, f, u, v, _ in pieces(slice(0, 128)):
        left_ref[top : top + rows] = pack_left(f, u, v)
    for top, rows, f, u, v, m in pieces(slice(far, across)):
        right_ref[top : top + rows] = pack_right(f, u, v, m)


def halo_tiles(from_right, from_left):
    lane = iota(from_right.shape, 1)
    right_side = lane < 64.0
    f = jnp.where(right_side, from_right, from_left)
    u = jnp.where(right_side, pltpu.roll(from_right, 112, 1), pltpu.roll(from_left, 16, 1))
    v = jnp.where(right_side, pltpu.roll(from_right, 96, 1), pltpu.roll(from_left, 32, 1))
    return f, u, v


def right_corners(meta, column, across):
    n = meta.shape[0]
    depth = column.shape[0]
    row = meta[:, 8:9]
    last = meta[:, 9:10] == float(across - 1)
    lane = phase((n, 3 * depth), depth)
    pick = jnp.concatenate([one_hot((lane == row) & last), one_hot((lane == row + 1.0) & last)], axis=0)
    return mm(pick, stack3(column))


def lane_sum(x):
    return jnp.sum(x, axis=1, keepdims=True)


def side_body(left_ref, mine_ref, side_ref, n, across):
    bands = side_ref.shape[0] // CAP
    left_meta = left_ref[0:n]
    left_both = right_corners(left_meta, mine_ref[0 : mine_ref.shape[0] - 16], across)
    facts = jnp.transpose(left_meta)
    flows = jnp.transpose(left_both)
    u1, u2 = flows[16:17, 0:n], flows[16:17, n:]
    v1, v2 = flows[32:33, 0:n], flows[32:33, n:]
    m = [facts[16 + i : 17 + i] for i in range(11)]
    hh = (m[3] + u1 * m[4] + u2 * m[5] + v1 * m[6] + v2 * m[7]) + (
        u1 * v1 * m[8] + (u1 * v2 + u2 * v1) * m[9] + u2 * v2 * m[10]
    )
    lh = (m[0] + u1 * m[1] + u2 * m[2]) - hh
    over = facts[11:12] == float(across - 1)
    line = iota((128, n), 0)
    line16 = line - 16.0 * jnp.floor(line * 0.0625)
    theirs = jnp.where(line16 == 8.0, facts[10:11], 0.0)
    theirs = jnp.where(line16 == 9.0, jnp.where(over, lh, 0.0), theirs)
    theirs = jnp.where(line16 == 10.0, jnp.where(over, hh, 0.0), theirs)
    theirs = jnp.transpose(theirs)
    slot = jnp.concatenate([facts[12:13]] * 3, axis=1)
    d4 = iota((bands, 3 * n), 0) * float(CAP)
    choose = jnp.concatenate([one_hot(d4 + float(k) == slot) for k in range(CAP)], axis=0)
    side_ref[...] = mm(choose, stack3(theirs))


def pack_body(part_ref, w_ref, x_ref, y_ref, meta_ref, right_ref, sel_ref, rw_ref, side_ref, out_ref, across):
    n = w_ref.shape[0]
    bands = out_ref.shape[0] // (4 * CAP + 1)
    depth = right_ref.shape[0] - 16
    meta = meta_ref[...]
    step = 4 * CAP + 1
    w = w_ref[...]
    both = right_corners(meta, right_ref[0:depth], across)
    fy = part_ref[1] + 0.5
    fx = part_ref[0] + 0.5
    e1 = DT * ((1.0 - fy) * fx)
    e2 = DT * (fy * fx)
    new_x = x_ref[...] + (e1 * both[0:n, 16:17] + e2 * both[n:, 16:17])
    new_y = y_ref[...] + (e1 * both[0:n, 32:33] + e2 * both[n:, 32:33])
    gy = new_y + 0.5
    gx = new_x + 0.5
    wy = w * gy
    wo = w - wy
    sums = [
        meta[:, 10:11],
        meta[:, 11:12],
        lane_sum(wo * (1.0 - gx)),
        lane_sum(wy * (1.0 - gx)),
        lane_sum(wo * gx),
        lane_sum(wy * gx),
    ]
    lane = iota((n, 128), 1)
    lane16 = lane - 16.0 * jnp.floor(lane * 0.0625)
    mine = jnp.zeros((n, 128), F32)
    for i, value in enumerate(sums):
        mine = jnp.where(lane16 == float(i), value, mine)
    choose = sel_ref[...]
    picked = mm(choose, stack3(jnp.concatenate([new_x, new_y, mine], axis=1)))
    for k in range(CAP):
        rows = slice(k * bands, (k + 1) * bands)
        for j, source in ((0, picked), (1, picked), (2, rw_ref), (3, rw_ref)):
            sl = slice(128 * (j % 2), 128 * (j % 2) + 128)
            out_ref[pl.ds(4 * k + j, bands, stride=step), :] = source[rows, sl]
    chosen = picked[:, 256:] + side_ref[...]
    lane = iota((bands, 128), 1)
    group = jnp.floor(lane * 0.0625)
    group = jnp.where(group >= float(CAP), group - float(CAP), group)
    table = jnp.zeros((bands, 128), F32)
    for k in range(CAP):
        table = jnp.where(group == float(k), chosen[k * bands : (k + 1) * bands], table)
    table = jnp.where(lane < 64.0, table, pltpu.roll(table, 1, 0))
    out_ref[pl.ds(4 * CAP, bands, stride=step), :] = table


def side_term(speed, e0, e1, e2, e3, e4, d2, d3):
    ahead = speed > 0.0
    p = jnp.where(ahead, e0, e4)
    q = jnp.where(ahead, e1, e3)
    s = jnp.where(ahead, e3, e1)
    c = jnp.where(ahead, d2, d3)
    r = e2
    rr = r * r
    t1 = p * (4.0 * p - 11.0 * q) + (10.0 * (q * q) + 3e-6)
    t2 = q * (4.0 * q - 5.0 * r) + (4.0 * rr + 3e-6)
    t3 = s * (4.0 * s - 11.0 * r) + (10.0 * rr + 3e-6)
    a1 = t2 * t3
    a2 = t1 * t3
    a3 = t1 * t2
    w1 = a1 * a1
    w2 = 6.0 * (a2 * a2)
    w3 = 3.0 * (a3 * a3)
    top = w1 * (2.0 * p - 5.0 * q) - w2 * (q + 2.0 * r) + w3 * (s - 4.0 * r)
    return speed * c + jnp.abs(speed) * (top / (6.0 * (w1 + w2 + w3)))


def stencil_body(f_ref, flow_ref, below_ref, right_ref, left_ref, out_ref, next_ref, f0, us, vs, f1, f2):
    height, across = f_ref.shape
    tiles = across // 128 + 1
    span = height + 24
    halos = halo_tiles(right_ref[...], left_ref[...])
    owns = (f_ref, flow_ref.at[0], flow_ref.at[1])
    for buf, own, halo, start, count in zip((f0, us, vs), owns, halos, (0, 18, 33), (18, 15, 15)):
        for j in range(tiles - 1):
            sl = slice(128 * j, 128 * j + 128)
            buf[span * j : span * j + height, :] = own[:, sl]
            buf[span * j + height : span * j + height + count, :] = below_ref[start : start + count, sl]
        buf[span * (tiles - 1) : span * tiles, :] = halo

    lane = lax.broadcasted_iota(jnp.int32, (8, 128), 1)

    def stage(src, dst_tiles, base, write):
        f = [src[pl.ds(span * j + base, 8), :] for j in range(tiles)]

        def shifted(k):
            turned = [pltpu.roll(t, (-k) % 128, 1) for t in f]
            if k > 0:
                return [jnp.where(lane < 128 - k, turned[j], turned[(j + 1) % tiles]) for j in range(dst_tiles)]
            return [jnp.where(lane >= -k, turned[j], turned[(j - 1) % tiles]) for j in range(dst_tiles)]

        near = {k: f if k == 0 else shifted(k) for k in range(-3, 4)}
        for j in range(dst_tiles):
            at = span * j + base
            u = us[pl.ds(at, 8), :]
            v = vs[pl.ds(at, 8), :]
            d = [near[k + 1][j] - near[k][j] for k in range(-3, 3)]
            e = [d[k] - d[k + 1] for k in range(5)]
            x_term = side_term(u, e[0], e[1], e[2], e[3], e[4], d[2], d[3])
            rows = [f[j] if k == 0 else src[pl.ds(at + k, 8), :] for k in range(-3, 4)]
            d = [rows[k + 1] - rows[k] for k in range(6)]
            e = [d[k] - d[k + 1] for k in range(5)]
            y_term = side_term(v, e[0], e[1], e[2], e[3], e[4], d[2], d[3])
            write(j, f[j] - DT * (x_term + y_term))

    def first(i, carry):
        base = i * 8 + 3

        def write(j, value):
            f1[pl.ds(span * j + base, 8), :] = value

        stage(f0, tiles, base, write)
        return carry

    def second(i, carry):
        base = i * 8 + 6

        def write(j, value):
            at = pl.ds(span * j + base, 8)
            f2[at, :] = 0.75 * f0[at, :] + 0.25 * value

        stage(f1, tiles, base, write)
        return carry

    def third(i, carry):
        base = i * 8 + 9

        def write(j, value):
            at = pl.ds(span * j + base, 8)
            out_ref[at, :] = f0[at, :] * (1.0 / 3.0) + (2.0 / 3.0) * value

        stage(f2, tiles - 1, base, write)
        return carry

    lax.fori_loop(0, height // 8 + 2, first, 0, unroll=2)
    lax.fori_loop(0, height // 8 + 1, second, 0, unroll=3)
    lax.fori_loop(0, height // 8, third, 0, unroll=2)
    for j in range(tiles - 1):
        next_ref[16 * j : 16 * j + 16] = out_ref[span * j + height : span * j + height + 16]


def deposit_body(rows_ref, recv_ref, base_ref, first_ref, out_ref, moved_ref, sem):
    height, across = out_ref.shape
    step = 4 * CAP + 1
    bands = recv_ref.shape[0] // step
    block = 4 * CAP
    copy = pltpu.make_async_copy(rows_ref.at[:, pl.ds(0, block)], moved_ref, sem)
    copy.start()
    table = recv_ref[pl.ds(block, bands, stride=step), :]
    turned = jnp.transpose(table)
    count = CAP * bands

    def line(first, i):
        return jnp.concatenate([turned[first + 16 * k + i : first + 16 * k + i + 1] for k in range(CAP)], axis=1)

    r = iota((height, count), 0)
    row, col, ll, hl, lh, hh = [line(0, i) for i in range(6)]
    inside = col < float(across - 1)
    at, under = r == row, r == row + 1.0
    low = jnp.where(at, ll, jnp.where(under, hl, 0.0))
    high = jnp.where(inside & at, lh, jnp.where(inside & under, hh, 0.0))
    row, lh, hh = [line(0, 8 + i) for i in range(3)]
    side = jnp.where(r == row, lh, jnp.where(r == row + 1.0, hh, 0.0))
    row, col, _, hl, _, hh = [line(64, i) for i in range(6)]
    top = (r == 0.0) & (row == float(height - 1))
    low = jnp.concatenate([low, jnp.where(top, hl, 0.0)], axis=1)
    high = jnp.concatenate([high, jnp.where(top & (col < float(across - 1)), hh, 0.0)], axis=1)
    side = side + jnp.where((r == 0.0) & (line(64, 8) == float(height - 1)), line(64, 10), 0.0)

    def two(x):
        hi = x.astype(BF16)
        return [hi, (x - hi.astype(F32)).astype(BF16)]

    lanes = iota((bands, across), 1)
    places = [table[:, o + 16 * k + 1 : o + 16 * k + 2] for o in (0, 64) for k in range(CAP)]
    spread = jnp.concatenate([one_hot(lanes == place) for place in places], axis=0)
    total = mm(jnp.concatenate(two(low) + two(high), axis=0), spread)
    same = total[0:height] + total[height : 2 * height]
    right = total[2 * height : 3 * height] + total[3 * height :]
    c = iota((height, across), 1)
    added = same + jnp.where(c == 0.0, lane_sum(side), pltpu.roll(right, 1, 1))
    span = height + 24
    early = iota((16, 128), 0) < 9.0
    for j in range(across // 128):
        sl = slice(128 * j, 128 * j + 128)
        at = span * j
        level = jnp.where(early, first_ref[16 * j : 16 * j + 16], base_ref[at : at + 16])
        out_ref[0:16, sl] = level + added[0:16, sl]
        out_ref[16:, sl] = base_ref[at + 16 : at + height] + added[16:, sl]
    copy.wait()


def ring(axis, distance):
    n = lax.axis_size(axis)
    return [(i, (i + distance) % n) for i in range(n)]


def shards(level_set, velocity, particles, escaped, home_cell, land_cell, dest_rank, block_count):
    height, across = level_set.shape
    n = particles.shape[0]
    bands = lax.axis_size("gy")
    step = 4 * CAP + 1
    sds = jax.ShapeDtypeStruct
    (head,) = call(
        heads_body,
        (sds((48, across), F32),),
        pltpu.with_memory_space_constraint(level_set, pltpu.HBM),
        pltpu.with_memory_space_constraint(velocity, pltpu.HBM),
        spaces=[pltpu.HBM, pltpu.HBM],
        scratch=[pltpu.VMEM((24, across), F32), pltpu.VMEM((2, 16, across), F32), pltpu.SemaphoreType.DMA((2,))],
    )
    below = lax.ppermute(head, "gy", ring("gy", -1))
    parts = jnp.transpose(particles, (1, 0, 2))
    meta, weight, near_x, near_y, select, fixed = call(
        prepare_body,
        (
            *[sds((n, 128), F32)] * 4,
            sds((bands * CAP, 3 * n), BF16),
            sds((bands * CAP, 256), F32),
        ),
        velocity, parts, escaped, home_cell.reshape(1, n), land_cell.reshape(1, n), dest_rank.reshape(1, n),
        scalars=(block_count,),
    )
    to_left, to_right, near_x, near_y = call(
        edges_body,
        (*[sds((height + 24, 128), F32)] * 2, *[sds((n, 128), F32)] * 2),
        level_set, velocity, below, meta, parts, weight, near_x, near_y,
    )
    from_left = lax.ppermute(to_right, "gx", ring("gx", 1))
    from_right = lax.ppermute(to_left, "gx", ring("gx", -1))
    (side,) = call(
        functools.partial(side_body, n=n, across=across),
        (sds((bands * CAP, 128), F32),),
        from_left, to_left,
    )
    (packed,) = call(
        functools.partial(pack_body, across=across),
        (sds((bands * step, 128), F32),),
        parts, weight, near_x, near_y, meta, from_right, select, fixed, side,
    )
    arrived = lax.all_to_all(
        packed.reshape(bands * step, 1, 128), "gy", split_axis=0, concat_axis=0, tiled=True
    )
    span = height + 24
    wide = pltpu.VMEM(((across // 128 + 1) * span, 128), F32)
    section, ahead = call(
        stencil_body,
        (sds((across // 128 * span, 128), F32), sds((across // 128 * 16, 128), F32)),
        level_set, velocity, below, from_right, from_left,
        scratch=[wide] * 5,
    )
    first_rows = lax.ppermute(ahead, "gy", ring("gy", 1))
    level, moved = call(
        deposit_body,
        (sds((height, across), F32), sds((bands, 4 * CAP, 1, 128), F32)),
        arrived.reshape(bands, step, 1, 128), arrived.reshape(bands * step, 128), section, first_rows,
        out_spaces=[pltpu.VMEM, pltpu.HBM],
        scratch=[pltpu.SemaphoreType.DMA],
    )
    return level, moved.reshape(bands * CAP, 4, 128)


def solution(mesh):
    in_specs = (
        P("gy", "gx"),
        P(None, "gy", "gx"),
        P(("gy", "gx"), None, None),
        P(("gy", "gx"), None),
        P(("gy", "gx")),
        P(("gy", "gx")),
        P(("gy", "gx")),
        P(("gy", "gx")),
    )
    out_specs = (P("gy", "gx"), P(("gy", "gx"), None, None))
    return jax.shard_map(shards, mesh=mesh, in_specs=in_specs, out_specs=out_specs, check_vma=False)
```

```python
import functools
import jax
import jax.numpy as jnp
from jax import lax
from jax.experimental import pallas as pl
from jax.experimental.pallas import tpu as pltpu
from jax.sharding import PartitionSpec as P

CAP = 4
DT = 0.3
INTERPRET = False
F32 = jnp.float32
BF16 = jnp.bfloat16


def iota(shape, dim):
    return lax.broadcasted_iota(jnp.int32, shape, dim).astype(F32)


def split3(x):
    hi = x.astype(BF16)
    rest = x - hi.astype(F32)
    mid = rest.astype(BF16)
    lo = (rest - mid.astype(F32)).astype(BF16)
    return hi, mid, lo


def mm(a, b):
    return lax.dot_general(a, b, (((1,), (0,)), ((), ())), preferred_element_type=F32)


def stack3(x):
    return jnp.concatenate(split3(x), axis=0)


def phase(shape, period):
    lane = iota(shape, 1)
    return lane - period * floor_div(lane, period)


def eye(n):
    return iota((n, n), 0) == iota((n, n), 1)


def to_column(row, n):
    return jnp.sum(jnp.where(eye(n), jnp.broadcast_to(row, (n, n)), 0.0), axis=1, keepdims=True)


def one_hot(mask):
    return jnp.where(mask, 1.0, 0.0).astype(BF16)


def floor_div(x, k):
    return jnp.floor((x + 0.5) * (1.0 / k))


def call(body, outs, *args, scratch=(), spaces=None, out_spaces=None, scalars=()):
    vm, sm = pltpu.VMEM, pltpu.SMEM
    spaces = spaces or [vm] * len(args)
    out_spaces = out_spaces or [vm] * len(outs)
    spec = lambda space: pl.BlockSpec(memory_space=space)
    return pl.pallas_call(
        body,
        out_shape=tuple(outs),
        in_specs=[spec(sm)] * len(scalars) + [spec(x) for x in spaces],
        out_specs=tuple(spec(x) for x in out_spaces),
        scratch_shapes=list(scratch),
        compiler_params=pltpu.CompilerParams(vmem_limit_bytes=16 * 1024 * 1024),
        interpret=INTERPRET,
    )(*scalars, *args)


def heads_body(f_ref, flow_ref, head_ref, tail_ref, f_rows, flow_rows, sems):
    height = f_ref.shape[0]
    copies = []
    for i, (f_top, flow_top) in enumerate(((0, 0), (height - 16, height - 8))):
        copies.append(pltpu.make_async_copy(f_ref.at[pl.ds(f_top, 16)], f_rows.at[i], sems.at[2 * i]))
        copies.append(pltpu.make_async_copy(flow_ref.at[:, pl.ds(flow_top, 8)], flow_rows.at[i], sems.at[2 * i + 1]))
    for copy in copies:
        copy.start()
    for copy in copies:
        copy.wait()
    for i, (ref, f0, v0) in enumerate(((head_ref, 0, 0), (tail_ref, 7, 2))):
        ref[0:9] = f_rows[i, f0 : f0 + 9]
        ref[9:15] = flow_rows[i, 0, v0 : v0 + 6]
        ref[15:21] = flow_rows[i, 1, v0 : v0 + 6]
        ref[21:24] = jnp.zeros((3, f_ref.shape[1]), F32)


def advanced(x, y, u, v):
    fy = y + 0.5
    fx = x + 0.5
    w00 = (1.0 - fy) * (1.0 - fx)
    w10 = fy * (1.0 - fx)
    w01 = (1.0 - fy) * fx
    w11 = fy * fx
    new_x = x + DT * (w00 * u[0] + w10 * u[1] + w01 * u[2] + w11 * u[3])
    new_y = y + DT * (w00 * v[0] + w10 * v[1] + w01 * v[2] + w11 * v[3])
    return new_x, new_y


def prepare_body(count_ref, f_ref, flow_ref, part_ref, esc_ref, home_ref, land_ref, dest_ref, meta_ref, w_ref, x_ref, y_ref, sel_ref, rw_ref):
    n = esc_ref.shape[0]
    height, across = flow_ref.shape[1:]
    home = to_column(home_ref[...].astype(F32), n)
    land = to_column(land_ref[...].astype(F32), n)
    dest_row = dest_ref[...].astype(F32)
    dest = to_column(dest_row, n)
    count = count_ref[0].astype(F32)
    row = floor_div(home, across)
    col = home - row * across
    land_row = floor_div(land, across)
    land_col = land - land_row * across
    other = iota((n, n), 0)
    mine = iota((n, n), 1)
    same = (dest == dest_row) & (other < mine) & (other < count)
    rank_row = jnp.sum(jnp.where(same, 1.0, 0.0), axis=0, keepdims=True)
    live_row = iota((1, n), 1) < count
    slot_row = jnp.where(live_row, dest_row * CAP + rank_row, -1.0)
    slot = to_column(slot_row, n)
    lane = phase((n, 3 * height), height)
    pick = jnp.concatenate([one_hot(lane == row), one_hot(lane == row + 1.0)], axis=0)
    lanes = iota((n, across), 1)
    at0 = lanes == col
    at1 = lanes == col + 1.0
    parts = []
    for component in range(2):
        both = mm(pick, stack3(flow_ref[component]))
        low = both[0:n]
        high = both[n:]
        for where_at in (at0, at1):
            for rows in (low, high):
                parts.append(jnp.sum(jnp.where(where_at, rows, 0.0), axis=1, keepdims=True))
    x_ref[...], y_ref[...] = advanced(part_ref[0], part_ref[1], parts[0:4], parts[4:8])
    lane = iota((n, 128), 1)
    meta = jnp.zeros((n, 128), F32)
    for i, value in enumerate((row, col, land_row, land_col, slot)):
        meta = jnp.where(lane == float(8 + i), value, meta)
    meta_ref[...] = meta
    w = esc_ref[...].astype(F32) * part_ref[2]
    w_ref[...] = w
    slots = sel_ref.shape[0]
    bands = slots // CAP
    r = iota((slots, 1), 0)
    k = floor_div(r, bands)
    choose = one_hot((r - k * bands) * CAP + k == jnp.concatenate([slot_row] * 3, axis=1))
    sel_ref[...] = choose
    rw_ref[...] = mm(choose, stack3(jnp.concatenate([part_ref[2], w], axis=1)))


def pack_left(f, u, v):
    lane = iota(f.shape, 1)
    return jnp.where(lane < 16.0, f, jnp.where(lane < 32.0, pltpu.roll(u, 16, 1), pltpu.roll(v, 32, 1)))


def pack_right(f, u, v, m):
    lane = iota(f.shape, 1)
    out = jnp.where(lane >= 112.0, f, jnp.where(lane >= 96.0, pltpu.roll(u, 112, 1), pltpu.roll(v, 96, 1)))
    return jnp.where(lane < 32.0, m, out)


def corners_body(above_ref, left_ref, right_ref):
    across = above_ref.shape[1]
    zero = jnp.zeros((8, 128), F32)
    near, far = slice(0, 128), slice(across - 128, across)
    left_ref[0:8] = pack_left(above_ref[0:8, near], above_ref[9:17, near], above_ref[15:23, near])
    left_ref[8:16] = pack_left(above_ref[8:16, near], zero, zero)
    right_ref[0:8] = pack_right(above_ref[0:8, far], above_ref[9:17, far], above_ref[15:23, far], zero)
    right_ref[8:16] = pack_right(above_ref[8:16, far], zero, zero, zero)


def edges_body(f_ref, flow_ref, below_ref, meta_ref, part_ref, w_ref, x_ref, y_ref, left_ref, right_ref, x2_ref, y2_ref):
    n = w_ref.shape[0]
    height, across = f_ref.shape
    meta = meta_ref[...]
    lane = iota((n, 128), 1)
    row = meta[:, 8:9]
    col = meta[:, 9:10]
    last = row == float(height - 1)
    lanes = iota((n, across), 1)
    at0 = (lanes == col) & last
    at1 = (lanes == col + 1.0) & last
    fix = []
    for r in (9, 15):
        line = jnp.broadcast_to(below_ref[r : r + 1, :], (n, across))
        for where_at in (at0, at1):
            fix.append(jnp.sum(jnp.where(where_at, line, 0.0), axis=1, keepdims=True))
    w = w_ref[...]
    fy = part_ref[1] + 0.5
    fx = part_ref[0] + 0.5
    low1 = fy * (1.0 - fx)
    high1 = fy * fx
    new_x = x_ref[...] + DT * (low1 * fix[0] + high1 * fix[1])
    new_y = y_ref[...] + DT * (low1 * fix[2] + high1 * fix[3])
    x2_ref[...] = new_x
    y2_ref[...] = new_y
    gx = new_x + 0.5
    gy = new_y + 0.5
    e1 = DT * ((1.0 - fy) * fx)
    e2 = DT * high1
    wgx, wgy, w1, w2 = w * gx, w * gy, w * e1, w * e2
    moments = [wgx, w1, w2, wgx * gy, wgy * e1, wgy * e2, wgx * e1, wgx * e2, w1 * e1, w1 * e2, w2 * e2]
    sent = meta
    for i, value in enumerate(moments):
        sent = jnp.where(lane == float(16 + i), lane_sum(value), sent)
    far = across - 128

    zero = jnp.zeros((8, 128), F32)

    def pieces(sl):
        yield 0, height, f_ref[:, sl], flow_ref[0, :, sl], flow_ref[1, :, sl], sent
        yield height, 8, below_ref[0:8, sl], below_ref[9:17, sl], below_ref[15:23, sl], zero
        yield height + 8, 8, below_ref[8:16, sl], zero, zero, zero

    for top, rows, f, u, v, _ in pieces(slice(0, 128)):
        left_ref[top : top + rows] = pack_left(f, u, v)
    for top, rows, f, u, v, m in pieces(slice(far, across)):
        right_ref[top : top + rows] = pack_right(f, u, v, m)


def halo_tiles(from_right, from_left):
    lane = iota(from_right.shape, 1)
    right_side = lane < 64.0
    f = jnp.where(right_side, from_right, from_left)
    u = jnp.where(right_side, pltpu.roll(from_right, 112, 1), pltpu.roll(from_left, 16, 1))
    v = jnp.where(right_side, pltpu.roll(from_right, 96, 1), pltpu.roll(from_left, 32, 1))
    return f, u, v


def right_corners(meta, column, across):
    n = meta.shape[0]
    depth = column.shape[0]
    row = meta[:, 8:9]
    last = meta[:, 9:10] == float(across - 1)
    lane = phase((n, 3 * depth), depth)
    pick = jnp.concatenate([one_hot((lane == row) & last), one_hot((lane == row + 1.0) & last)], axis=0)
    return mm(pick, stack3(column))


def lane_sum(x):
    return jnp.sum(x, axis=1, keepdims=True)


def side_body(left_ref, mine_ref, side_ref, n, across):
    bands = side_ref.shape[0] // CAP
    left_meta = left_ref[0:n]
    left_both = right_corners(left_meta, mine_ref[0 : mine_ref.shape[0] - 8], across)
    facts = jnp.transpose(left_meta)
    flows = jnp.transpose(left_both)
    u1, u2 = flows[16:17, 0:n], flows[16:17, n:]
    v1, v2 = flows[32:33, 0:n], flows[32:33, n:]
    m = [facts[16 + i : 17 + i] for i in range(11)]
    hh = (m[3] + u1 * m[4] + u2 * m[5] + v1 * m[6] + v2 * m[7]) + (
        u1 * v1 * m[8] + (u1 * v2 + u2 * v1) * m[9] + u2 * v2 * m[10]
    )
    lh = (m[0] + u1 * m[1] + u2 * m[2]) - hh
    over = facts[11:12] == float(across - 1)
    line = iota((128, n), 0)
    line16 = line - 16.0 * jnp.floor(line * 0.0625)
    theirs = jnp.where(line16 == 8.0, facts[10:11], 0.0)
    theirs = jnp.where(line16 == 9.0, jnp.where(over, lh, 0.0), theirs)
    theirs = jnp.where(line16 == 10.0, jnp.where(over, hh, 0.0), theirs)
    theirs = jnp.transpose(theirs)
    slot = jnp.concatenate([facts[12:13]] * 3, axis=1)
    d4 = iota((bands, 3 * n), 0) * float(CAP)
    choose = jnp.concatenate([one_hot(d4 + float(k) == slot) for k in range(CAP)], axis=0)
    side_ref[...] = mm(choose, stack3(theirs))


def pack_body(part_ref, w_ref, x_ref, y_ref, meta_ref, right_ref, sel_ref, rw_ref, side_ref, out_ref, across):
    n = w_ref.shape[0]
    bands = out_ref.shape[0] // (4 * CAP + 1)
    depth = right_ref.shape[0] - 8
    meta = meta_ref[...]
    step = 4 * CAP + 1
    w = w_ref[...]
    both = right_corners(meta, right_ref[0:depth], across)
    fy = part_ref[1] + 0.5
    fx = part_ref[0] + 0.5
    e1 = DT * ((1.0 - fy) * fx)
    e2 = DT * (fy * fx)
    new_x = x_ref[...] + (e1 * both[0:n, 16:17] + e2 * both[n:, 16:17])
    new_y = y_ref[...] + (e1 * both[0:n, 32:33] + e2 * both[n:, 32:33])
    gy = new_y + 0.5
    gx = new_x + 0.5
    wy = w * gy
    wo = w - wy
    sums = [
        meta[:, 10:11],
        meta[:, 11:12],
        lane_sum(wo * (1.0 - gx)),
        lane_sum(wy * (1.0 - gx)),
        lane_sum(wo * gx),
        lane_sum(wy * gx),
    ]
    lane = iota((n, 128), 1)
    lane16 = lane - 16.0 * jnp.floor(lane * 0.0625)
    mine = jnp.zeros((n, 128), F32)
    for i, value in enumerate(sums):
        mine = jnp.where(lane16 == float(i), value, mine)
    choose = sel_ref[...]
    picked = mm(choose, stack3(jnp.concatenate([new_x, new_y, mine], axis=1)))
    for k in range(CAP):
        rows = slice(k * bands, (k + 1) * bands)
        for j, source in ((0, picked), (1, picked), (2, rw_ref), (3, rw_ref)):
            sl = slice(128 * (j % 2), 128 * (j % 2) + 128)
            out_ref[pl.ds(4 * k + j, bands, stride=step), :] = source[rows, sl]
    chosen = picked[:, 256:] + side_ref[...]
    lane = iota((bands, 128), 1)
    group = jnp.floor(lane * 0.0625)
    group = jnp.where(group >= float(CAP), group - float(CAP), group)
    table = jnp.zeros((bands, 128), F32)
    for k in range(CAP):
        table = jnp.where(group == float(k), chosen[k * bands : (k + 1) * bands], table)
    table = jnp.where(lane < 64.0, table, pltpu.roll(table, 1, 0))
    out_ref[pl.ds(4 * CAP, bands, stride=step), :] = table


def side_term(speed, e0, e1, e2, e3, e4, d2, d3):
    ahead = speed > 0.0
    p = jnp.where(ahead, e0, e4)
    q = jnp.where(ahead, e1, e3)
    s = jnp.where(ahead, e3, e1)
    c = jnp.where(ahead, d2, d3)
    r = e2
    rr = r * r
    t1 = p * (4.0 * p - 11.0 * q) + (10.0 * (q * q) + 3e-6)
    t2 = q * (4.0 * q - 5.0 * r) + (4.0 * rr + 3e-6)
    t3 = s * (4.0 * s - 11.0 * r) + (10.0 * rr + 3e-6)
    a1 = t2 * t3
    a2 = t1 * t3
    a3 = t1 * t2
    w1 = a1 * a1
    w2 = 6.0 * (a2 * a2)
    w3 = 3.0 * (a3 * a3)
    top = w1 * (2.0 * p - 5.0 * q) - w2 * (q + 2.0 * r) + w3 * (s - 4.0 * r)
    return speed * c + jnp.abs(speed) * (top / (6.0 * (w1 + w2 + w3)))


def stencil_body(f_ref, flow_ref, below_ref, above_ref, right_ref, left_ref, right2_ref, left2_ref, out_ref, f0, us, vs, f1, f2):
    height, across = f_ref.shape
    width = across + 128
    tiles = width // 128
    off = 16
    span = height + 32
    halos = halo_tiles(right_ref[...], left_ref[...])
    uppers = halo_tiles(right2_ref[...], left2_ref[...])
    owns = (f_ref, flow_ref.at[0], flow_ref.at[1])
    for buf, own, halo, upper, start, count in zip((f0, us, vs), owns, halos, uppers, (0, 9, 15), (9, 6, 6)):
        for j in range(tiles):
            sl = slice(128 * j, 128 * j + 128)
            top = span * j + off
            if j < tiles - 1:
                buf[top : top + height, :] = own[:, sl]
                buf[top + height : top + height + count, :] = below_ref[start : start + count, sl]
                buf[top - count : top, :] = above_ref[start : start + count, sl]
            else:
                buf[top : top + height + count, :] = halo[0 : height + count]
                buf[top - count : top, :] = upper[0:count]

    lane = lax.broadcasted_iota(jnp.int32, (8, 128), 1)

    def stage(src, dst_tiles, base, write):
        f = [src[pl.ds(span * j + base, 8), :] for j in range(tiles)]

        def shifted(k):
            turned = [pltpu.roll(t, (-k) % 128, 1) for t in f]
            if k > 0:
                return [jnp.where(lane < 128 - k, turned[j], turned[(j + 1) % tiles]) for j in range(dst_tiles)]
            return [jnp.where(lane >= -k, turned[j], turned[(j - 1) % tiles]) for j in range(dst_tiles)]

        near = {k: f if k == 0 else shifted(k) for k in range(-3, 4)}
        for j in range(dst_tiles):
            at = span * j + base
            u = us[pl.ds(at, 8), :]
            v = vs[pl.ds(at, 8), :]
            d = [near[k + 1][j] - near[k][j] for k in range(-3, 3)]
            e = [d[k] - d[k + 1] for k in range(5)]
            x_term = side_term(u, e[0], e[1], e[2], e[3], e[4], d[2], d[3])
            rows = [f[j] if k == 0 else src[pl.ds(at + k, 8), :] for k in range(-3, 4)]
            d = [rows[k + 1] - rows[k] for k in range(6)]
            e = [d[k] - d[k + 1] for k in range(5)]
            y_term = side_term(v, e[0], e[1], e[2], e[3], e[4], d[2], d[3])
            write(j, f[j] - DT * (x_term + y_term))

    def first(i, carry):
        base = pl.multiple_of(i * 8 + 8, 8)

        def write(j, value):
            f1[pl.ds(span * j + base, 8), :] = value

        stage(f0, tiles, base, write)
        return carry

    def second(i, carry):
        base = pl.multiple_of(i * 8 + 8, 8)

        def write(j, value):
            at = pl.ds(span * j + base, 8)
            f2[at, :] = 0.75 * f0[at, :] + 0.25 * value

        stage(f1, tiles, base, write)
        return carry

    def third(i, carry):
        base = pl.multiple_of(i * 8 + 16, 8)
        place = pl.multiple_of(i * 8, 8)

        def write(j, value):
            kept = f0[pl.ds(span * j + base, 8), :]
            out_ref[pl.ds(place, 8), 128 * j : 128 * j + 128] = kept * (1.0 / 3.0) + (2.0 / 3.0) * value

        stage(f2, tiles - 1, base, write)
        return carry

    lax.fori_loop(0, height // 8 + 2, first, 0, unroll=2)
    lax.fori_loop(0, height // 8 + 2, second, 0, unroll=2)
    lax.fori_loop(0, height // 8, third, 0, unroll=2)


def deposit_body(rows_ref, recv_ref, base_ref, out_ref, moved_ref, sem):
    height, across = out_ref.shape
    step = 4 * CAP + 1
    bands = recv_ref.shape[0] // step
    block = 4 * CAP
    copy = pltpu.make_async_copy(rows_ref.at[:, pl.ds(0, block)], moved_ref, sem)
    copy.start()
    table = recv_ref[pl.ds(block, bands, stride=step), :]
    turned = jnp.transpose(table)
    count = CAP * bands

    def line(first, i):
        return jnp.concatenate([turned[first + 16 * k + i : first + 16 * k + i + 1] for k in range(CAP)], axis=1)

    r = iota((height, count), 0)
    row, col, ll, hl, lh, hh = [line(0, i) for i in range(6)]
    inside = col < float(across - 1)
    at, under = r == row, r == row + 1.0
    low = jnp.where(at, ll, jnp.where(under, hl, 0.0))
    high = jnp.where(inside & at, lh, jnp.where(inside & under, hh, 0.0))
    row, lh, hh = [line(0, 8 + i) for i in range(3)]
    side = jnp.where(r == row, lh, jnp.where(r == row + 1.0, hh, 0.0))
    row, col, _, hl, _, hh = [line(64, i) for i in range(6)]
    top = (r == 0.0) & (row == float(height - 1))
    low = jnp.concatenate([low, jnp.where(top, hl, 0.0)], axis=1)
    high = jnp.concatenate([high, jnp.where(top & (col < float(across - 1)), hh, 0.0)], axis=1)
    side = side + jnp.where((r == 0.0) & (line(64, 8) == float(height - 1)), line(64, 10), 0.0)

    def two(x):
        hi = x.astype(BF16)
        return [hi, (x - hi.astype(F32)).astype(BF16)]

    lanes = iota((bands, across), 1)
    places = [table[:, o + 16 * k + 1 : o + 16 * k + 2] for o in (0, 64) for k in range(CAP)]
    spread = jnp.concatenate([one_hot(lanes == place) for place in places], axis=0)
    total = mm(jnp.concatenate(two(low) + two(high), axis=0), spread)
    same = total[0:height] + total[height : 2 * height]
    right = total[2 * height : 3 * height] + total[3 * height :]
    c = iota((height, across), 1)
    out_ref[...] = base_ref[...] + (same + jnp.where(c == 0.0, lane_sum(side), pltpu.roll(right, 1, 1)))
    copy.wait()


def ring(axis, distance):
    n = lax.axis_size(axis)
    return [(i, (i + distance) % n) for i in range(n)]


def shards(level_set, velocity, particles, escaped, home_cell, land_cell, dest_rank, block_count):
    height, across = level_set.shape
    n = particles.shape[0]
    bands = lax.axis_size("gy")
    step = 4 * CAP + 1
    sds = jax.ShapeDtypeStruct
    head, tail = call(
        heads_body,
        (sds((24, across), F32), sds((24, across), F32)),
        pltpu.with_memory_space_constraint(level_set, pltpu.HBM),
        pltpu.with_memory_space_constraint(velocity, pltpu.HBM),
        spaces=[pltpu.HBM, pltpu.HBM],
        scratch=[pltpu.VMEM((2, 16, across), F32), pltpu.VMEM((2, 2, 8, across), F32), pltpu.SemaphoreType.DMA((4,))],
    )
    below = lax.ppermute(head, "gy", ring("gy", -1))
    above = lax.ppermute(tail, "gy", ring("gy", 1))
    parts = jnp.transpose(particles, (1, 0, 2))
    meta, weight, near_x, near_y, select, fixed = call(
        prepare_body,
        (
            *[sds((n, 128), F32)] * 4,
            sds((bands * CAP, 3 * n), BF16),
            sds((bands * CAP, 256), F32),
        ),
        level_set, velocity, parts, escaped, home_cell.reshape(1, n), land_cell.reshape(1, n), dest_rank.reshape(1, n),
        scalars=(block_count,),
    )
    to_left, to_right, near_x, near_y = call(
        edges_body,
        (*[sds((height + 16, 128), F32)] * 2, *[sds((n, 128), F32)] * 2),
        level_set, velocity, below, meta, parts, weight, near_x, near_y,
    )
    from_left = lax.ppermute(to_right, "gx", ring("gx", 1))
    from_right = lax.ppermute(to_left, "gx", ring("gx", -1))
    (side,) = call(
        functools.partial(side_body, n=n, across=across),
        (sds((bands * CAP, 128), F32),),
        from_left, to_left,
    )
    (packed,) = call(
        functools.partial(pack_body, across=across),
        (sds((bands * step, 128), F32),),
        parts, weight, near_x, near_y, meta, from_right, select, fixed, side,
    )
    arrived = lax.all_to_all(
        packed.reshape(bands * step, 1, 128), "gy", split_axis=0, concat_axis=0, tiled=True
    )
    to_left2, to_right2 = call(corners_body, (sds((16, 128), F32), sds((16, 128), F32)), above)
    from_left2 = lax.ppermute(to_right2, "gx", ring("gx", 1))
    from_right2 = lax.ppermute(to_left2, "gx", ring("gx", -1))
    wide = pltpu.VMEM(((across // 128 + 1) * (height + 32), 128), F32)
    (section,) = call(
        stencil_body,
        (sds((height, across), F32),),
        level_set, velocity, below, above, from_right, from_left, from_right2, from_left2,
        scratch=[wide] * 5,
    )
    level, moved = call(
        deposit_body,
        (sds((height, across), F32), sds((bands, 4 * CAP, 1, 128), F32)),
        arrived.reshape(bands, step, 1, 128), arrived.reshape(bands * step, 128), section,
        out_spaces=[pltpu.VMEM, pltpu.HBM],
        scratch=[pltpu.SemaphoreType.DMA],
    )
    return level, moved.reshape(bands * CAP, 4, 128)


def solution(mesh):
    in_specs = (
        P("gy", "gx"),
        P(None, "gy", "gx"),
        P(("gy", "gx"), None, None),
        P(("gy", "gx"), None),
        P(("gy", "gx")),
        P(("gy", "gx")),
        P(("gy", "gx")),
        P(("gy", "gx")),
    )
    out_specs = (P("gy", "gx"), P(("gy", "gx"), None, None))
    return jax.shard_map(shards, mesh=mesh, in_specs=in_specs, out_specs=out_specs, check_vma=False)
```
